32 devices in a mesh: seq: 4 (over y, x), dp: 8 (over z, core).
Axes of the slice: x: 2, y: 2, z: 4, core: 2. Of those that a mesh axis runs over, the one named last changes fastest.
Arguments:
- hidden_in: bfloat16 [8, 2048, 768], P('dp', 'seq'), may hold values from -6 to 6
- seq_lengths: int32 [8], P('dp'), may hold values from 128 to 2048, as said below
- attention_gain: float32 [768], replicated, may hold values from 0.1 to 1.9
- attention_shift: float32 [768], replicated, may hold values from -3 to 3
- feed_gain: float32 [768], replicated, may hold values from 0.1 to 1.9
- feed_shift: float32 [768], replicated, may hold values from -3 to 3
- query_weight: bfloat16 [768, 768], replicated, may hold values from -0.21875 to 0.21875
- query_bias: float32 [768], replicated, may hold values from -3 to 3
- keyval_weight: bfloat16 [768, 128], replicated, may hold values from -0.21875 to 0.21875
- keyval_bias: float32 [128], replicated, may hold values from -3 to 3
- dense_weight: bfloat16 [768, 768], replicated, may hold values from -1.75 to 1.75
- dense_bias: float32 [768], replicated, may hold values from -3 to 3
- expand_weight: bfloat16 [768, 3072], replicated, may hold values from -0.21875 to 0.21875
- expand_bias: float32 [3072], replicated, may hold values from -3 to 3
- project_weight: bfloat16 [3072, 768], replicated, may hold values from -0.109375 to 0.109375
- project_bias: float32 [768], replicated, may hold values from -3 to 3
- out_grad: bfloat16 [8, 2048, 768], P('dp', 'seq'), may hold values from -6 to 6
Outputs:
- output: bfloat16 [8, 2048, 768], P('dp', 'seq')
- input_grad: float32 [8, 2048, 768], P('dp', 'seq')
- attention_gain_grad: float32 [768], replicated
- attention_shift_grad: float32 [768], replicated
- feed_gain_grad: float32 [768], replicated
- feed_shift_grad: float32 [768], replicated
- query_weight_grad: float32 [768, 768], P('dp', 'seq')
- query_bias_grad: float32 [768], replicated
- keyval_weight_grad: float32 [768, 128], P('dp', 'seq')
- keyval_bias_grad: float32 [128], replicated
- dense_weight_grad: float32 [768, 768], P('dp', 'seq')
- dense_bias_grad: float32 [768], replicated
- expand_weight_grad: float32 [768, 3072], P('dp', 'seq')
- expand_bias_grad: float32 [3072], replicated
- project_weight_grad: float32 [3072, 768], P('dp', 'seq')
- project_bias_grad: float32 [768], replicated
The draws below stay inside these ranges and needn't reach their ends.
Inputs may be any that keep to these rules, and one draw needn't show every extreme that they name: `seq_lengths`: the valid tokens of a sequence are its first ones; in every draw one sequence fills all 2048 slots and one has exactly 128.
All inputs are finite; a program needn't handle non-finite values.
Results may differ from the reference program's by a relative error of at most 0.012.
Values may be sent and summed in bfloat16 or wider, within the bound.
A program may use at most 192 MiB of HBM per device.

```python
import jax
import jax.numpy as jnp
from jax import lax

D = 768
HEADS = 12
HD = 64
ROT = 16
FF = 3072
LEN = 2048
MINLEN = 128
NSEQ = 8


def draw_seq_lengths(key, part):
    subkeys = jax.random.split(key, 3)
    lengths = jax.random.randint(subkeys[0], (NSEQ,), MINLEN, LEN + 1)
    longest = jax.random.randint(subkeys[1], (), 0, NSEQ)
    shortest = (longest + 1 + jax.random.randint(subkeys[2], (), 0, NSEQ - 1)) % NSEQ
    places = jnp.arange(NSEQ, dtype=jnp.int32)
    lengths = jnp.where(places == longest, LEN, lengths)
    lengths = jnp.where(places == shortest, MINLEN, lengths)
    return lengths.astype(jnp.int32)


def level_of(key, shape, cuts, least, top_value):
    gain = 1.0
    for dim, parts in cuts:
        steps = jax.random.uniform(jax.random.fold_in(jax.random.fold_in(key, 6), dim), (parts,), jnp.float32, least / len(cuts), top_value / len(cuts))
        gain = gain * jnp.repeat(jnp.exp(steps), shape[dim] // parts).reshape((-1,) + (1,) * (len(shape) - 1 - dim))
    return gain


def bell_draw(stream_key, shape, scale, limit, pieces=(), kind=jnp.bfloat16):
    values = jax.random.normal(stream_key, shape, jnp.float32) * scale
    if len(pieces) > 0:
        values = level_of(stream_key, shape, pieces, -0.22, 0.18) * values
    return jnp.clip(values, min=-limit, max=limit).astype(kind)


def setup_inputs(seed: int = 0) -> dict:
    seeds = jax.random.split(jax.random.key(seed), 18)
    return {
        "hidden_in": bell_draw(seeds[0], (NSEQ, LEN, D), 1.0, 6.0, ((0, 8), (1, 4))),
        "seq_lengths": draw_seq_lengths(jax.random.fold_in(seeds[17], 71), 0),
        "attention_gain": jnp.clip(1.0 + 0.18 * jax.random.normal(seeds[2], (D,), jnp.float32), 0.1, 1.9),
        "attention_shift": bell_draw(seeds[3], (D,), 0.5, 3.0, (), jnp.float32),
        "feed_gain": jnp.clip(1.0 + 0.18 * jax.random.normal(seeds[4], (D,), jnp.float32), 0.1, 1.9),
        "feed_shift": bell_draw(seeds[5], (D,), 0.5, 3.0, (), jnp.float32),
        "query_weight": bell_draw(seeds[6], (D, D), D ** -0.5, 0.21875),
        "query_bias": bell_draw(seeds[7], (D,), 0.5, 3.0, (), jnp.float32),
        "keyval_weight": bell_draw(seeds[8], (D, 2 * HD), D ** -0.5, 0.21875),
        "keyval_bias": bell_draw(seeds[9], (2 * HD,), 0.5, 3.0, (), jnp.float32),
        "dense_weight": bell_draw(seeds[10], (D, D), (D // 64) ** -0.5, 1.75),
        "dense_bias": bell_draw(seeds[11], (D,), 0.5, 3.0, (), jnp.float32),
        "expand_weight": bell_draw(seeds[12], (D, FF), D ** -0.5, 0.21875),
        "expand_bias": bell_draw(seeds[13], (FF,), 0.5, 3.0, (), jnp.float32),
        "project_weight": bell_draw(seeds[14], (FF, D), FF ** -0.5, 0.109375),
        "project_bias": bell_draw(seeds[15], (D,), 0.5, 3.0, (), jnp.float32),
        "out_grad": bell_draw(seeds[16], (NSEQ, LEN, D), 1.0, 6.0, ((0, 8), (1, 4))),
    }


@jax.custom_vjp
def low(v):
    return lax.optimization_barrier(v.astype(jnp.bfloat16)).astype(jnp.float32)

@jax.custom_vjp
def low_back(v):
    return v

def low_keep(v):
    return (low(v), None)

def low_pass(kept, grad):
    return (grad,)

def back_keep(v):
    return (v, None)

def back_low(kept, grad):
    return (low(grad),)
low.defvjp(low_keep, low_pass)
low_back.defvjp(back_keep, back_low)
norm_eps = 1e-05
masked_score = -1e+30

def matmul(left, right):
    return jnp.dot(left, right, precision=lax.Precision.HIGHEST)

def layer_norm(values, gains, shifts):
    average = lax.optimization_barrier(jnp.mean(values, axis=-1, keepdims=True))
    centered = values - average
    variance = lax.optimization_barrier(jnp.mean(centered * centered, axis=-1, keepdims=True))
    return centered * lax.rsqrt(variance + norm_eps) * gains + shifts

def rotate(vectors, positions):
    half_rot = ROT // 2
    frequency = 10000.0 ** (-2.0 * jnp.arange(half_rot, dtype=jnp.float32) / ROT)
    angles = positions.astype(jnp.float32)[:, None] * frequency[None, :]
    cosine = jnp.cos(angles)
    sine_part = jnp.sin(angles)
    lead_part = vectors[..., :half_rot]
    pair_part = vectors[..., half_rot:ROT]
    rest_part = vectors[..., ROT:]
    return jnp.concatenate([lead_part * cosine - pair_part * sine_part, pair_part * cosine + lead_part * sine_part, rest_part], axis=-1)

def one_sequence(weights, hidden, length):
    attention_gain, attention_shift, feed_gain, feed_shift, query_weight, query_bias, keyval_weight, keyval_bias, dense_weight, dense_bias, expand_weight, expand_bias, project_weight, project_bias = weights
    positions = jnp.arange(LEN, dtype=jnp.int32)
    attn_in = low(layer_norm(hidden, attention_gain, attention_shift))
    feed_in = low(layer_norm(hidden, feed_gain, feed_shift))
    query_pre = low_back(matmul(attn_in, query_weight) + query_bias)
    keyval_pre = low_back(matmul(attn_in, keyval_weight) + keyval_bias)
    shaped = query_pre.reshape(LEN, HEADS, HD).transpose(1, 0, 2)
    query = low(rotate(shaped, positions) * HD ** (-0.5))
    keyval = low(jnp.concatenate([rotate(keyval_pre[:, :HD], positions), keyval_pre[:, HD:]], axis=-1))
    key_rows = keyval[:, :HD]
    values = keyval[:, HD:]
    allowed = (positions[None, :] <= positions[:, None]) & (positions[None, :] < length)

    def one_head(query_head):
        scores = low_back(matmul(query_head, key_rows.T))
        scores = jnp.where(allowed, scores, masked_score)
        soft_weights = jnp.exp(scores - jax.nn.logsumexp(scores, axis=-1, keepdims=True))
        return matmul(low(soft_weights), values)
    mixed = lax.map(jax.checkpoint(one_head), query)
    mixed = low(low_back(mixed.transpose(1, 0, 2).reshape(LEN, D)))
    attn_out = matmul(mixed, dense_weight) + dense_bias
    upper = low_back(matmul(feed_in, expand_weight) + expand_bias)
    active = low(jax.nn.gelu(upper, approximate=False))
    feed_out = matmul(active, project_weight) + project_bias
    return hidden + attn_out + feed_out

def reference(hidden_in, seq_lengths, attention_gain, attention_shift, feed_gain, feed_shift, query_weight, query_bias, keyval_weight, keyval_bias, dense_weight, dense_bias, expand_weight, expand_bias, project_weight, project_bias, out_grad):
    weights = (attention_gain.astype(jnp.float32), attention_shift.astype(jnp.float32), feed_gain.astype(jnp.float32), feed_shift.astype(jnp.float32), query_weight.astype(jnp.float32), query_bias.astype(jnp.float32), keyval_weight.astype(jnp.float32), keyval_bias.astype(jnp.float32), dense_weight.astype(jnp.float32), dense_bias.astype(jnp.float32), expand_weight.astype(jnp.float32), expand_bias.astype(jnp.float32), project_weight.astype(jnp.float32), project_bias.astype(jnp.float32))
    inputs = hidden_in.astype(jnp.float32)

    def forward(weight_set, hidden_all):

        def per_sequence(operands):
            return one_sequence(weight_set, operands[0], operands[1])
        return lax.map(jax.checkpoint(per_sequence), (hidden_all, seq_lengths))
    result, pullback = jax.vjp(forward, weights, inputs)
    valid_rows = jnp.arange(LEN, dtype=jnp.int32)[None, :] < seq_lengths[:, None]
    cotangent = jnp.where(valid_rows[:, :, None], out_grad.astype(jnp.float32), jnp.zeros_like(result))
    weight_grads, input_grad = pullback(cotangent)
    return (result.astype(jnp.bfloat16), input_grad, weight_grads[0], weight_grads[1], weight_grads[2], weight_grads[3], weight_grads[4], weight_grads[5], weight_grads[6], weight_grads[7], weight_grads[8], weight_grads[9], weight_grads[10], weight_grads[11], weight_grads[12], weight_grads[13])
```

```python
import functools

import jax
import jax.numpy as jnp
from jax import lax
from jax.experimental import pallas as pl
from jax.experimental.pallas import tpu as pltpu
from jax.sharding import PartitionSpec as P

HEADS = 12
HD = 64
ROT = 16
f32 = jnp.float32
bf16 = jnp.bfloat16


norm_eps = 1e-05
masked_score = -1e30


def layer_norm(values, gains, shifts):
    average = jnp.mean(values, axis=-1, keepdims=True)
    centered = values - average
    variance = jnp.mean(centered * centered, axis=-1, keepdims=True)
    return centered * lax.rsqrt(variance + norm_eps) * gains + shifts


def rotate(vectors, positions):
    half_rot = ROT // 2
    frequency = 10000.0 ** (-2.0 * jnp.arange(half_rot, dtype=jnp.float32) / ROT)
    angles = positions.astype(jnp.float32)[:, None] * frequency[None, :]
    cosine = jnp.cos(angles)
    sine_part = jnp.sin(angles)
    lead_part = vectors[..., :half_rot]
    pair_part = vectors[..., half_rot:ROT]
    rest_part = vectors[..., ROT:]
    return jnp.concatenate(
        [
            lead_part * cosine - pair_part * sine_part,
            pair_part * cosine + lead_part * sine_part,
            rest_part,
        ],
        axis=-1,
    )


def exact_gelu(values):
    return jax.nn.gelu(values, approximate=False)


def outer_sum(left, right):
    return lax.dot_general(
        left, right, (((0,), (0,)), ((), ())), preferred_element_type=jnp.float32
    )


def per_device(
    hidden_in,
    seq_lengths,
    attention_gain,
    attention_shift,
    feed_gain,
    feed_shift,
    query_weight,
    query_bias,
    keyval_weight,
    keyval_bias,
    dense_weight,
    dense_bias,
    expand_weight,
    expand_bias,
    project_weight,
    project_bias,
    out_grad,
):
    seq_count, stretch_len, model_width = hidden_in.shape
    seq_parts = lax.axis_size("seq")
    whole_len = stretch_len * seq_parts
    offset = lax.axis_index("seq") * stretch_len
    positions = offset + jnp.arange(stretch_len, dtype=jnp.int32)
    row_count = seq_count * stretch_len
    query_scale = HD ** (-0.5)
    inputs = hidden_in.astype(jnp.float32).reshape(row_count, model_width)
    valid_rows = positions[None, :] < seq_lengths[:, None]
    grad_out = jnp.where(valid_rows[:, :, None], out_grad, jnp.zeros_like(out_grad)).reshape(
        row_count, model_width
    )
    attn_norm, attn_norm_back = jax.vjp(layer_norm, inputs, attention_gain, attention_shift)
    feed_norm, feed_norm_back = jax.vjp(layer_norm, inputs, feed_gain, feed_shift)
    attn_in = attn_norm.astype(jnp.bfloat16)
    feed_in = feed_norm.astype(jnp.bfloat16)
    query_pre = jnp.dot(attn_in, query_weight, preferred_element_type=jnp.float32) + query_bias
    keyval_pre = jnp.dot(attn_in, keyval_weight, preferred_element_type=jnp.float32) + keyval_bias

    def turn_query(flat_query):
        shaped = flat_query.reshape(seq_count, stretch_len, HEADS, HD).transpose(0, 2, 1, 3)
        return rotate(shaped, positions) * query_scale

    def turn_keyval(flat_keyval):
        shaped = flat_keyval.reshape(seq_count, stretch_len, 2 * HD)
        return jnp.concatenate([rotate(shaped[..., :HD], positions), shaped[..., HD:]], axis=-1)

    query_rot, query_back = jax.vjp(turn_query, query_pre)
    keyval_rot, keyval_back = jax.vjp(turn_keyval, keyval_pre)
    query_low = query_rot.astype(jnp.bfloat16)
    keyval_low = keyval_rot.astype(jnp.bfloat16)
    gathered = lax.all_gather(keyval_low, "seq", axis=1, tiled=True)
    grad_mixed = jnp.dot(grad_out, dense_weight.T, preferred_element_type=jnp.float32).astype(
        jnp.bfloat16
    )
    grad_heads = grad_mixed.reshape(seq_count, stretch_len, HEADS, HD).transpose(0, 2, 1, 3)
    key_block = min(512, whole_len)
    block_count = whole_len // key_block
    group_size = 4

    def attend(operands):
        query_seq, grad_seq, keyval_seq, length = operands
        extent = block_count * key_block
        key_rows = keyval_seq[:extent, :HD]
        values = keyval_seq[:extent, HD:]
        key_pos = jnp.arange(extent, dtype=jnp.int32)
        allowed = (key_pos[None, :] <= positions[:, None]) & (key_pos[None, :] < length)

        def one_group(group_pair):
            query_grp, grad_grp = group_pair
            scores = jnp.einsum(
                "gtd,sd->gts", query_grp, key_rows, preferred_element_type=jnp.float32
            )
            scores = jnp.where(allowed[None], scores, masked_score)
            log_total = jax.nn.logsumexp(scores, axis=-1, keepdims=True)
            soft_weights = jnp.exp(scores - log_total)
            soft_low = soft_weights.astype(jnp.bfloat16)
            mixed_part = jnp.einsum(
                "gts,sd->gtd", soft_low, values, preferred_element_type=jnp.float32
            )
            grad_soft = jnp.einsum(
                "gtd,sd->gts", grad_grp, values, preferred_element_type=jnp.float32
            )
            row_delta = jnp.sum(soft_weights * grad_soft, axis=-1, keepdims=True)
            grad_scores = (soft_weights * (grad_soft - row_delta)).astype(jnp.bfloat16)
            grad_query = jnp.einsum(
                "gts,sd->gtd", grad_scores, key_rows, preferred_element_type=jnp.float32
            )
            grad_keys = jnp.einsum(
                "gts,gtd->sd", grad_scores, query_grp, preferred_element_type=jnp.float32
            )
            grad_values = jnp.einsum(
                "gts,gtd->sd", soft_low, grad_grp, preferred_element_type=jnp.float32
            )
            return (mixed_part, grad_query, jnp.concatenate([grad_keys, grad_values], axis=-1))

        grouped_query = query_seq.reshape(HEADS // group_size, group_size, stretch_len, HD)
        grouped_grad = grad_seq.reshape(HEADS // group_size, group_size, stretch_len, HD)
        mixed_part, grad_query, grad_keyval = lax.map(one_group, (grouped_query, grouped_grad))
        grad_keyval = jnp.sum(grad_keyval, axis=0)
        return (
            mixed_part.reshape(HEADS, stretch_len, HD),
            grad_query.reshape(HEADS, stretch_len, HD),
            grad_keyval,
        )

    mixed_all, grad_query_all, grad_keyval_all = lax.map(
        attend, (query_low, grad_heads, gathered, seq_lengths)
    )
    grad_keyval_own = lax.psum_scatter(grad_keyval_all, "seq", scatter_dimension=1, tiled=True)
    mixed_low = mixed_all.transpose(0, 2, 1, 3).reshape(row_count, model_width).astype(jnp.bfloat16)
    attn_out = jnp.dot(mixed_low, dense_weight, preferred_element_type=jnp.float32) + dense_bias
    upper = jnp.dot(feed_in, expand_weight, preferred_element_type=jnp.float32) + expand_bias
    active, active_back = jax.vjp(exact_gelu, upper)
    active_low = active.astype(jnp.bfloat16)
    feed_out = (
        jnp.dot(active_low, project_weight, preferred_element_type=jnp.float32) + project_bias
    )
    output = (
        (inputs + attn_out + feed_out)
        .astype(jnp.bfloat16)
        .reshape(seq_count, stretch_len, model_width)
    )
    grad_active = jnp.dot(grad_out, project_weight.T, preferred_element_type=jnp.float32)
    grad_upper = active_back(grad_active)[0].astype(jnp.bfloat16)
    grad_query_pre = query_back(grad_query_all)[0].astype(jnp.bfloat16)
    grad_keyval_pre = keyval_back(grad_keyval_own)[0].astype(jnp.bfloat16)
    grad_attn_in = jnp.dot(
        grad_query_pre, query_weight.T, preferred_element_type=jnp.float32
    ) + jnp.dot(grad_keyval_pre, keyval_weight.T, preferred_element_type=jnp.float32)
    grad_feed_in = jnp.dot(grad_upper, expand_weight.T, preferred_element_type=jnp.float32)
    attn_dx, attn_dgain, attn_dshift = attn_norm_back(grad_attn_in)
    feed_dx, feed_dgain, feed_dshift = feed_norm_back(grad_feed_in)
    input_grad = (grad_out.astype(jnp.float32) + attn_dx + feed_dx).reshape(
        seq_count, stretch_len, model_width
    )
    query_term = outer_sum(attn_in, grad_query_pre)
    keyval_term = outer_sum(attn_in, grad_keyval_pre)
    dense_term = outer_sum(mixed_low, grad_out)
    expand_term = outer_sum(feed_in, grad_upper)
    project_term = outer_sum(active_low, grad_out)
    row_sums = (
        lax.psum_scatter(query_term, "dp", scatter_dimension=0, tiled=True),
        lax.psum_scatter(keyval_term, "dp", scatter_dimension=0, tiled=True),
        lax.psum_scatter(dense_term, "dp", scatter_dimension=0, tiled=True),
        lax.psum_scatter(expand_term, "dp", scatter_dimension=0, tiled=True),
        lax.psum_scatter(project_term, "dp", scatter_dimension=0, tiled=True),
    )
    weight_grads = (
        lax.psum_scatter(row_sums[0], "seq", scatter_dimension=1, tiled=True),
        lax.psum_scatter(row_sums[1], "seq", scatter_dimension=1, tiled=True),
        lax.psum_scatter(row_sums[2], "seq", scatter_dimension=1, tiled=True),
        lax.psum_scatter(row_sums[3], "seq", scatter_dimension=1, tiled=True),
        lax.psum_scatter(row_sums[4], "seq", scatter_dimension=1, tiled=True),
    )
    out_total = jnp.sum(grad_out, axis=0, dtype=jnp.float32)
    small_sums = lax.psum(
        (
            attn_dgain,
            attn_dshift,
            feed_dgain,
            feed_dshift,
            jnp.sum(grad_query_pre, axis=0, dtype=jnp.float32),
            jnp.sum(grad_keyval_pre, axis=0, dtype=jnp.float32),
            out_total,
            jnp.sum(grad_upper, axis=0, dtype=jnp.float32),
        ),
        ("seq", "dp"),
    )
    return (
        output,
        input_grad,
        small_sums[0],
        small_sums[1],
        small_sums[2],
        small_sums[3],
        weight_grads[0],
        small_sums[4],
        weight_grads[1],
        small_sums[5],
        weight_grads[2],
        small_sums[6],
        weight_grads[3],
        small_sums[7],
        weight_grads[4],
        small_sums[6],
    )


NT_DIMS = (((1,), (1,)), ((), ()))
MESH_ID = pl.DeviceIdType.MESH


def attend_kernel(
    seq_parts, half_parts, q_ref, gm_ref, kaug_ref, val_ref, kvt_ref, ge_ref, gp_ref,
    mix_ref, dq_ref, dkv_ref, oute_ref, outp_ref,
    score, expo, qaug, pair, core_e, core_p, plane_e, plane_p, part_e, part_p, line_e, line_p,
    core_send, core_recv, es_send, es_recv, ps_send, ps_recv, ez_send, ez_recv, pz_send, pz_recv,
):
    width, stretch = q_ref.shape
    whole_len = kaug_ref.shape[0]
    blocks = whole_len // stretch
    seq = lax.axis_index("seq")
    dp = lax.axis_index("dp")
    core = lax.rem(dp, 2)
    line = lax.div(dp, 2)
    e_rows, e_cols = oute_ref.shape
    p_rows, p_cols = outp_ref.shape

    def seq_of(step):
        return lax.rem(seq + step, seq_parts)

    def line_of(step):
        return lax.rem(line + step, half_parts)

    barrier = pltpu.get_barrier_semaphore()
    pl.semaphore_signal(barrier, inc=1, device_id={"dp": dp + 1 - 2 * core}, device_id_type=MESH_ID)
    for step in range(1, seq_parts):
        pl.semaphore_signal(barrier, inc=1, device_id={"seq": seq_of(step)}, device_id_type=MESH_ID)
    for step in range(1, half_parts):
        pl.semaphore_signal(
            barrier, inc=1, device_id={"dp": line_of(step) * 2 + core}, device_id_type=MESH_ID
        )
    pl.semaphore_wait(barrier, seq_parts + half_parts - 1)

    def ds(start, size, unit):
        return pl.ds(pl.multiple_of(start, unit), size)

    def core_copies(step):
        part = seq_of(step + 1)
        peer = {"dp": dp + 1 - 2 * core}
        copies = []
        for place in range(half_parts):
            copies.append(
                pltpu.make_async_remote_copy(
                    src_ref=ge_ref.at[
                        ds((2 * place + 1 - core) * e_rows, e_rows, 16), ds(part * e_cols, e_cols, 128)
                    ],
                    dst_ref=core_e.at[step, place],
                    send_sem=core_send.at[step, place],
                    recv_sem=core_recv.at[step, place],
                    device_id=peer,
                    device_id_type=MESH_ID,
                )
            )
        copies.append(
            pltpu.make_async_remote_copy(
                src_ref=gp_ref.at[:, ds((2 * part + 1 - core) * p_cols, p_cols, 128)],
                dst_ref=core_p.at[step],
                send_sem=core_send.at[step, half_parts],
                recv_sem=core_recv.at[step, half_parts],
                device_id=peer,
                device_id_type=MESH_ID,
            )
        )
        return copies

    def plane_e_copy(step):
        return pltpu.make_async_remote_copy(
            src_ref=core_e.at[step],
            dst_ref=plane_e.at[step],
            send_sem=es_send.at[step],
            recv_sem=es_recv.at[step],
            device_id={"seq": seq_of(step + 1)},
            device_id_type=MESH_ID,
        )

    def plane_p_copy(step, hop):
        part = seq_of(step + 1)
        return pltpu.make_async_remote_copy(
            src_ref=core_p.at[step, ds(seq_of(hop) * p_rows, p_rows, 16), :],
            dst_ref=plane_p.at[part, hop - 1],
            send_sem=ps_send.at[step, hop - 1],
            recv_sem=ps_recv.at[part, hop - 1],
            device_id={"seq": seq_of(hop)},
            device_id_type=MESH_ID,
        )

    def line_e_copy(hop):
        return pltpu.make_async_remote_copy(
            src_ref=part_e.at[line_of(hop)],
            dst_ref=line_e.at[hop - 1],
            send_sem=ez_send.at[hop - 1],
            recv_sem=ez_recv.at[hop - 1],
            device_id={"dp": line_of(hop) * 2 + core},
            device_id_type=MESH_ID,
        )

    def line_p_copy(hop):
        return pltpu.make_async_remote_copy(
            src_ref=part_p.at[line_of(hop)],
            dst_ref=line_p.at[hop - 1],
            send_sem=pz_send.at[hop - 1],
            recv_sem=pz_recv.at[hop - 1],
            device_id={"dp": line_of(hop) * 2 + core},
            device_id_type=MESH_ID,
        )

    def add_core(step):
        part = seq_of(step + 1)
        for copy in core_copies(step):
            copy.wait()
        for place in range(half_parts):
            own = ge_ref[ds((2 * place + core) * e_rows, e_rows, 16), ds(part * e_cols, e_cols, 128)]
            core_e[step, place] = (own.astype(f32) + core_e[step, place].astype(f32)).astype(bf16)
        own = gp_ref[:, ds((2 * part + core) * p_cols, p_cols, 128)]
        core_p[step] = (own.astype(f32) + core_p[step].astype(f32)).astype(bf16)

    def send_plane(step):
        if step < seq_parts - 1:
            plane_e_copy(step).start()
        for hop in range(1, seq_parts):
            plane_p_copy(step, hop).start()

    def add_plane_p(step):
        part = seq_of(step + 1)
        total = core_p[step, ds(seq * p_rows, p_rows, 16), :].astype(f32)
        for hop in range(1, seq_parts):
            copy = plane_p_copy(step, hop)
            copy.wait_send()
            copy.wait_recv()
            total = total + plane_p[part, hop - 1].astype(f32)
        part_p[part] = total.astype(bf16)

    def add_plane_e():
        last = seq_parts - 1
        for step in range(last):
            copy = plane_e_copy(step)
            copy.wait()
        for place in range(half_parts):
            total = core_e[last, place].astype(f32)
            for step in range(last):
                total = total + plane_e[step, place].astype(f32)
            part_e[place] = total.astype(bf16)

    ones_row = lax.broadcasted_iota(jnp.int32, (16, stretch), 0) == 0
    qaug[HD : HD + 16, :] = jnp.where(ones_row, 1.0, 0.0).astype(bf16)
    qaug[HD + 16 :, :] = jnp.zeros((HD - 16, stretch), bf16)
    pair[...] = jnp.zeros(pair.shape, bf16)
    dkv_ref[...] = jnp.zeros(dkv_ref.shape, f32)
    for step in range(seq_parts):
        for copy in core_copies(step):
            copy.start()
    key_pos = lax.broadcasted_iota(jnp.int32, (stretch, stretch), 0)
    query_pos = lax.broadcasted_iota(jnp.int32, (stretch, stretch), 1)

    def one_head(head, carry):
        for step in range(seq_parts):
            @pl.when(head == 1 + 2 * step)
            def _(step=step):
                add_core(step)

            @pl.when(head == 2 + 2 * step)
            def _(step=step):
                send_plane(step)

        rows = ds(head * HD, HD, HD)
        query = q_ref[rows, :]
        qaug[0:HD, :] = query
        top = None
        for block in range(blocks):
            span = slice(block * stretch, (block + 1) * stretch)
            part = jnp.dot(kaug_ref[span, :], qaug[...], preferred_element_type=f32)
            if block == 0:
                part = jnp.where(key_pos <= query_pos, part, masked_score)
            score[span, :] = part
            block_top = jnp.max(part, axis=0, keepdims=True)
            top = block_top if top is None else jnp.maximum(top, block_top)
        total = jnp.zeros((1, stretch), f32)
        mixed = jnp.zeros((HD, stretch), f32)
        for block in range(blocks):
            span = slice(block * stretch, (block + 1) * stretch)
            raised = jnp.exp(score[span, :] - top)
            total = total + jnp.sum(raised, axis=0, keepdims=True)
            low = raised.astype(bf16)
            expo[span, :] = low
            mixed = mixed + jnp.dot(kvt_ref[HD:, span], low, preferred_element_type=f32)
        scale = 1.0 / total
        mixed = mixed * scale
        mix_ref[rows, :] = mixed.astype(bf16)
        grad = gm_ref[rows, :].astype(f32) * scale
        delta = jnp.sum(grad * mixed, axis=0, keepdims=True)
        grad = grad.astype(bf16)
        pair[0:HD, 0:stretch] = query
        pair[HD:, stretch:] = grad
        grad_query = jnp.zeros((HD, stretch), f32)
        for block in range(blocks):
            span = slice(block * stretch, (block + 1) * stretch)
            part = jnp.dot(val_ref[span, :], grad, preferred_element_type=f32)
            low = expo[span, :]
            grad_score = (low.astype(f32) * (part - delta)).astype(bf16)
            grad_query = grad_query + jnp.dot(
                kvt_ref[0:HD, span], grad_score, preferred_element_type=f32
            )
            dkv_ref[span, :] += lax.dot_general(
                jnp.concatenate([grad_score, low], axis=1), pair[...], NT_DIMS,
                preferred_element_type=f32,
            )
        dq_ref[rows, :] = grad_query
        return carry

    lax.fori_loop(0, HEADS, one_head, 0)
    for step in range(seq_parts):
        add_plane_p(step)
    add_plane_e()
    for hop in range(1, half_parts):
        line_e_copy(hop).start()
        line_p_copy(hop).start()
    total_e = part_e[line].astype(f32)
    total_p = part_p[line].astype(f32)
    for hop in range(1, half_parts):
        line_e_copy(hop).wait()
        line_p_copy(hop).wait()
        total_e = total_e + line_e[hop - 1].astype(f32)
        total_p = total_p + line_p[hop - 1].astype(f32)
    oute_ref[...] = total_e
    outp_ref[...] = total_p


def attend_and_reduce(seq_parts, dp_parts, query_t, grad_t, kaug, values, kvt, grad_e, grad_p):
    half = dp_parts // 2
    width, stretch = query_t.shape
    whole_len = kaug.shape[0]
    e_rows, e_cols = grad_e.shape[0] // dp_parts, grad_e.shape[1] // seq_parts
    p_rows, p_cols = grad_p.shape[0] // seq_parts, grad_p.shape[1] // dp_parts
    dma = pltpu.SemaphoreType.DMA
    vm = pl.BlockSpec(memory_space=pltpu.VMEM)
    return pl.pallas_call(
        functools.partial(attend_kernel, seq_parts, half),
        out_shape=(
            jax.ShapeDtypeStruct((width, stretch), bf16),
            jax.ShapeDtypeStruct((width, stretch), f32),
            jax.ShapeDtypeStruct((whole_len, 2 * HD), f32),
            jax.ShapeDtypeStruct((e_rows, e_cols), f32),
            jax.ShapeDtypeStruct((p_rows, p_cols), f32),
        ),
        in_specs=[vm] * 7,
        out_specs=(vm,) * 5,
        scratch_shapes=[
            pltpu.VMEM((whole_len, stretch), f32),
            pltpu.VMEM((whole_len, stretch), bf16),
            pltpu.VMEM((2 * HD, stretch), bf16),
            pltpu.VMEM((2 * HD, 2 * stretch), bf16),
            pltpu.VMEM((seq_parts, half, e_rows, e_cols), bf16),
            pltpu.VMEM((seq_parts, grad_p.shape[0], p_cols), bf16),
            pltpu.VMEM((seq_parts - 1, half, e_rows, e_cols), bf16),
            pltpu.VMEM((seq_parts, seq_parts - 1, p_rows, p_cols), bf16),
            pltpu.VMEM((half, e_rows, e_cols), bf16),
            pltpu.VMEM((half, p_rows, p_cols), bf16),
            pltpu.VMEM((half - 1, e_rows, e_cols), bf16),
            pltpu.VMEM((half - 1, p_rows, p_cols), bf16),
            dma((seq_parts, half + 1)), dma((seq_parts, half + 1)),
            dma((seq_parts - 1,)), dma((seq_parts - 1,)),
            dma((seq_parts, seq_parts - 1)), dma((seq_parts, seq_parts - 1)),
            dma((half - 1,)), dma((half - 1,)),
            dma((half - 1,)), dma((half - 1,)),
        ],
        compiler_params=pltpu.CompilerParams(
            collective_id=0, has_side_effects=True, vmem_limit_bytes=60 << 20
        ),
        cost_estimate=pl.CostEstimate(
            flops=24 * width * stretch * whole_len, bytes_accessed=20 << 20, transcendentals=0
        ),
    )(query_t, grad_t, kaug, values, kvt, grad_e, grad_p)


def fast_device(
    hidden_in, seq_lengths, attention_gain, attention_shift, feed_gain, feed_shift, query_weight,
    query_bias, keyval_weight, keyval_bias, dense_weight, dense_bias, expand_weight, expand_bias,
    project_weight, project_bias, out_grad,
):
    _, stretch, width = hidden_in.shape
    seq_parts = lax.axis_size("seq")
    dp_parts = lax.axis_size("dp")
    whole_len = stretch * seq_parts
    seq = lax.axis_index("seq")
    positions = seq * stretch + jnp.arange(stretch, dtype=jnp.int32)
    query_scale = HD ** (-0.5)
    inputs = hidden_in[0].astype(f32)
    length = seq_lengths[0]
    grad_out = jnp.where((positions < length)[:, None], out_grad[0], jnp.zeros_like(out_grad[0]))
    attn_norm, attn_norm_back = jax.vjp(layer_norm, inputs, attention_gain, attention_shift)
    feed_norm, feed_norm_back = jax.vjp(layer_norm, inputs, feed_gain, feed_shift)
    attn_in = attn_norm.astype(bf16)
    feed_in = feed_norm.astype(bf16)

    def turn_query(flat_query):
        shaped = flat_query.reshape(stretch, HEADS, HD).transpose(1, 0, 2)
        return rotate(shaped, positions) * query_scale

    def turn_keyval(flat_keyval):
        return jnp.concatenate([rotate(flat_keyval[:, :HD], positions), flat_keyval[:, HD:]], axis=-1)

    keyval_pre = jnp.dot(attn_in, keyval_weight, preferred_element_type=f32) + keyval_bias
    keyval_rot, keyval_back = jax.vjp(turn_keyval, keyval_pre)
    gathered = lax.all_gather(keyval_rot.astype(bf16), "seq", axis=0, tiled=True)
    query_pre = jnp.dot(attn_in, query_weight, preferred_element_type=f32) + query_bias
    query_rot, query_back = jax.vjp(turn_query, query_pre)
    query_t = query_rot.astype(bf16).transpose(0, 2, 1).reshape(width, stretch)
    grad_mixed_t = lax.dot_general(
        dense_weight, grad_out, NT_DIMS, preferred_element_type=f32
    ).astype(bf16)
    upper = jnp.dot(feed_in, expand_weight, preferred_element_type=f32) + expand_bias
    active, active_back = jax.vjp(exact_gelu, upper)
    active_low = active.astype(bf16)
    feed_out = jnp.dot(active_low, project_weight, preferred_element_type=f32) + project_bias
    grad_active = jnp.dot(grad_out, project_weight.T, preferred_element_type=f32)
    grad_upper = active_back(grad_active)[0].astype(bf16)
    grad_feed_in = jnp.dot(grad_upper, expand_weight.T, preferred_element_type=f32)
    feed_dx, feed_dgain, feed_dshift = feed_norm_back(grad_feed_in)
    expand_term = outer_sum(feed_in, grad_upper).astype(bf16)
    project_term = outer_sum(grad_out, active_low).astype(bf16)

    rolled = jnp.roll(gathered.reshape(seq_parts, stretch, 2 * HD), -seq, axis=0)
    block_seq = lax.rem(seq + jnp.arange(seq_parts, dtype=jnp.int32), seq_parts)
    key_pos = block_seq[:, None] * stretch + jnp.arange(stretch, dtype=jnp.int32)[None, :]
    usable = (block_seq <= seq)[:, None] & (key_pos < length)
    rolled = rolled.reshape(whole_len, 2 * HD)
    fence = jnp.where(usable.reshape(whole_len, 1), 0.0, masked_score).astype(bf16)
    kaug = jnp.concatenate(
        [rolled[:, :HD], fence, jnp.zeros((whole_len, HD - 1), bf16)], axis=1
    )
    mixed_t, grad_query_t, grad_keyval, expand_grad, project_grad = attend_and_reduce(
        seq_parts, dp_parts, query_t, grad_mixed_t, kaug, rolled[:, HD:], rolled.T,
        expand_term, project_term,
    )
    grad_keyval = jnp.roll(grad_keyval.reshape(seq_parts, stretch, 2 * HD), seq, axis=0)
    grad_keyval_own = lax.psum_scatter(
        grad_keyval.reshape(whole_len, 2 * HD), "seq", scatter_dimension=0, tiled=True
    )
    attn_out = lax.dot_general(
        mixed_t, dense_weight, (((0,), (0,)), ((), ())), preferred_element_type=f32
    ) + dense_bias
    output = (inputs + attn_out + feed_out).astype(bf16)[None]
    grad_query_all = grad_query_t.reshape(HEADS, HD, stretch).transpose(0, 2, 1)
    grad_query_pre = query_back(grad_query_all)[0].astype(bf16)
    grad_keyval_pre = keyval_back(grad_keyval_own)[0].astype(bf16)
    grad_attn_in = jnp.dot(grad_query_pre, query_weight.T, preferred_element_type=f32) + jnp.dot(
        grad_keyval_pre, keyval_weight.T, preferred_element_type=f32
    )
    attn_dx, attn_dgain, attn_dshift = attn_norm_back(grad_attn_in)
    input_grad = (grad_out.astype(f32) + attn_dx + feed_dx)[None]
    terms = (
        outer_sum(attn_in, grad_query_pre),
        outer_sum(attn_in, grad_keyval_pre),
        jnp.dot(mixed_t, grad_out, preferred_element_type=f32),
    )
    row_sums = [lax.psum_scatter(v, "dp", scatter_dimension=0, tiled=True) for v in terms]
    grads = [lax.psum_scatter(v, "seq", scatter_dimension=1, tiled=True) for v in row_sums]
    small = lax.psum(
        (
            attn_dgain, attn_dshift, feed_dgain, feed_dshift,
            jnp.sum(grad_query_pre, axis=0, dtype=f32),
            jnp.sum(grad_keyval_pre, axis=0, dtype=f32),
            jnp.sum(grad_out, axis=0, dtype=f32),
            jnp.sum(grad_upper, axis=0, dtype=f32),
        ),
        ("seq", "dp"),
    )
    return (
        output, input_grad, small[0], small[1], small[2], small[3], grads[0], small[4], grads[1],
        small[5], grads[2], small[6], expand_grad, small[7], project_grad.T, small[6],
    )


def fits(hidden, expand_weight):
    seq_parts, dp_parts = lax.axis_size("seq"), lax.axis_size("dp")
    width, hidden_units = expand_weight.shape
    return (
        hidden.shape[0] == 1
        and dp_parts == 2 * seq_parts
        and width % (16 * dp_parts) == 0
        and width % (16 * seq_parts) == 0
        and hidden_units % (128 * dp_parts) == 0
        and hidden.shape[1] % 128 == 0
    )


def solution(mesh):
    def either_way(*args):
        return (fast_device if fits(args[0], args[12]) else per_device)(*args)

    return jax.shard_map(
        either_way,
        mesh=mesh,
        in_specs=(
            P("dp", "seq", None),
            P("dp"),
            P(),
            P(),
            P(),
            P(),
            P(),
            P(),
            P(),
            P(),
            P(),
            P(),
            P(),
            P(),
            P(),
            P(),
            P("dp", "seq", None),
        ),
        out_specs=(
            P("dp", "seq", None),
            P("dp", "seq", None),
            P(),
            P(),
            P(),
            P(),
            P("dp", "seq"),
            P(),
            P("dp", "seq"),
            P(),
            P("dp", "seq"),
            P(),
            P("dp", "seq"),
            P(),
            P("dp", "seq"),
            P(),
        ),
        check_vma=False,
    )
```

```python
import functools

import jax
import jax.numpy as jnp
from jax import lax
from jax.experimental import pallas as pl
from jax.experimental.pallas import tpu as pltpu
from jax.sharding import PartitionSpec as P

HEADS = 12
HD = 64
ROT = 16
f32 = jnp.float32
bf16 = jnp.bfloat16


norm_eps = 1e-05
masked_score = -1e30


def layer_norm(values, gains, shifts):
    average = jnp.mean(values, axis=-1, keepdims=True)
    centered = values - average
    variance = jnp.mean(centered * centered, axis=-1, keepdims=True)
    return centered * lax.rsqrt(variance + norm_eps) * gains + shifts


def rotate(vectors, positions):
    half_rot = ROT // 2
    frequency = 10000.0 ** (-2.0 * jnp.arange(half_rot, dtype=jnp.float32) / ROT)
    angles = positions.astype(jnp.float32)[:, None] * frequency[None, :]
    cosine = jnp.cos(angles)
    sine_part = jnp.sin(angles)
    lead_part = vectors[..., :half_rot]
    pair_part = vectors[..., half_rot:ROT]
    rest_part = vectors[..., ROT:]
    return jnp.concatenate(
        [
            lead_part * cosine - pair_part * sine_part,
            pair_part * cosine + lead_part * sine_part,
            rest_part,
        ],
        axis=-1,
    )


def exact_gelu(values):
    return jax.nn.gelu(values, approximate=False)


def outer_sum(left, right):
    return lax.dot_general(
        left, right, (((0,), (0,)), ((), ())), preferred_element_type=jnp.float32
    )


def per_device(
    hidden_in,
    seq_lengths,
    attention_gain,
    attention_shift,
    feed_gain,
    feed_shift,
    query_weight,
    query_bias,
    keyval_weight,
    keyval_bias,
    dense_weight,
    dense_bias,
    expand_weight,
    expand_bias,
    project_weight,
    project_bias,
    out_grad,
):
    seq_count, stretch_len, model_width = hidden_in.shape
    seq_parts = lax.axis_size("seq")
    whole_len = stretch_len * seq_parts
    offset = lax.axis_index("seq") * stretch_len
    positions = offset + jnp.arange(stretch_len, dtype=jnp.int32)
    row_count = seq_count * stretch_len
    query_scale = HD ** (-0.5)
    inputs = hidden_in.astype(jnp.float32).reshape(row_count, model_width)
    valid_rows = positions[None, :] < seq_lengths[:, None]
    grad_out = jnp.where(valid_rows[:, :, None], out_grad, jnp.zeros_like(out_grad)).reshape(
        row_count, model_width
    )
    attn_norm, attn_norm_back = jax.vjp(layer_norm, inputs, attention_gain, attention_shift)
    feed_norm, feed_norm_back = jax.vjp(layer_norm, inputs, feed_gain, feed_shift)
    attn_in = attn_norm.astype(jnp.bfloat16)
    feed_in = feed_norm.astype(jnp.bfloat16)
    query_pre = jnp.dot(attn_in, query_weight, preferred_element_type=jnp.float32) + query_bias
    keyval_pre = jnp.dot(attn_in, keyval_weight, preferred_element_type=jnp.float32) + keyval_bias

    def turn_query(flat_query):
        shaped = flat_query.reshape(seq_count, stretch_len, HEADS, HD).transpose(0, 2, 1, 3)
        return rotate(shaped, positions) * query_scale

    def turn_keyval(flat_keyval):
        shaped = flat_keyval.reshape(seq_count, stretch_len, 2 * HD)
        return jnp.concatenate([rotate(shaped[..., :HD], positions), shaped[..., HD:]], axis=-1)

    query_rot, query_back = jax.vjp(turn_query, query_pre)
    keyval_rot, keyval_back = jax.vjp(turn_keyval, keyval_pre)
    query_low = query_rot.astype(jnp.bfloat16)
    keyval_low = keyval_rot.astype(jnp.bfloat16)
    gathered = lax.all_gather(keyval_low, "seq", axis=1, tiled=True)
    grad_mixed = jnp.dot(grad_out, dense_weight.T, preferred_element_type=jnp.float32).astype(
        jnp.bfloat16
    )
    grad_heads = grad_mixed.reshape(seq_count, stretch_len, HEADS, HD).transpose(0, 2, 1, 3)
    key_block = min(512, whole_len)
    block_count = whole_len // key_block
    group_size = 4

    def attend(operands):
        query_seq, grad_seq, keyval_seq, length = operands
        extent = block_count * key_block
        key_rows = keyval_seq[:extent, :HD]
        values = keyval_seq[:extent, HD:]
        key_pos = jnp.arange(extent, dtype=jnp.int32)
        allowed = (key_pos[None, :] <= positions[:, None]) & (key_pos[None, :] < length)

        def one_group(group_pair):
            query_grp, grad_grp = group_pair
            scores = jnp.einsum(
                "gtd,sd->gts", query_grp, key_rows, preferred_element_type=jnp.float32
            )
            scores = jnp.where(allowed[None], scores, masked_score)
            log_total = jax.nn.logsumexp(scores, axis=-1, keepdims=True)
            soft_weights = jnp.exp(scores - log_total)
            soft_low = soft_weights.astype(jnp.bfloat16)
            mixed_part = jnp.einsum(
                "gts,sd->gtd", soft_low, values, preferred_element_type=jnp.float32
            )
            grad_soft = jnp.einsum(
                "gtd,sd->gts", grad_grp, values, preferred_element_type=jnp.float32
            )
            row_delta = jnp.sum(soft_weights * grad_soft, axis=-1, keepdims=True)
            grad_scores = (soft_weights * (grad_soft - row_delta)).astype(jnp.bfloat16)
            grad_query = jnp.einsum(
                "gts,sd->gtd", grad_scores, key_rows, preferred_element_type=jnp.float32
            )
            grad_keys = jnp.einsum(
                "gts,gtd->sd", grad_scores, query_grp, preferred_element_type=jnp.float32
            )
            grad_values = jnp.einsum(
                "gts,gtd->sd", soft_low, grad_grp, preferred_element_type=jnp.float32
            )
            return (mixed_part, grad_query, jnp.concatenate([grad_keys, grad_values], axis=-1))

        grouped_query = query_seq.reshape(HEADS // group_size, group_size, stretch_len, HD)
        grouped_grad = grad_seq.reshape(HEADS // group_size, group_size, stretch_len, HD)
        mixed_part, grad_query, grad_keyval = lax.map(one_group, (grouped_query, grouped_grad))
        grad_keyval = jnp.sum(grad_keyval, axis=0)
        return (
            mixed_part.reshape(HEADS, stretch_len, HD),
            grad_query.reshape(HEADS, stretch_len, HD),
            grad_keyval,
        )

    mixed_all, grad_query_all, grad_keyval_all = lax.map(
        attend, (query_low, grad_heads, gathered, seq_lengths)
    )
    grad_keyval_own = lax.psum_scatter(grad_keyval_all, "seq", scatter_dimension=1, tiled=True)
    mixed_low = mixed_all.transpose(0, 2, 1, 3).reshape(row_count, model_width).astype(jnp.bfloat16)
    attn_out = jnp.dot(mixed_low, dense_weight, preferred_element_type=jnp.float32) + dense_bias
    upper = jnp.dot(feed_in, expand_weight, preferred_element_type=jnp.float32) + expand_bias
    active, active_back = jax.vjp(exact_gelu, upper)
    active_low = active.astype(jnp.bfloat16)
    feed_out = (
        jnp.dot(active_low, project_weight, preferred_element_type=jnp.float32) + project_bias
    )
    output = (
        (inputs + attn_out + feed_out)
        .astype(jnp.bfloat16)
        .reshape(seq_count, stretch_len, model_width)
    )
    grad_active = jnp.dot(grad_out, project_weight.T, preferred_element_type=jnp.float32)
    grad_upper = active_back(grad_active)[0].astype(jnp.bfloat16)
    grad_query_pre = query_back(grad_query_all)[0].astype(jnp.bfloat16)
    grad_keyval_pre = keyval_back(grad_keyval_own)[0].astype(jnp.bfloat16)
    grad_attn_in = jnp.dot(
        grad_query_pre, query_weight.T, preferred_element_type=jnp.float32
    ) + jnp.dot(grad_keyval_pre, keyval_weight.T, preferred_element_type=jnp.float32)
    grad_feed_in = jnp.dot(grad_upper, expand_weight.T, preferred_element_type=jnp.float32)
    attn_dx, attn_dgain, attn_dshift = attn_norm_back(grad_attn_in)
    feed_dx, feed_dgain, feed_dshift = feed_norm_back(grad_feed_in)
    input_grad = (grad_out.astype(jnp.float32) + attn_dx + feed_dx).reshape(
        seq_count, stretch_len, model_width
    )
    query_term = outer_sum(attn_in, grad_query_pre)
    keyval_term = outer_sum(attn_in, grad_keyval_pre)
    dense_term = outer_sum(mixed_low, grad_out)
    expand_term = outer_sum(feed_in, grad_upper)
    project_term = outer_sum(active_low, grad_out)
    row_sums = (
        lax.psum_scatter(query_term, "dp", scatter_dimension=0, tiled=True),
        lax.psum_scatter(keyval_term, "dp", scatter_dimension=0, tiled=True),
        lax.psum_scatter(dense_term, "dp", scatter_dimension=0, tiled=True),
        lax.psum_scatter(expand_term, "dp", scatter_dimension=0, tiled=True),
        lax.psum_scatter(project_term, "dp", scatter_dimension=0, tiled=True),
    )
    weight_grads = (
        lax.psum_scatter(row_sums[0], "seq", scatter_dimension=1, tiled=True),
        lax.psum_scatter(row_sums[1], "seq", scatter_dimension=1, tiled=True),
        lax.psum_scatter(row_sums[2], "seq", scatter_dimension=1, tiled=True),
        lax.psum_scatter(row_sums[3], "seq", scatter_dimension=1, tiled=True),
        lax.psum_scatter(row_sums[4], "seq", scatter_dimension=1, tiled=True),
    )
    out_total = jnp.sum(grad_out, axis=0, dtype=jnp.float32)
    small_sums = lax.psum(
        (
            attn_dgain,
            attn_dshift,
            feed_dgain,
            feed_dshift,
            jnp.sum(grad_query_pre, axis=0, dtype=jnp.float32),
            jnp.sum(grad_keyval_pre, axis=0, dtype=jnp.float32),
            out_total,
            jnp.sum(grad_upper, axis=0, dtype=jnp.float32),
        ),
        ("seq", "dp"),
    )
    return (
        output,
        input_grad,
        small_sums[0],
        small_sums[1],
        small_sums[2],
        small_sums[3],
        weight_grads[0],
        small_sums[4],
        weight_grads[1],
        small_sums[5],
        weight_grads[2],
        small_sums[6],
        weight_grads[3],
        small_sums[7],
        weight_grads[4],
        small_sums[6],
    )


NT_DIMS = (((1,), (1,)), ((), ()))
MESH_ID = pl.DeviceIdType.MESH
VMEM_BYTES = 67043328


def dot(left, right):
    return jnp.dot(left, right, preferred_element_type=f32)


def dot_nt(left, right):
    return lax.dot_general(left, right, NT_DIMS, preferred_element_type=f32)


def aligned(start, size, unit):
    return pl.ds(pl.multiple_of(start, unit), size)


class Place:
    def __init__(self, seq_parts, half):
        self.seq_parts, self.half = seq_parts, half
        self.seq = lax.axis_index("seq")
        self.dp = lax.axis_index("dp")
        self.core = lax.rem(self.dp, 2)
        self.line = lax.div(self.dp, 2)
        self.partner = {"dp": self.dp + 1 - 2 * self.core}

    def seq_at(self, hop):
        return lax.rem(self.seq + hop, self.seq_parts)

    def line_at(self, hop):
        return lax.rem(self.line + hop, self.half)

    def plane_peer(self, hop):
        return {"seq": self.seq_at(hop)}

    def line_peer(self, hop):
        return {"dp": self.line_at(hop) * 2 + self.core}


def remote(src, dst, send, recv, peer):
    return pltpu.make_async_remote_copy(
        src_ref=src, dst_ref=dst, send_sem=send, recv_sem=recv, device_id=peer,
        device_id_type=MESH_ID,
    )


class Reduction:
    def __init__(self, place, bufs, sems):
        self.at = place
        (self.ge, self.gp, self.ce, self.cp, self.pe, self.pp, self.te, self.tp, self.le,
         self.lp) = bufs
        (self.cs, self.cr, self.es, self.er, self.ps, self.pr, self.zs, self.zr) = sems

    def core_copies(self, step):
        at, slot = self.at, lax.rem(step, 2)
        return [
            remote(src.at[slot, 1 - at.core], dst.at[step], self.cs.at[step, i], self.cr.at[step, i],
                   at.partner)
            for i, (src, dst) in enumerate(((self.ge, self.ce), (self.gp, self.cp)))
        ]

    def core_start(self, step):
        for copy in self.core_copies(step):
            copy.start()

    def core_finish(self, step):
        at, slot = self.at, lax.rem(step, 2)
        for copy in self.core_copies(step):
            copy.wait()
        for src, dst in ((self.ge, self.ce), (self.gp, self.cp)):
            for i in range(dst.shape[1]):
                dst[step, i] = (src[slot, at.core, i].astype(f32) + dst[step, i].astype(f32)).astype(
                    bf16
                )

    def col_copy(self, step):
        return remote(self.ce.at[step], self.pe.at[step], self.es.at[step], self.er.at[step],
                      self.at.plane_peer(step + 1))

    def row_copy(self, step, hop):
        at, part = self.at, self.at.seq_at(step + 1)
        return remote(self.cp.at[step, at.seq_at(hop)], self.pp.at[part, hop - 1],
                      self.ps.at[step, hop - 1], self.pr.at[part, hop - 1], at.plane_peer(hop))

    def plane_start(self, step):
        @pl.when(step < self.at.seq_parts - 1)
        def _():
            self.col_copy(step).start()

        for hop in range(1, self.at.seq_parts):
            self.row_copy(step, hop).start()

    def col_finish(self):
        last = self.at.seq_parts - 1
        for step in range(last):
            self.col_copy(step).wait()
        for i in range(self.at.half):
            total = self.ce[last, i].astype(f32)
            for step in range(last):
                total = total + self.pe[step, i].astype(f32)
            self.te[i] = total.astype(bf16)

    def row_finish(self, step):
        at, part = self.at, self.at.seq_at(step + 1)
        total = self.cp[step, at.seq].astype(f32)
        for hop in range(1, at.seq_parts):
            self.row_copy(step, hop).wait()
            total = total + self.pp[part, hop - 1].astype(f32)
        self.tp[part] = total.astype(bf16)

    def line_copy(self, family, hop):
        at = self.at
        src, dst = ((self.te, self.le), (self.tp, self.lp))[family]
        return remote(src.at[at.line_at(hop)], dst.at[hop - 1], self.zs.at[family, hop - 1],
                      self.zr.at[family, hop - 1], at.line_peer(hop))

    def line_start(self, family):
        for hop in range(1, self.at.half):
            self.line_copy(family, hop).start()

    def line_finish(self, family):
        src, dst = ((self.te, self.le), (self.tp, self.lp))[family]
        total = src[self.at.line].astype(f32)
        for hop in range(1, self.at.half):
            self.line_copy(family, hop).wait()
            total = total + dst[hop - 1].astype(f32)
        return total


def reduction_scratch(seq_parts, half, col_block, row_block):
    dma = pltpu.SemaphoreType.DMA
    hops, legs = seq_parts - 1, half - 1
    bufs = [
        (2, 2, half) + col_block, (2, 2, seq_parts) + row_block,
        (seq_parts, half) + col_block, (seq_parts, seq_parts) + row_block,
        (hops, half) + col_block, (seq_parts, hops) + row_block,
        (half,) + col_block, (half,) + row_block,
        (legs,) + col_block, (legs,) + row_block,
    ]
    sems = [
        dma((seq_parts, 2)), dma((seq_parts, 2)), dma((hops,)), dma((hops,)),
        dma((seq_parts, hops)), dma((seq_parts, hops)), dma((2, legs)), dma((2, legs)),
    ]
    return [pltpu.VMEM(shape, bf16) for shape in bufs] + sems


class Small:
    def __init__(self, place, cbuf, pbuf, zbuf, sems):
        self.at, self.cbuf, self.pbuf, self.zbuf = place, cbuf, pbuf, zbuf
        self.cs, self.cr, self.ps, self.pr, self.zs, self.zr = sems

    def core_copy(self, src):
        return remote(src, self.cbuf, self.cs.at[0], self.cr.at[0], self.at.partner)

    def plane_copy(self, hop):
        at = self.at
        mine = self.pbuf.at[at.seq]
        return remote(mine, mine, self.ps.at[hop - 1], self.pr.at[hop - 1], at.plane_peer(hop))

    def plane_start(self, value):
        self.pbuf[self.at.seq] = value
        for hop in range(1, self.at.seq_parts):
            self.plane_copy(hop).start()

    def plane_finish(self):
        for hop in range(1, self.at.seq_parts):
            self.plane_copy(hop).wait()
        total = self.pbuf[0].astype(f32)
        for i in range(1, self.at.seq_parts):
            total = total + self.pbuf[i].astype(f32)
        return total

    def line_copy(self, hop, src=None):
        at = self.at
        mine = self.zbuf.at[at.line]
        return remote(mine if src is None else src, mine, self.zs.at[hop - 1], self.zr.at[hop - 1],
                      at.line_peer(hop))

    def line_sum(self):
        total = self.zbuf[0].astype(f32)
        for i in range(1, self.at.half):
            total = total + self.zbuf[i].astype(f32)
        return total


def layer_kernel(seq_parts, half, *refs):
    refs = list(refs)

    def take(count):
        taken, refs[:count] = refs[:count], []
        return taken

    (length_ref, cos_ref, sin_ref, again_ref, ashift_ref, fgain_ref, fshift_ref, qbias_ref,
     kvbias_ref, dbias_ref, ebias_ref, pbias_ref) = take(12)
    hid_hbm, og_hbm, wq_hbm, wkv_hbm, wd_hbm, we_hbm, wp_hbm = take(7)
    out_ref, dx_ref, eout_ref, pout_ref, qout_ref, dout_ref, kvout_ref, small_ref = take(8)
    (hid, go, wq, wkv, wd, we, wp, norm, rstd, feed, feed_t, go_t, attn_t, base, query_t, gm_t, mix_t,
     gq_t, kvt, kt, vt, kaug, kv, score, expo, qaug, pair, dkv, dkv_out, dkv_in, kvg, small_own,
     kvz) = take(33)
    load_sem, kv_send, kv_recv, dk_send, dk_recv = take(5)
    place = Place(seq_parts, half)
    feed_sum = Reduction(place, take(10), take(8))
    attn_sum = Reduction(place, take(10), take(8))
    vec_sum = Small(place, *take(3), take(6))
    kvw_sum = Small(place, *take(3), take(6))
    seq, core, line = place.seq, place.core, place.line
    stretch, width = hid.shape
    chunk = we.shape[2]
    col_rows = feed_sum.ge.shape[3]
    row_rows = feed_sum.gp.shape[3]
    row_cols = feed_sum.gp.shape[4]
    group = HEADS // seq_parts
    group_rows = group * HD
    half_rot = ROT // 2
    scale = HD ** (-0.5)

    def load(src, dst, index):
        return pltpu.make_async_copy(src, dst, load_sem.at[index])

    def load_chunk(step):
        slot = lax.rem(step, 2)
        start = place.seq_at(step + 1) * chunk
        return (
            load(we_hbm.at[:, aligned(start, chunk, 128)], we.at[slot], 5 + 2 * slot),
            load(wp_hbm.at[aligned(start, chunk, 16), :], wp.at[slot], 6 + 2 * slot),
        )

    loads = (load(hid_hbm, hid, 0), load(wkv_hbm, wkv, 1), load(wq_hbm, wq, 2), load(og_hbm, go, 3),
             load(wd_hbm, wd, 4))
    for copy in loads:
        copy.start()
    for copy in load_chunk(0):
        copy.start()

    barrier = pltpu.get_barrier_semaphore()
    pl.semaphore_signal(barrier, inc=1, device_id=place.partner, device_id_type=MESH_ID)
    for hop in range(1, seq_parts):
        pl.semaphore_signal(barrier, inc=1, device_id=place.plane_peer(hop), device_id_type=MESH_ID)
    for hop in range(1, half):
        pl.semaphore_signal(barrier, inc=1, device_id=place.line_peer(hop), device_id_type=MESH_ID)

    length = length_ref[0]
    loads[0].wait()
    values = hid[...].astype(f32)
    average = jnp.mean(values, axis=1, keepdims=True)
    centered = values - average
    inverse = lax.rsqrt(jnp.mean(centered * centered, axis=1, keepdims=True) + norm_eps)
    normed = centered * inverse
    norm[...] = normed
    rstd[...] = jnp.broadcast_to(inverse, rstd.shape)
    base[...] = values + (dbias_ref[...] + pbias_ref[...])
    attn_t[...] = (normed * again_ref[...] + ashift_ref[...]).astype(bf16).T
    low = (normed * fgain_ref[...] + fshift_ref[...]).astype(bf16)
    feed[...] = low
    feed_t[...] = low.T

    def turn(rows, direction):
        lead, pair_part = rows[0:half_rot, :], rows[half_rot:ROT, :]
        cosine, sine = cos_ref[...], sin_ref[...] * direction
        return jnp.concatenate(
            [lead * cosine - pair_part * sine, pair_part * cosine + lead * sine, rows[ROT:, :]], axis=0
        )

    loads[1].wait()
    own = lax.dot_general(wkv[...], attn_t[...], (((0,), (0,)), ((), ())),
                          preferred_element_type=f32) + kvbias_ref[...]
    kvt[0] = jnp.concatenate([turn(own[0:HD, :], 1.0), own[HD:, :]], axis=0).astype(bf16)

    def kv_copy(hop):
        return remote(kvt.at[0], kvt.at[seq_parts - hop], kv_send.at[hop - 1], kv_recv.at[hop - 1],
                      place.plane_peer(hop))

    pl.semaphore_wait(barrier, seq_parts + half - 1)
    loads[2].wait()
    wq_t = wq[...].T
    for hop in range(1, seq_parts):
        kv_copy(hop).start()
    for head in range(HEADS):
        span = slice(head * HD, (head + 1) * HD)
        rows = dot(wq_t[span, :], attn_t[...]) + qbias_ref[span, :]
        query_t[span, :] = (turn(rows, 1.0) * scale).astype(bf16)

    loads[3].wait()
    token = seq * stretch + lax.broadcasted_iota(jnp.int32, (stretch, 1), 0)
    masked = jnp.where(token < length, go[...].astype(f32), 0.0).astype(bf16)
    go[...] = masked
    go_t[...] = masked.T
    loads[4].wait()
    gm_t[...] = dot(wd[...], go_t[...]).astype(bf16)
    ones = jnp.ones((16, stretch), bf16)
    small_own[...] = jnp.zeros(small_own.shape, f32)
    parts = seq_parts
    small_own[parts + 2 : parts + 3, :] = dot(ones, go[...])[0:1, :]

    dx_ref[...] = jnp.zeros(dx_ref.shape, f32)

    def feed_step(step, carry):
        slot = lax.rem(step, 2)
        part = place.seq_at(step + 1)

        @pl.when(step + 1 < seq_parts)
        def _():
            for copy in load_chunk(step + 1):
                copy.start()

        for copy in load_chunk(step):
            copy.wait()
        upper = dot(feed[...], we[slot]) + ebias_ref[part]
        grad_active = dot_nt(go[...], wp[slot])
        share = 0.5 * (1.0 + lax.erf(upper * (0.5**0.5)))
        slope = share + upper * (jnp.exp(-0.5 * upper * upper) * 0.3989422804014327)
        active = (upper * share).astype(bf16)
        grad_upper = (grad_active * slope).astype(bf16)
        col_grad = dot(feed_t[...], grad_upper).astype(bf16)
        for i in range(2 * half):
            feed_sum.ge[slot, i % 2, i // 2] = col_grad[i * col_rows : (i + 1) * col_rows, :]
        row_grad = dot(go_t[...], active).astype(bf16)
        for c in range(2):
            for i in range(seq_parts):
                feed_sum.gp[slot, c, i] = row_grad[
                    i * row_rows : (i + 1) * row_rows, c * row_cols : (c + 1) * row_cols
                ]
        small_own[pl.ds(part, 1), :] = dot(ones, grad_upper)[0:1, :]

        @pl.when(step > 0)
        def _():
            feed_sum.core_finish(step - 1)

        base[...] += dot(active, wp[slot])
        dx_ref[...] += dot_nt(grad_upper, we[slot])

        @pl.when(step > 0)
        def _():
            feed_sum.plane_start(step - 1)

        feed_sum.core_start(step)
        return carry

    lax.fori_loop(0, seq_parts, feed_step, 0)
    grad_feed = dx_ref[...]
    small_own[parts : parts + 1, :] = jnp.sum(grad_feed * norm[...], axis=0, keepdims=True)
    small_own[parts + 1 : parts + 2, :] = jnp.sum(grad_feed, axis=0, keepdims=True)
    dx_ref[...] = grad_feed * fgain_ref[...]

    lane = lax.broadcasted_iota(jnp.int32, (16, stretch), 1)
    first = lax.broadcasted_iota(jnp.int32, (16, stretch), 0) == 0
    unit_row = jnp.where(first, 1.0, 0.0).astype(bf16)
    rest = jnp.zeros((HD - 16, stretch), bf16)
    for hop in range(1, seq_parts):
        kv_copy(hop).wait()
    for i in range(seq_parts):
        span = slice(i * stretch, (i + 1) * stretch)
        held = kvt[i]
        owner = place.seq_at(i)
        usable = (owner * stretch + lane < length) & (owner <= seq)
        fence = jnp.where(first & jnp.logical_not(usable), masked_score, 0.0).astype(bf16)
        kaug[span, :] = jnp.concatenate([held[0:HD, :], fence, rest], axis=0).T
        kv[span, :] = held.T
        kt[:, span] = held[0:HD, :]
        vt[0:HD, span] = held[HD:, :]
        vt[HD:, span] = unit_row
    qaug[HD : HD + 16, :] = unit_row
    qaug[HD + 16 :, :] = rest
    pair[...] = jnp.zeros(pair.shape, bf16)
    dkv[...] = jnp.zeros(dkv.shape, f32)
    key_pos = lax.broadcasted_iota(jnp.int32, (stretch, stretch), 0)
    query_pos = lax.broadcasted_iota(jnp.int32, (stretch, stretch), 1)

    def attend(head):
        rows = aligned(head * HD, HD, HD)
        query = query_t[rows, :]
        qaug[0:HD, :] = query
        top = None
        for i in range(seq_parts):
            span = slice(i * stretch, (i + 1) * stretch)
            block = dot(kaug[span, :], qaug[...])
            if i == 0:
                block = jnp.where(key_pos <= query_pos, block, masked_score)
            score[span, :] = block
            block_top = jnp.max(block, axis=0, keepdims=True)
            top = block_top if top is None else jnp.maximum(top, block_top)
        mixed = jnp.zeros((HD + 16, stretch), f32)
        for i in range(seq_parts):
            span = slice(i * stretch, (i + 1) * stretch)
            low = jnp.exp(score[span, :] - top).astype(bf16)
            expo[span, :] = low
            mixed = mixed + dot(vt[:, span], low)
        inverse = 1.0 / mixed[HD : HD + 1, :]
        mixed = mixed[0:HD, :] * inverse
        mix_t[rows, :] = mixed.astype(bf16)
        grad = (gm_t[rows, :].astype(f32) * inverse).astype(bf16)
        delta = jnp.sum(grad.astype(f32) * mixed, axis=0, keepdims=True)
        pair[0:HD, 0:stretch] = query
        pair[HD:, stretch:] = grad
        grad_query = jnp.zeros((HD, stretch), f32)
        for i in range(seq_parts):
            span = slice(i * stretch, (i + 1) * stretch)
            block = dot(kv[span, :], pair[:, stretch:])
            low = expo[span, :]
            grad_score = (low.astype(f32) * (block - delta)).astype(bf16)
            grad_query = grad_query + dot(kt[:, span], grad_score)
            dkv[span, :] += dot_nt(jnp.concatenate([grad_score, low], axis=1), pair[...])
        gq_t[rows, :] = (turn(grad_query, -1.0) * scale).astype(bf16)

    def group_grads(step):
        slot = lax.rem(step, 2)
        rows = aligned(place.seq_at(step + 1) * group_rows, group_rows, 16)
        col_grad = dot_nt(attn_t[...], gq_t[rows, :]).astype(bf16)
        each = col_grad.shape[0] // (2 * half)
        for i in range(2 * half):
            attn_sum.ge[slot, i % 2, i // 2] = col_grad[i * each : (i + 1) * each, :]
        mixed_rows = mix_t[rows, :]
        across = width // seq_parts
        for i in range(seq_parts):
            block = dot_nt(mixed_rows, go_t[i * across : (i + 1) * across, :]).astype(bf16)
            for c in range(2):
                attn_sum.gp[slot, c, i] = block[c * each : (c + 1) * each, :]

    def head_step(index, carry):
        step = lax.div(index, group)
        attend(place.seq_at(step + 1) * group + lax.rem(index, group))

        @pl.when(index == 0)
        def _():
            feed_sum.core_finish(seq_parts - 1)
            feed_sum.plane_start(seq_parts - 1)

        @pl.when((lax.rem(index, group) == 0) & (index > 0))
        def _():
            attn_sum.core_finish(step - 1)
            attn_sum.plane_start(step - 1)

        @pl.when(lax.rem(index, group) == group - 1)
        def _():
            group_grads(step)
            attn_sum.core_start(step)

        @pl.when(index == COL_EVENT)
        def _():
            feed_sum.col_finish()
            feed_sum.line_start(0)

        @pl.when(index == ROW_EVENT)
        def _():
            for i in range(seq_parts):
                feed_sum.row_finish(i)
            feed_sum.line_start(1)

        return carry

    lax.fori_loop(0, HEADS, head_step, 0)

    def dkv_copy(hop):
        return remote(dkv_out.at[hop - 1], dkv_in.at[hop - 1], dk_send.at[hop - 1],
                      dk_recv.at[hop - 1], place.plane_peer(hop))

    for hop in range(1, seq_parts):
        dkv_out[hop - 1] = dkv[hop * stretch : (hop + 1) * stretch, :].astype(bf16)
    for hop in range(1, seq_parts):
        dkv_copy(hop).start()
    out_ref[...] = (base[...] + dot(mix_t[...].T, wd[...])).astype(bf16)
    small_own[parts + 3 : parts + 4, :] = dot_nt(ones, gq_t[...])[0:1, :]
    grad_attn = dot_nt(gq_t[...].T, wq[...])
    attn_sum.core_finish(seq_parts - 1)
    attn_sum.plane_start(seq_parts - 1)
    total = dkv[0:stretch, :]
    for hop in range(1, seq_parts):
        dkv_copy(hop).wait()
        total = total + dkv_in[hop - 1].astype(f32)
    total_t = total.T
    gkv_t = jnp.concatenate([turn(total_t[0:HD, :], -1.0), total_t[HD:, :]], axis=0).astype(bf16)
    kv_grad = dot_nt(attn_t[...], gkv_t)
    each = kvg.shape[2]
    for i in range(2 * half):
        kvg[i % 2, i // 2] = kv_grad[i * each : (i + 1) * each, :].astype(bf16)
    kvw_sum.core_copy(kvg.at[1 - core]).start()
    grad_attn = grad_attn + dot_nt(gkv_t.T, wkv[...])
    small_own[parts + 4 : parts + 5, :] = jnp.sum(grad_attn * norm[...], axis=0, keepdims=True)
    small_own[parts + 5 : parts + 6, :] = jnp.sum(grad_attn, axis=0, keepdims=True)
    small_own[parts + 6 : parts + 7, 0 : 2 * HD] = dot_nt(ones, gkv_t)[0:1, :]
    vec_sum.core_copy(small_own).start()
    back = dx_ref[...] + grad_attn * again_ref[...]
    normed = norm[...]
    back_mean = jnp.mean(back, axis=1, keepdims=True)
    back_dot = jnp.mean(back * normed, axis=1, keepdims=True)
    kvw_sum.core_copy(kvg.at[1 - core]).wait()
    kvw_sum.plane_start((kvg[core].astype(f32) + kvw_sum.cbuf[...].astype(f32)).astype(bf16))
    vec_sum.core_copy(small_own).wait()
    vec_sum.plane_start(small_own[...] + vec_sum.cbuf[...])
    dx_ref[...] = go[...].astype(f32) + (back - back_mean - normed * back_dot) * rstd[:, 0:1]
    attn_sum.col_finish()
    attn_sum.line_start(0)
    for i in range(seq_parts):
        attn_sum.row_finish(i)
    attn_sum.line_start(1)
    eout_ref[...] = feed_sum.line_finish(0)
    pout_ref[...] = feed_sum.line_finish(1).T
    plane_kv = kvw_sum.plane_finish().astype(bf16)
    for i in range(half):
        kvz[i] = plane_kv[i]
    kvw_sum.zbuf[line] = kvz[line]
    for hop in range(1, half):
        kvw_sum.line_copy(hop, kvz.at[place.line_at(hop)]).start()
    vec_sum.zbuf[line] = vec_sum.plane_finish()
    for hop in range(1, half):
        vec_sum.line_copy(hop).start()
    qout_ref[...] = attn_sum.line_finish(0)
    dout_ref[...] = attn_sum.line_finish(1)
    for hop in range(1, half):
        kvw_sum.line_copy(hop, kvz.at[place.line_at(hop)]).wait()
        vec_sum.line_copy(hop).wait()
    summed = kvw_sum.line_sum()
    kv_cols = kvout_ref.shape[1]
    chosen = summed[:, 0:kv_cols]
    for i in range(1, seq_parts):
        chosen = jnp.where(seq == i, summed[:, i * kv_cols : (i + 1) * kv_cols], chosen)
    kvout_ref[...] = chosen
    small_ref[...] = vec_sum.line_sum()


COL_EVENT = 5
ROW_EVENT = 8


def small_scratch(seq_parts, half, block, line_block, dtype):
    dma = pltpu.SemaphoreType.DMA
    return [
        pltpu.VMEM(block, dtype), pltpu.VMEM((seq_parts,) + block, dtype),
        pltpu.VMEM((half,) + line_block, dtype), dma((1,)), dma((1,)), dma((seq_parts - 1,)),
        dma((seq_parts - 1,)), dma((half - 1,)), dma((half - 1,)),
    ]


def fast_device(
    hidden_in, seq_lengths, attention_gain, attention_shift, feed_gain, feed_shift, query_weight,
    query_bias, keyval_weight, keyval_bias, dense_weight, dense_bias, expand_weight, expand_bias,
    project_weight, project_bias, out_grad,
):
    _, stretch, width = hidden_in.shape
    seq_parts, dp_parts = lax.axis_size("seq"), lax.axis_size("dp")
    half = dp_parts // 2
    hidden_units = expand_weight.shape[1]
    chunk = hidden_units // seq_parts
    whole_len = stretch * seq_parts
    positions = lax.axis_index("seq") * stretch + jnp.arange(stretch, dtype=jnp.int32)
    half_rot = ROT // 2
    frequency = 10000.0 ** (-2.0 * jnp.arange(half_rot, dtype=f32) / ROT)
    angles = frequency[:, None] * positions.astype(f32)[None, :]
    rows, cols = width // dp_parts, width // seq_parts
    col_block, row_block = (rows, chunk), (cols, hidden_units // dp_parts)
    vec_rows = -(-(seq_parts + 7) // 8) * 8
    sd, dma = jax.ShapeDtypeStruct, pltpu.SemaphoreType.DMA

    def vm(shape, dtype=bf16):
        return pltpu.VMEM(shape, dtype)

    in_vmem, in_hbm = pl.BlockSpec(memory_space=pltpu.VMEM), pl.BlockSpec(memory_space=pl.ANY)
    outs = pl.pallas_call(
        functools.partial(layer_kernel, seq_parts, half),
        out_shape=(
            sd((stretch, width), bf16), sd((stretch, width), f32), sd(col_block, f32),
            sd(row_block[::-1], f32), sd((rows, cols), f32), sd((rows, cols), f32),
            sd((rows, 2 * HD // seq_parts), f32), sd((vec_rows, width), f32),
        ),
        in_specs=[pl.BlockSpec(memory_space=pltpu.SMEM)] + [in_vmem] * 11 + [in_hbm] * 7,
        out_specs=(in_vmem,) * 8,
        scratch_shapes=[
            vm((stretch, width)), vm((stretch, width)), vm((width, width)), vm((width, 2 * HD)),
            vm((width, width)), vm((2, width, chunk)), vm((2, chunk, width)),
            vm((stretch, width), f32), vm((stretch, 128), f32), vm((stretch, width)),
            vm((width, stretch)), vm((width, stretch)), vm((width, stretch)),
            vm((stretch, width), f32), vm((width, stretch)), vm((width, stretch)),
            vm((width, stretch)), vm((width, stretch)), vm((seq_parts, 2 * HD, stretch)),
            vm((HD, whole_len)), vm((HD + 16, whole_len)), vm((whole_len, 2 * HD)),
            vm((whole_len, 2 * HD)), vm((whole_len, stretch), f32), vm((whole_len, stretch)),
            vm((2 * HD, stretch)), vm((2 * HD, 2 * stretch)), vm((whole_len, 2 * HD), f32),
            vm((seq_parts - 1, stretch, 2 * HD)), vm((seq_parts - 1, stretch, 2 * HD)),
            vm((2, half, rows, 2 * HD)), vm((vec_rows, width), f32), vm((half, rows, 2 * HD)),
            dma((9,)), dma((seq_parts - 1,)), dma((seq_parts - 1,)), dma((seq_parts - 1,)),
            dma((seq_parts - 1,)),
        ]
        + reduction_scratch(seq_parts, half, col_block, row_block)
        + reduction_scratch(seq_parts, half, (rows, cols), (rows, cols))
        + small_scratch(seq_parts, half, (vec_rows, width), (vec_rows, width), f32)
        + small_scratch(seq_parts, half, (half, rows, 2 * HD), (rows, 2 * HD), bf16),
        compiler_params=pltpu.CompilerParams(
            collective_id=0, has_side_effects=True, vmem_limit_bytes=VMEM_BYTES
        ),
    )(
        seq_lengths, jnp.cos(angles), jnp.sin(angles), attention_gain[None], attention_shift[None],
        feed_gain[None], feed_shift[None], query_bias[:, None], keyval_bias[:, None], dense_bias[None],
        expand_bias.reshape(seq_parts, 1, chunk), project_bias[None], hidden_in[0], out_grad[0],
        query_weight, keyval_weight, dense_weight, expand_weight, project_weight,
    )
    output, input_grad, expand_grad, project_grad, query_grad, dense_grad, keyval_grad, small = outs
    n = seq_parts
    return (
        output[None], input_grad[None], small[n + 4], small[n + 5], small[n], small[n + 1], query_grad,
        small[n + 3], keyval_grad, small[n + 6, : 2 * HD], dense_grad, small[n + 2], expand_grad,
        small[:n].reshape(hidden_units), project_grad, small[n + 2],
    )


def fits(hidden, expand_weight):
    seq_parts, dp_parts = lax.axis_size("seq"), lax.axis_size("dp")
    width, hidden_units = expand_weight.shape
    return (
        hidden.shape[0] == 1
        and dp_parts == 2 * seq_parts
        and HEADS % seq_parts == 0
        and hidden_units == seq_parts * width
        and width % (16 * dp_parts) == 0
        and width % (16 * seq_parts) == 0
        and hidden_units % (128 * dp_parts) == 0
        and hidden.shape[1] % 128 == 0
    )


def solution(mesh):
    def either_way(*args):
        return (fast_device if fits(args[0], args[12]) else per_device)(*args)

    return jax.shard_map(
        either_way,
        mesh=mesh,
        in_specs=(
            P("dp", "seq", None),
            P("dp"),
            P(),
            P(),
            P(),
            P(),
            P(),
            P(),
            P(),
            P(),
            P(),
            P(),
            P(),
            P(),
            P(),
            P(),
            P("dp", "seq", None),
        ),
        out_specs=(
            P("dp", "seq", None),
            P("dp", "seq", None),
            P(),
            P(),
            P(),
            P(),
            P("dp", "seq"),
            P(),
            P("dp", "seq"),
            P(),
            P("dp", "seq"),
            P(),
            P("dp", "seq"),
            P(),
            P("dp", "seq"),
            P(),
        ),
        check_vma=False,
    )
```

```python
import functools

import jax
import jax.numpy as jnp
from jax import lax
from jax.experimental import pallas as pl
from jax.experimental.pallas import tpu as pltpu
from jax.sharding import PartitionSpec as P

HEADS = 12
HD = 64
ROT = 16
f32 = jnp.float32
bf16 = jnp.bfloat16


norm_eps = 1e-05
masked_score = -1e30


def layer_norm(values, gains, shifts):
    average = jnp.mean(values, axis=-1, keepdims=True)
    centered = values - average
    variance = jnp.mean(centered * centered, axis=-1, keepdims=True)
    return centered * lax.rsqrt(variance + norm_eps) * gains + shifts


def rotate(vectors, positions):
    half_rot = ROT // 2
    frequency = 10000.0 ** (-2.0 * jnp.arange(half_rot, dtype=jnp.float32) / ROT)
    angles = positions.astype(jnp.float32)[:, None] * frequency[None, :]
    cosine = jnp.cos(angles)
    sine_part = jnp.sin(angles)
    lead_part = vectors[..., :half_rot]
    pair_part = vectors[..., half_rot:ROT]
    rest_part = vectors[..., ROT:]
    return jnp.concatenate(
        [
            lead_part * cosine - pair_part * sine_part,
            pair_part * cosine + lead_part * sine_part,
            rest_part,
        ],
        axis=-1,
    )


def exact_gelu(values):
    return jax.nn.gelu(values, approximate=False)


def outer_sum(left, right):
    return lax.dot_general(
        left, right, (((0,), (0,)), ((), ())), preferred_element_type=jnp.float32
    )


def per_device(
    hidden_in,
    seq_lengths,
    attention_gain,
    attention_shift,
    feed_gain,
    feed_shift,
    query_weight,
    query_bias,
    keyval_weight,
    keyval_bias,
    dense_weight,
    dense_bias,
    expand_weight,
    expand_bias,
    project_weight,
    project_bias,
    out_grad,
):
    seq_count, stretch_len, model_width = hidden_in.shape
    seq_parts = lax.axis_size("seq")
    whole_len = stretch_len * seq_parts
    offset = lax.axis_index("seq") * stretch_len
    positions = offset + jnp.arange(stretch_len, dtype=jnp.int32)
    row_count = seq_count * stretch_len
    query_scale = HD ** (-0.5)
    inputs = hidden_in.astype(jnp.float32).reshape(row_count, model_width)
    valid_rows = positions[None, :] < seq_lengths[:, None]
    grad_out = jnp.where(valid_rows[:, :, None], out_grad, jnp.zeros_like(out_grad)).reshape(
        row_count, model_width
    )
    attn_norm, attn_norm_back = jax.vjp(layer_norm, inputs, attention_gain, attention_shift)
    feed_norm, feed_norm_back = jax.vjp(layer_norm, inputs, feed_gain, feed_shift)
    attn_in = attn_norm.astype(jnp.bfloat16)
    feed_in = feed_norm.astype(jnp.bfloat16)
    query_pre = jnp.dot(attn_in, query_weight, preferred_element_type=jnp.float32) + query_bias
    keyval_pre = jnp.dot(attn_in, keyval_weight, preferred_element_type=jnp.float32) + keyval_bias

    def turn_query(flat_query):
        shaped = flat_query.reshape(seq_count, stretch_len, HEADS, HD).transpose(0, 2, 1, 3)
        return rotate(shaped, positions) * query_scale

    def turn_keyval(flat_keyval):
        shaped = flat_keyval.reshape(seq_count, stretch_len, 2 * HD)
        return jnp.concatenate([rotate(shaped[..., :HD], positions), shaped[..., HD:]], axis=-1)

    query_rot, query_back = jax.vjp(turn_query, query_pre)
    keyval_rot, keyval_back = jax.vjp(turn_keyval, keyval_pre)
    query_low = query_rot.astype(jnp.bfloat16)
    keyval_low = keyval_rot.astype(jnp.bfloat16)
    gathered = lax.all_gather(keyval_low, "seq", axis=1, tiled=True)
    grad_mixed = jnp.dot(grad_out, dense_weight.T, preferred_element_type=jnp.float32).astype(
        jnp.bfloat16
    )
    grad_heads = grad_mixed.reshape(seq_count, stretch_len, HEADS, HD).transpose(0, 2, 1, 3)
    key_block = min(512, whole_len)
    block_count = whole_len // key_block
    group_size = 4

    def attend(operands):
        query_seq, grad_seq, keyval_seq, length = operands
        extent = block_count * key_block
        key_rows = keyval_seq[:extent, :HD]
        values = keyval_seq[:extent, HD:]
        key_pos = jnp.arange(extent, dtype=jnp.int32)
        allowed = (key_pos[None, :] <= positions[:, None]) & (key_pos[None, :] < length)

        def one_group(group_pair):
            query_grp, grad_grp = group_pair
            scores = jnp.einsum(
                "gtd,sd->gts", query_grp, key_rows, preferred_element_type=jnp.float32
            )
            scores = jnp.where(allowed[None], scores, masked_score)
            log_total = jax.nn.logsumexp(scores, axis=-1, keepdims=True)
            soft_weights = jnp.exp(scores - log_total)
            soft_low = soft_weights.astype(jnp.bfloat16)
            mixed_part = jnp.einsum(
                "gts,sd->gtd", soft_low, values, preferred_element_type=jnp.float32
            )
            grad_soft = jnp.einsum(
                "gtd,sd->gts", grad_grp, values, preferred_element_type=jnp.float32
            )
            row_delta = jnp.sum(soft_weights * grad_soft, axis=-1, keepdims=True)
            grad_scores = (soft_weights * (grad_soft - row_delta)).astype(jnp.bfloat16)
            grad_query = jnp.einsum(
                "gts,sd->gtd", grad_scores, key_rows, preferred_element_type=jnp.float32
            )
            grad_keys = jnp.einsum(
                "gts,gtd->sd", grad_scores, query_grp, preferred_element_type=jnp.float32
            )
            grad_values = jnp.einsum(
                "gts,gtd->sd", soft_low, grad_grp, preferred_element_type=jnp.float32
            )
            return (mixed_part, grad_query, jnp.concatenate([grad_keys, grad_values], axis=-1))

        grouped_query = query_seq.reshape(HEADS // group_size, group_size, stretch_len, HD)
        grouped_grad = grad_seq.reshape(HEADS // group_size, group_size, stretch_len, HD)
        mixed_part, grad_query, grad_keyval = lax.map(one_group, (grouped_query, grouped_grad))
        grad_keyval = jnp.sum(grad_keyval, axis=0)
        return (
            mixed_part.reshape(HEADS, stretch_len, HD),
            grad_query.reshape(HEADS, stretch_len, HD),
            grad_keyval,
        )

    mixed_all, grad_query_all, grad_keyval_all = lax.map(
        attend, (query_low, grad_heads, gathered, seq_lengths)
    )
    grad_keyval_own = lax.psum_scatter(grad_keyval_all, "seq", scatter_dimension=1, tiled=True)
    mixed_low = mixed_all.transpose(0, 2, 1, 3).reshape(row_count, model_width).astype(jnp.bfloat16)
    attn_out = jnp.dot(mixed_low, dense_weight, preferred_element_type=jnp.float32) + dense_bias
    upper = jnp.dot(feed_in, expand_weight, preferred_element_type=jnp.float32) + expand_bias
    active, active_back = jax.vjp(exact_gelu, upper)
    active_low = active.astype(jnp.bfloat16)
    feed_out = (
        jnp.dot(active_low, project_weight, preferred_element_type=jnp.float32) + project_bias
    )
    output = (
        (inputs + attn_out + feed_out)
        .astype(jnp.bfloat16)
        .reshape(seq_count, stretch_len, model_width)
    )
    grad_active = jnp.dot(grad_out, project_weight.T, preferred_element_type=jnp.float32)
    grad_upper = active_back(grad_active)[0].astype(jnp.bfloat16)
    grad_query_pre = query_back(grad_query_all)[0].astype(jnp.bfloat16)
    grad_keyval_pre = keyval_back(grad_keyval_own)[0].astype(jnp.bfloat16)
    grad_attn_in = jnp.dot(
        grad_query_pre, query_weight.T, preferred_element_type=jnp.float32
    ) + jnp.dot(grad_keyval_pre, keyval_weight.T, preferred_element_type=jnp.float32)
    grad_feed_in = jnp.dot(grad_upper, expand_weight.T, preferred_element_type=jnp.float32)
    attn_dx, attn_dgain, attn_dshift = attn_norm_back(grad_attn_in)
    feed_dx, feed_dgain, feed_dshift = feed_norm_back(grad_feed_in)
    input_grad = (grad_out.astype(jnp.float32) + attn_dx + feed_dx).reshape(
        seq_count, stretch_len, model_width
    )
    query_term = outer_sum(attn_in, grad_query_pre)
    keyval_term = outer_sum(attn_in, grad_keyval_pre)
    dense_term = outer_sum(mixed_low, grad_out)
    expand_term = outer_sum(feed_in, grad_upper)
    project_term = outer_sum(active_low, grad_out)
    row_sums = (
        lax.psum_scatter(query_term, "dp", scatter_dimension=0, tiled=True),
        lax.psum_scatter(keyval_term, "dp", scatter_dimension=0, tiled=True),
        lax.psum_scatter(dense_term, "dp", scatter_dimension=0, tiled=True),
        lax.psum_scatter(expand_term, "dp", scatter_dimension=0, tiled=True),
        lax.psum_scatter(project_term, "dp", scatter_dimension=0, tiled=True),
    )
    weight_grads = (
        lax.psum_scatter(row_sums[0], "seq", scatter_dimension=1, tiled=True),
        lax.psum_scatter(row_sums[1], "seq", scatter_dimension=1, tiled=True),
        lax.psum_scatter(row_sums[2], "seq", scatter_dimension=1, tiled=True),
        lax.psum_scatter(row_sums[3], "seq", scatter_dimension=1, tiled=True),
        lax.psum_scatter(row_sums[4], "seq", scatter_dimension=1, tiled=True),
    )
    out_total = jnp.sum(grad_out, axis=0, dtype=jnp.float32)
    small_sums = lax.psum(
        (
            attn_dgain,
            attn_dshift,
            feed_dgain,
            feed_dshift,
            jnp.sum(grad_query_pre, axis=0, dtype=jnp.float32),
            jnp.sum(grad_keyval_pre, axis=0, dtype=jnp.float32),
            out_total,
            jnp.sum(grad_upper, axis=0, dtype=jnp.float32),
        ),
        ("seq", "dp"),
    )
    return (
        output,
        input_grad,
        small_sums[0],
        small_sums[1],
        small_sums[2],
        small_sums[3],
        weight_grads[0],
        small_sums[4],
        weight_grads[1],
        small_sums[5],
        weight_grads[2],
        small_sums[6],
        weight_grads[3],
        small_sums[7],
        weight_grads[4],
        small_sums[6],
    )


NT_DIMS = (((1,), (1,)), ((), ()))
MESH_ID = pl.DeviceIdType.MESH
VMEM_BYTES = 67043328


def dot(left, right):
    return jnp.dot(left, right, preferred_element_type=f32)


def dot_nt(left, right):
    return lax.dot_general(left, right, NT_DIMS, preferred_element_type=f32)


def aligned(start, size, unit):
    return pl.ds(pl.multiple_of(start, unit), size)


class Place:
    def __init__(self, seq_parts, half):
        self.seq_parts, self.half = seq_parts, half
        self.seq = lax.axis_index("seq")
        self.dp = lax.axis_index("dp")
        self.core = lax.rem(self.dp, 2)
        self.line = lax.div(self.dp, 2)
        self.partner = {"dp": self.dp + 1 - 2 * self.core}

    def seq_at(self, hop):
        return lax.rem(self.seq + hop, self.seq_parts)

    def line_at(self, hop):
        return lax.rem(self.line + hop, self.half)

    def flip(self, mask):
        return {"seq": self.swapped(mask)}

    def swapped(self, mask):
        low, high = lax.rem(self.seq, 2), lax.div(self.seq, 2)
        low = lax.rem(low + lax.rem(mask, 2), 2)
        return low + 2 * lax.rem(high + lax.div(mask, 2), 2)

    def plane_peer(self, hop):
        return {"seq": self.seq_at(hop)}

    def line_peer(self, hop):
        return {"dp": self.line_at(hop) * 2 + self.core}


def remote(src, dst, send, recv, peer):
    return pltpu.make_async_remote_copy(
        src_ref=src, dst_ref=dst, send_sem=send, recv_sem=recv, device_id=peer,
        device_id_type=MESH_ID,
    )


class Reduction:
    def __init__(self, place, bufs, sems):
        self.at = place
        self.ge, self.gp, self.ce, self.cp, self.pe, self.pp, self.sums, self.landed = bufs
        (self.cs, self.cr, self.es, self.er, self.ps, self.pr, self.zs, self.zr) = sems

    def core_copies(self, step):
        at, slot = self.at, lax.rem(step, 2)
        return [
            remote(src.at[slot, 1 - at.core], dst.at[step], self.cs.at[step, i], self.cr.at[step, i],
                   at.partner)
            for i, (src, dst) in enumerate(((self.ge, self.ce), (self.gp, self.cp)))
        ]

    def core_start(self, step):
        for copy in self.core_copies(step):
            copy.start()

    def core_finish(self, step):
        at, slot = self.at, lax.rem(step, 2)
        for copy in self.core_copies(step):
            copy.wait()
        for src, dst in ((self.ge, self.ce), (self.gp, self.cp)):
            for i in range(dst.shape[1]):
                dst[step, i] = (src[slot, at.core, i].astype(f32) + dst[step, i].astype(f32)).astype(
                    bf16
                )

    def col_copy(self, step):
        return remote(self.ce.at[step], self.pe.at[step], self.es.at[step], self.er.at[step],
                      self.at.plane_peer(step + 1))

    def row_copy(self, step, hop):
        at, part = self.at, self.at.seq_at(step + 1)
        return remote(self.cp.at[step, at.seq_at(hop)], self.pp.at[part, hop - 1],
                      self.ps.at[step, hop - 1], self.pr.at[part, hop - 1], at.plane_peer(hop))

    def plane_start(self, step):
        @pl.when(step < self.at.seq_parts - 1)
        def _():
            self.col_copy(step).start()

        for hop in range(1, self.at.seq_parts):
            self.row_copy(step, hop).start()

    def sum_finish(self):
        at, last = self.at, self.at.seq_parts - 1
        for step in range(last):
            self.col_copy(step).wait()
        for step in range(at.seq_parts):
            for hop in range(1, at.seq_parts):
                self.row_copy(step, hop).wait()
        split = self.ce.shape[-1]
        for i in range(at.half):
            total = self.ce[last, i].astype(f32)
            for step in range(last):
                total = total + self.pe[step, i].astype(f32)
            self.sums[i, :, 0:split] = total.astype(bf16)
        for step in range(at.seq_parts):
            part = at.seq_at(step + 1)
            total = self.cp[step, at.seq].astype(f32)
            for hop in range(1, at.seq_parts):
                total = total + self.pp[part, hop - 1].astype(f32)
            self.sums[part, :, split:] = total.astype(bf16)

    def line_copy(self, hop):
        at = self.at
        return remote(self.sums.at[at.line_at(hop)], self.landed.at[hop - 1], self.zs.at[hop - 1],
                      self.zr.at[hop - 1], at.line_peer(hop))

    def line_start(self):
        for hop in range(1, self.at.half):
            self.line_copy(hop).start()

    def line_finish(self):
        total = self.sums[self.at.line].astype(f32)
        for hop in range(1, self.at.half):
            self.line_copy(hop).wait()
            total = total + self.landed[hop - 1].astype(f32)
        return total


def reduction_scratch(seq_parts, half, col_block, row_block):
    dma = pltpu.SemaphoreType.DMA
    hops, legs = seq_parts - 1, half - 1
    bufs = [
        (2, 2, half) + col_block, (2, 2, seq_parts) + row_block,
        (seq_parts, half) + col_block, (seq_parts, seq_parts) + row_block,
        (hops, half) + col_block, (seq_parts, hops) + row_block,
        (half, col_block[0], col_block[1] + row_block[1]),
        (legs, col_block[0], col_block[1] + row_block[1]),
    ]
    sems = [
        dma((seq_parts, 2)), dma((seq_parts, 2)), dma((hops,)), dma((hops,)),
        dma((seq_parts, hops)), dma((seq_parts, hops)), dma((legs,)), dma((legs,)),
    ]
    return [pltpu.VMEM(shape, bf16) for shape in bufs] + sems


class TreeSum:
    def __init__(self, place, bufs, sems):
        self.at = place
        self.made, self.core, self.via, self.side, self.sums, self.landed = bufs
        self.cs, self.cr, self.vs, self.vr, self.ss, self.sr, self.zs, self.zr = sems
        self.half = self.at.half // 2

    def core_copy(self, step):
        at, slot = self.at, lax.rem(step, 2)
        return remote(self.made.at[slot, 1 - at.core], self.core.at[step], self.cs.at[step],
                      self.cr.at[step], at.partner)

    def core_finish(self, step):
        at, slot = self.at, lax.rem(step, 2)
        self.core_copy(step).wait()
        for i in range(at.half):
            self.core[step, i] = (
                self.made[slot, at.core, i].astype(f32) + self.core[step, i].astype(f32)
            ).astype(bf16)

    def via_copy(self, side):
        span = pl.ds(side * self.half, self.half)
        return remote(self.core.at[0, span], self.via.at[side], self.vs.at[side], self.vr.at[side],
                      self.at.flip(1 + side))

    def via_start(self):
        for side in range(2):
            self.via_copy(side).start()

    def side_copy(self, side):
        return remote(self.core.at[1 + side], self.side.at[side], self.ss.at[side],
                      self.sr.at[side], self.at.flip(2 - side))

    def side_start(self):
        for side in range(2):
            self.via_copy(side).wait()
            for i in range(self.half):
                j = side * self.half + i
                self.core[1 + side, j] = (
                    self.core[1 + side, j].astype(f32) + self.via[side, i].astype(f32)
                ).astype(bf16)
        for side in range(2):
            self.side_copy(side).start()

    def side_finish(self):
        for side in range(2):
            self.side_copy(side).wait()
        for i in range(self.at.half):
            self.sums[i] = (
                self.core[3, i].astype(f32) + self.side[0, i].astype(f32) + self.side[1, i].astype(f32)
            ).astype(bf16)

    def line_copy(self, hop):
        at = self.at
        return remote(self.sums.at[at.line_at(hop)], self.landed.at[hop - 1], self.zs.at[hop - 1],
                      self.zr.at[hop - 1], at.line_peer(hop))

    def line_start(self):
        for hop in range(1, self.at.half):
            self.line_copy(hop).start()

    def line_finish(self):
        total = self.sums[self.at.line].astype(f32)
        for hop in range(1, self.at.half):
            self.line_copy(hop).wait()
            total = total + self.landed[hop - 1].astype(f32)
        return total


def tree_scratch(half, block):
    dma = pltpu.SemaphoreType.DMA
    bufs = [
        (2, 2, half) + block, (4, half) + block, (2, half // 2) + block, (2, half) + block,
        (half,) + block, (half - 1,) + block,
    ]
    return [pltpu.VMEM(shape, bf16) for shape in bufs] + [
        dma((4,)), dma((4,)), dma((2,)), dma((2,)), dma((2,)), dma((2,)), dma((half - 1,)),
        dma((half - 1,)),
    ]


class Small:
    def __init__(self, place, own, cbuf, pbuf, zbuf, sems):
        self.at, self.own, self.cbuf, self.pbuf, self.zbuf = place, own, cbuf, pbuf, zbuf
        self.cs, self.cr, self.ps, self.pr, self.zs, self.zr = sems

    def core_copy(self):
        return remote(self.own, self.cbuf, self.cs.at[0], self.cr.at[0], self.at.partner)

    def plane_copy(self, hop):
        at = self.at
        mine = self.pbuf.at[at.seq]
        return remote(mine, mine, self.ps.at[hop - 1], self.pr.at[hop - 1], at.plane_peer(hop))

    def plane_start(self):
        self.core_copy().wait()
        self.pbuf[self.at.seq] = self.own[...] + self.cbuf[...]
        for hop in range(1, self.at.seq_parts):
            self.plane_copy(hop).start()

    def plane_finish(self):
        for hop in range(1, self.at.seq_parts):
            self.plane_copy(hop).wait()
        total = self.pbuf[0].astype(f32)
        for i in range(1, self.at.seq_parts):
            total = total + self.pbuf[i].astype(f32)
        return total

    def line_copy(self, hop):
        at = self.at
        mine = self.zbuf.at[at.line]
        return remote(mine, mine, self.zs.at[hop - 1], self.zr.at[hop - 1], at.line_peer(hop))

    def line_start(self):
        self.zbuf[self.at.line] = self.plane_finish()
        for hop in range(1, self.at.half):
            self.line_copy(hop).start()

    def line_sum(self):
        for hop in range(1, self.at.half):
            self.line_copy(hop).wait()
        total = self.zbuf[0].astype(f32)
        for i in range(1, self.at.half):
            total = total + self.zbuf[i].astype(f32)
        return total


class KeyvalSum:
    def __init__(self, place, bufs, sems):
        self.at = place
        self.made, self.core, self.side, self.sums, self.landed = bufs
        self.cs, self.cr, self.ps, self.pr, self.zs, self.zr = sems

    def core_copy(self):
        return remote(self.made.at[1 - self.at.core], self.core, self.cs.at[0], self.cr.at[0],
                      self.at.partner)

    def plane_copy(self, hop):
        return remote(self.core.at[self.at.seq_at(hop)], self.side.at[hop - 1], self.ps.at[hop - 1],
                      self.pr.at[hop - 1], self.at.plane_peer(hop))

    def core_finish(self):
        self.core_copy().wait()
        self.core[...] = (
            self.made[self.at.core].astype(f32) + self.core[...].astype(f32)
        ).astype(bf16)

    def plane_start(self):
        for hop in range(1, self.at.seq_parts):
            self.plane_copy(hop).start()

    def plane_finish(self):
        total = self.core[self.at.seq].astype(f32)
        for hop in range(1, self.at.seq_parts):
            self.plane_copy(hop).wait()
            total = total + self.side[hop - 1].astype(f32)
        self.sums[...] = total.astype(bf16)

    def line_copy(self, hop):
        at = self.at
        return remote(self.sums.at[at.line_at(hop)], self.landed.at[hop - 1], self.zs.at[hop - 1],
                      self.zr.at[hop - 1], at.line_peer(hop))

    def line_start(self):
        for hop in range(1, self.at.half):
            self.line_copy(hop).start()

    def line_finish(self):
        total = self.sums[self.at.line].astype(f32)
        for hop in range(1, self.at.half):
            self.line_copy(hop).wait()
            total = total + self.landed[hop - 1].astype(f32)
        return total


def keyval_scratch(seq_parts, half, block):
    dma = pltpu.SemaphoreType.DMA
    bufs = [
        (2, seq_parts, half) + block, (seq_parts, half) + block, (seq_parts - 1, half) + block,
        (half,) + block, (half - 1,) + block,
    ]
    return [pltpu.VMEM(shape, bf16) for shape in bufs] + [
        dma((1,)), dma((1,)), dma((seq_parts - 1,)), dma((seq_parts - 1,)), dma((half - 1,)),
        dma((half - 1,)),
    ]


def layer_kernel(seq_parts, half, *refs):
    refs = list(refs)

    def take(count):
        taken, refs[:count] = refs[:count], []
        return taken

    (length_ref, again_ref, ashift_ref, fgain_ref, fshift_ref, qbias_ref, kvbias_ref, dbias_ref,
     ebias_ref, pbias_ref) = take(10)
    hid_hbm, og_hbm, wq_hbm, wkv_hbm, wd_hbm, we_hbm, wp_hbm = take(7)
    out_hbm, dx_hbm, eout_hbm, pout_hbm, qd_ref, kvout_ref, feed_small_ref, attn_small_ref = take(8)
    (hid, go, wq, wkv, wd, we, wp, norm, rstd, feed, feed_t, go_t, attn_t, base, query_t, gm_t, mix_t,
     gq_t, active_all, kvt, kt, vt, kaug, kv, score, expo, qaug, pair, dkv, dkv_out, dkv_in, ebias,
     turns, dx, eout, pout) = take(36)
    load_sem, store_sem, kv_send, kv_recv, dk_send, dk_recv = take(6)
    place = Place(seq_parts, half)
    expand_sum = TreeSum(place, take(6), take(8))
    project_sum = TreeSum(place, take(6), take(8))
    attn_sum = Reduction(place, take(8), take(8))
    feed_small = Small(place, *take(4), take(6))
    attn_small = Small(place, *take(4), take(6))
    keyval_sum = KeyvalSum(place, take(5), take(6))
    seq = place.seq
    stretch, width = hid.shape
    chunk = we.shape[2]
    col_rows = expand_sum.made.shape[3]
    row_rows, row_cols = project_sum.made.shape[3:]
    group = HEADS // seq_parts
    group_rows = group * HD
    half_rot = ROT // 2
    scale = HD ** (-0.5)

    def load(src, dst, index):
        return pltpu.make_async_copy(src, dst, load_sem.at[index])

    def load_chunk(step):
        slot = lax.rem(step, 2)
        start = place.swapped(3 - step) * chunk
        return (
            load(we_hbm.at[:, aligned(start, chunk, 128)], we.at[slot], 5 + 2 * slot),
            load(wp_hbm.at[aligned(start, chunk, 16), :], wp.at[slot], 6 + 2 * slot),
        )

    loads = (load(hid_hbm.at[0], hid, 0), load(wkv_hbm, wkv, 1), load(wq_hbm, wq, 2), load(og_hbm.at[0], go, 3),
             load(wd_hbm, wd, 4))
    for copy in loads:
        copy.start()
    for copy in load_chunk(0):
        copy.start()

    barrier = pltpu.get_barrier_semaphore()
    pl.semaphore_signal(barrier, inc=1, device_id=place.partner, device_id_type=MESH_ID)
    for hop in range(1, seq_parts):
        pl.semaphore_signal(barrier, inc=1, device_id=place.plane_peer(hop), device_id_type=MESH_ID)
    for hop in range(1, half):
        pl.semaphore_signal(barrier, inc=1, device_id=place.line_peer(hop), device_id_type=MESH_ID)

    def row(ref):
        return ref[...].reshape(1, ref.shape[0])

    def column(ref):
        return jnp.broadcast_to(row(ref), (128, ref.shape[0])).T[:, 0:1]

    def store(src, dst, index):
        return pltpu.make_async_copy(src, dst, store_sem.at[index])

    length = length_ref[0]
    loads[0].wait()
    values = hid[...].astype(f32)
    average = jnp.mean(values, axis=1, keepdims=True)
    centered = values - average
    inverse = lax.rsqrt(jnp.mean(centered * centered, axis=1, keepdims=True) + norm_eps)
    normed = centered * inverse
    norm[...] = normed
    rstd[...] = jnp.broadcast_to(inverse, rstd.shape)
    base[...] = values + (row(dbias_ref) + row(pbias_ref))
    attn_t[...] = (normed * row(again_ref) + row(ashift_ref)).astype(bf16).T
    low = (normed * row(fgain_ref) + row(fshift_ref)).astype(bf16)
    feed[...] = low
    feed_t[...] = low.T

    for i in range(seq_parts):
        ebias[i : i + 1, :] = ebias_ref[i * chunk : (i + 1) * chunk].reshape(1, chunk)
    which = lax.broadcasted_iota(jnp.int32, (half_rot, stretch), 0)
    spot = (seq * stretch + lax.broadcasted_iota(jnp.int32, (half_rot, stretch), 1)).astype(f32)
    frequency = jnp.zeros((half_rot, stretch), f32)
    for i in range(half_rot):
        frequency = jnp.where(which == i, 10000.0 ** (-2.0 * i / ROT), frequency)
    whole_cos, whole_sin = jnp.cos(spot * frequency), jnp.sin(spot * frequency)
    turns[0:half_rot, :] = whole_cos
    turns[half_rot:, :] = whole_sin

    def turn(rows, direction):
        lead, pair_part = rows[0:half_rot, :], rows[half_rot:ROT, :]
        cosine, sine = turns[0:half_rot, :], turns[half_rot:, :] * direction
        return jnp.concatenate(
            [lead * cosine - pair_part * sine, pair_part * cosine + lead * sine, rows[ROT:, :]], axis=0
        )

    loads[1].wait()
    own = lax.dot_general(wkv[...], attn_t[...], (((0,), (0,)), ((), ())),
                          preferred_element_type=f32) + column(kvbias_ref)
    kvt[0] = jnp.concatenate([turn(own[0:HD, :], 1.0), own[HD:, :]], axis=0).astype(bf16)

    def kv_copy(hop):
        return remote(kvt.at[0], kvt.at[seq_parts - hop], kv_send.at[hop - 1], kv_recv.at[hop - 1],
                      place.plane_peer(hop))

    pl.semaphore_wait(barrier, seq_parts + half - 1)
    loads[2].wait()
    wq_t = wq[...].T
    query_bias = column(qbias_ref)
    for hop in range(1, seq_parts):
        kv_copy(hop).start()
    for head in range(HEADS):
        span = slice(head * HD, (head + 1) * HD)
        rows = dot(wq_t[span, :], attn_t[...]) + query_bias[span, :]
        query_t[span, :] = (turn(rows, 1.0) * scale).astype(bf16)

    loads[3].wait()
    token = seq * stretch + lax.broadcasted_iota(jnp.int32, (stretch, 1), 0)
    masked = jnp.where(token < length, go[...].astype(f32), 0.0).astype(bf16)
    go[...] = masked
    go_t[...] = masked.T
    loads[4].wait()
    gm_t[...] = dot(wd[...], go_t[...]).astype(bf16)
    ones = jnp.ones((16, stretch), bf16)
    feed_own, attn_own = feed_small.own, attn_small.own
    feed_own[...] = jnp.zeros(feed_own.shape, f32)
    attn_own[...] = jnp.zeros(attn_own.shape, f32)
    parts = seq_parts
    feed_own[parts + 2 : parts + 3, :] = dot(ones, go[...])[0:1, :]

    dx[...] = jnp.zeros(dx.shape, f32)

    def feed_step(step, carry):
        slot = lax.rem(step, 2)
        part = place.swapped(3 - step)

        @pl.when(step + 1 < seq_parts)
        def _():
            for copy in load_chunk(step + 1):
                copy.start()

        for copy in load_chunk(step):
            copy.wait()
        upper = dot(feed[...], we[slot]) + ebias[pl.ds(part, 1), :]
        grad_active = dot_nt(go[...], wp[slot])
        share = 0.5 * (1.0 + lax.erf(upper * (0.5**0.5)))
        slope = share + upper * (jnp.exp(-0.5 * upper * upper) * 0.3989422804014327)
        active = (upper * share).astype(bf16)
        active_all[:, aligned(part * chunk, chunk, 128)] = active
        grad_upper = (grad_active * slope).astype(bf16)
        col_grad = dot(feed_t[...], grad_upper).astype(bf16)
        for i in range(2 * half):
            expand_sum.made[slot, i % 2, i // 2] = col_grad[i * col_rows : (i + 1) * col_rows, :]
        feed_own[pl.ds(part, 1), :] = dot(ones, grad_upper)[0:1, :]

        @pl.when(step > 0)
        def _():
            expand_sum.core_finish(step - 1)

        base[...] += dot(active, wp[slot])
        dx[...] += dot_nt(grad_upper, we[slot])

        @pl.when(step == 1)
        def _():
            expand_sum.via_start()

        @pl.when(step == 3)
        def _():
            expand_sum.side_start()

        expand_sum.core_copy(step).start()
        return carry

    lax.fori_loop(0, seq_parts, feed_step, 0)

    def project_step(step, carry):
        slot = lax.rem(step, 2)

        @pl.when(step == 1)
        def _():
            expand_sum.core_finish(3)

        @pl.when(step > 1)
        def _():
            project_sum.core_finish(step - 2)

        rows = aligned(place.swapped(3 - step) * row_rows, row_rows, 16)
        row_grad = dot(go_t[rows, :], active_all[...]).astype(bf16)
        for i in range(2 * half):
            project_sum.made[slot, i % 2, i // 2] = row_grad[:, i * row_cols : (i + 1) * row_cols]

        @pl.when(step == 2)
        def _():
            project_sum.via_start()

        project_sum.core_copy(step).start()
        return carry

    lax.fori_loop(0, seq_parts, project_step, 0)
    grad_feed = dx[...]
    feed_own[parts : parts + 1, :] = jnp.sum(grad_feed * norm[...], axis=0, keepdims=True)
    feed_own[parts + 1 : parts + 2, :] = jnp.sum(grad_feed, axis=0, keepdims=True)
    dx[...] = grad_feed * row(fgain_ref)

    lane = lax.broadcasted_iota(jnp.int32, (16, stretch), 1)
    first = lax.broadcasted_iota(jnp.int32, (16, stretch), 0) == 0
    unit_row = jnp.where(first, 1.0, 0.0).astype(bf16)
    rest = jnp.zeros((HD - 16, stretch), bf16)
    for hop in range(1, seq_parts):
        kv_copy(hop).wait()
    for i in range(seq_parts):
        span = slice(i * stretch, (i + 1) * stretch)
        held = kvt[i]
        owner = place.seq_at(i)
        usable = (owner * stretch + lane < length) & (owner <= seq)
        fence = jnp.where(first & jnp.logical_not(usable), masked_score, 0.0).astype(bf16)
        kaug[span, :] = jnp.concatenate([held[0:HD, :], fence, rest], axis=0).T
        kv[span, :] = held.T
        kt[:, span] = held[0:HD, :]
        vt[0:HD, span] = held[HD:, :]
        vt[HD:, span] = unit_row
    qaug[HD : HD + 16, :] = unit_row
    qaug[HD + 16 :, :] = rest
    pair[...] = jnp.zeros(pair.shape, bf16)
    dkv[...] = jnp.zeros(dkv.shape, f32)
    key_pos = lax.broadcasted_iota(jnp.int32, (stretch, stretch), 0)
    query_pos = lax.broadcasted_iota(jnp.int32, (stretch, stretch), 1)

    def attend(head):
        rows = aligned(head * HD, HD, HD)
        query = query_t[rows, :]
        qaug[0:HD, :] = query
        top = None
        for i in range(seq_parts):
            span = slice(i * stretch, (i + 1) * stretch)
            block = dot(kaug[span, :], qaug[...])
            if i == 0:
                block = jnp.where(key_pos <= query_pos, block, masked_score)
            score[span, :] = block
            block_top = jnp.max(block, axis=0, keepdims=True)
            top = block_top if top is None else jnp.maximum(top, block_top)
        mixed = jnp.zeros((HD + 16, stretch), f32)
        for i in range(seq_parts):
            span = slice(i * stretch, (i + 1) * stretch)
            low = jnp.exp(score[span, :] - top).astype(bf16)
            expo[span, :] = low
            mixed = mixed + dot(vt[:, span], low)
        inverse = 1.0 / mixed[HD : HD + 1, :]
        mixed = mixed[0:HD, :] * inverse
        mix_t[rows, :] = mixed.astype(bf16)
        grad = (gm_t[rows, :].astype(f32) * inverse).astype(bf16)
        delta = jnp.sum(grad.astype(f32) * mixed, axis=0, keepdims=True)
        pair[0:HD, 0:stretch] = query
        pair[HD:, stretch:] = grad
        grad_query = jnp.zeros((HD, stretch), f32)
        for i in range(seq_parts):
            span = slice(i * stretch, (i + 1) * stretch)
            block = dot(kv[span, :], pair[:, stretch:])
            low = expo[span, :]
            grad_score = (low.astype(f32) * (block - delta)).astype(bf16)
            grad_query = grad_query + dot(kt[:, span], grad_score)
            dkv[span, :] += dot_nt(jnp.concatenate([grad_score, low], axis=1), pair[...])
        gq_t[rows, :] = (turn(grad_query, -1.0) * scale).astype(bf16)

    def group_grads(step):
        slot = lax.rem(step, 2)
        rows = aligned(place.seq_at(step + 1) * group_rows, group_rows, 16)
        col_grad = dot_nt(attn_t[...], gq_t[rows, :]).astype(bf16)
        each = col_grad.shape[0] // (2 * half)
        for i in range(2 * half):
            attn_sum.ge[slot, i % 2, i // 2] = col_grad[i * each : (i + 1) * each, :]
        mixed_rows = mix_t[rows, :]
        across = width // seq_parts
        for i in range(seq_parts):
            block = dot_nt(mixed_rows, go_t[i * across : (i + 1) * across, :]).astype(bf16)
            for c in range(2):
                attn_sum.gp[slot, c, i] = block[c * each : (c + 1) * each, :]

    def head_step(index, carry):
        step = lax.div(index, group)
        attend(place.seq_at(step + 1) * group + lax.rem(index, group))

        @pl.when(index == 0)
        def _():
            project_sum.core_finish(2)
            project_sum.core_finish(3)
            expand_sum.side_finish()
            expand_sum.line_start()

        @pl.when(index == 2)
        def _():
            feed_small.core_copy().start()

        @pl.when(index == 3)
        def _():
            feed_small.plane_start()

        @pl.when(index == 4)
        def _():
            feed_small.line_start()

        @pl.when(index == SIDE_EVENT)
        def _():
            project_sum.side_start()

        @pl.when(index == LINE_EVENT)
        def _():
            project_sum.side_finish()
            project_sum.line_start()

        @pl.when((lax.rem(index, group) == 0) & (index > 0))
        def _():
            attn_sum.core_finish(step - 1)
            attn_sum.plane_start(step - 1)

        @pl.when((lax.rem(index, group) == group - 1) & (index < HEADS - 1))
        def _():
            group_grads(step)
            attn_sum.core_start(step)

        return carry

    lax.fori_loop(0, HEADS, head_step, 0)

    def dkv_copy(hop):
        return remote(dkv_out.at[hop - 1], dkv_in.at[hop - 1], dk_send.at[hop - 1],
                      dk_recv.at[hop - 1], place.plane_peer(hop))

    for hop in range(1, seq_parts):
        dkv_out[hop - 1] = dkv[hop * stretch : (hop + 1) * stretch, :].astype(bf16)
    for hop in range(1, seq_parts):
        dkv_copy(hop).start()
    last = seq_parts - 1
    group_grads(last)
    attn_sum.core_start(last)
    feed[...] = (base[...] + dot(mix_t[...].T, wd[...])).astype(bf16)
    attn_own[2:3, :] = dot_nt(ones, gq_t[...])[0:1, :]
    grad_attn = dot_nt(gq_t[...].T, wq[...])
    attn_sum.core_finish(last)
    attn_sum.plane_start(last)
    stores = [store(feed, out_hbm.at[0], 0)]
    stores[0].start()
    total = dkv[0:stretch, :]
    for hop in range(1, seq_parts):
        dkv_copy(hop).wait()
        total = total + dkv_in[hop - 1].astype(f32)
    total_t = total.T
    gkv_t = jnp.concatenate([turn(total_t[0:HD, :], -1.0), total_t[HD:, :]], axis=0).astype(bf16)
    kv_each, each = keyval_sum.made.shape[3:]
    for i in range(2 * half):
        block = dot_nt(gkv_t, attn_t[i * each : (i + 1) * each, :]).astype(bf16)
        for j in range(seq_parts):
            keyval_sum.made[i % 2, j, i // 2] = block[j * kv_each : (j + 1) * kv_each, :]
    keyval_sum.core_copy().start()
    grad_attn = grad_attn + dot_nt(gkv_t.T, wkv[...])
    attn_own[0:1, :] = jnp.sum(grad_attn * norm[...], axis=0, keepdims=True)
    attn_own[1:2, :] = jnp.sum(grad_attn, axis=0, keepdims=True)
    attn_own[3:4, 0 : 2 * HD] = dot_nt(ones, gkv_t)[0:1, :]
    attn_small.core_copy().start()
    attn_sum.sum_finish()
    attn_sum.line_start()
    back = dx[...] + grad_attn * row(again_ref)
    normed = norm[...]
    back_mean = jnp.mean(back, axis=1, keepdims=True)
    back_dot = jnp.mean(back * normed, axis=1, keepdims=True)
    keyval_sum.core_finish()
    keyval_sum.plane_start()
    attn_small.plane_start()
    dx[...] = go[...].astype(f32) + (back - back_mean - normed * back_dot) * rstd[:, 0:1]
    eout[...] = expand_sum.line_finish()
    pout[...] = project_sum.line_finish().T
    stores += [store(dx, dx_hbm.at[0], 1), store(eout, eout_hbm, 2), store(pout, pout_hbm, 3)]
    for copy in stores[1:]:
        copy.start()
    keyval_sum.plane_finish()
    keyval_sum.line_start()
    attn_small.line_start()
    feed_small_ref[...] = feed_small.line_sum()
    qd_ref[...] = attn_sum.line_finish()
    summed = keyval_sum.line_finish()
    kvout_ref[...] = summed
    attn_small_ref[...] = attn_small.line_sum()
    for copy in stores:
        copy.wait()


def finish_kernel(
    parts, out_in, dx_in, e_in, p_in, qd_ref, kv_ref, feed_ref, attn_ref, out_hbm, dx_hbm, e_hbm, p_hbm,
    wq_ref, wd_ref, wkv_ref, again_ref, ashift_ref, fgain_ref, fshift_ref, qbias_ref, kvbias_ref,
    dbias_ref, ebias_ref, pbias_ref, out_buf, dx_buf, e_buf, p_buf, in_sem, out_sem,
):
    sources, targets = (out_in, dx_in, e_in, p_in), (out_hbm, dx_hbm, e_hbm, p_hbm)
    held = (out_buf, dx_buf, e_buf, p_buf)
    incoming = [pltpu.make_async_copy(s, b, in_sem.at[i]) for i, (s, b) in enumerate(zip(sources, held))]
    outgoing = [pltpu.make_async_copy(b, t, out_sem.at[i]) for i, (b, t) in enumerate(zip(held, targets))]
    for copy in incoming:
        copy.start()
    cols = wq_ref.shape[1]
    wq_ref[...] = qd_ref[:, 0:cols]
    wd_ref[...] = qd_ref[:, cols:]
    summed = kv_ref[...]
    rest = jnp.zeros((summed.shape[0], 128 - summed.shape[1]), f32)
    wkv_ref[...] = jnp.concatenate([summed, rest], axis=1).T[0 : summed.shape[1], :]
    fgain_ref[...] = feed_ref[parts, :]
    fshift_ref[...] = feed_ref[parts + 1, :]
    dbias_ref[...] = feed_ref[parts + 2, :]
    pbias_ref[...] = feed_ref[parts + 2, :]
    width = feed_ref.shape[1]
    for i in range(parts):
        ebias_ref[i * width : (i + 1) * width] = feed_ref[i, :]
    again_ref[...] = attn_ref[0, :]
    ashift_ref[...] = attn_ref[1, :]
    qbias_ref[...] = attn_ref[2, :]
    kvbias_ref[...] = attn_ref[3, 0 : kvbias_ref.shape[0]]
    for i in range(len(held)):
        incoming[i].wait()
        outgoing[i].start()
    for copy in outgoing:
        copy.wait()


SIDE_EVENT = 1
LINE_EVENT = 5


def small_scratch(seq_parts, half, block):
    dma = pltpu.SemaphoreType.DMA
    return [
        pltpu.VMEM(block, f32), pltpu.VMEM(block, f32), pltpu.VMEM((seq_parts,) + block, f32),
        pltpu.VMEM((half,) + block, f32), dma((1,)), dma((1,)), dma((seq_parts - 1,)),
        dma((seq_parts - 1,)), dma((half - 1,)), dma((half - 1,)),
    ]


def fast_device(
    hidden_in, seq_lengths, attention_gain, attention_shift, feed_gain, feed_shift, query_weight,
    query_bias, keyval_weight, keyval_bias, dense_weight, dense_bias, expand_weight, expand_bias,
    project_weight, project_bias, out_grad,
):
    _, stretch, width = hidden_in.shape
    seq_parts, dp_parts = lax.axis_size("seq"), lax.axis_size("dp")
    half = dp_parts // 2
    hidden_units = expand_weight.shape[1]
    chunk = hidden_units // seq_parts
    whole_len = stretch * seq_parts
    rows, cols = width // dp_parts, width // seq_parts
    col_block, row_block = (rows, chunk), (cols, hidden_units // dp_parts)
    kv_block = (2 * HD // seq_parts, rows)
    small_block = (-(-(seq_parts + 3) // 8) * 8, width)
    sd, dma = jax.ShapeDtypeStruct, pltpu.SemaphoreType.DMA

    def vm(shape, dtype=bf16):
        return pltpu.VMEM(shape, dtype)

    in_vmem, in_hbm = pl.BlockSpec(memory_space=pltpu.VMEM), pl.BlockSpec(memory_space=pl.ANY)
    large = (
        sd((1, stretch, width), bf16), sd((1, stretch, width), f32), sd(col_block, f32),
        sd(row_block[::-1], f32),
    )
    mids = pl.pallas_call(
        functools.partial(layer_kernel, seq_parts, half),
        out_shape=large
        + (sd((rows, 2 * cols), f32), sd(kv_block, f32), sd(small_block, f32), sd(small_block, f32)),
        in_specs=[pl.BlockSpec(memory_space=pltpu.SMEM)] + [in_vmem] * 9 + [in_hbm] * 7,
        out_specs=(in_hbm,) * 4 + (in_vmem,) * 4,
        scratch_shapes=[
            vm((stretch, width)), vm((stretch, width)), vm((width, width)), vm((width, 2 * HD)),
            vm((width, width)), vm((2, width, chunk)), vm((2, chunk, width)),
            vm((stretch, width), f32), vm((stretch, 128), f32), vm((stretch, width)),
            vm((width, stretch)), vm((width, stretch)), vm((width, stretch)),
            vm((stretch, width), f32), vm((width, stretch)), vm((width, stretch)),
            vm((width, stretch)), vm((width, stretch)), vm((stretch, hidden_units)),
            vm((seq_parts, 2 * HD, stretch)), vm((HD, whole_len)), vm((HD + 16, whole_len)),
            vm((whole_len, 2 * HD)), vm((whole_len, 2 * HD)), vm((whole_len, stretch), f32),
            vm((whole_len, stretch)), vm((2 * HD, stretch)), vm((2 * HD, 2 * stretch)),
            vm((whole_len, 2 * HD), f32), vm((seq_parts - 1, stretch, 2 * HD)),
            vm((seq_parts - 1, stretch, 2 * HD)), vm((8, chunk), f32), vm((ROT, stretch), f32),
            vm((stretch, width), f32), vm(col_block, f32), vm(row_block[::-1], f32),
            dma((9,)), dma((4,)), dma((seq_parts - 1,)), dma((seq_parts - 1,)), dma((seq_parts - 1,)),
            dma((seq_parts - 1,)),
        ]
        + tree_scratch(half, col_block)
        + tree_scratch(half, row_block)
        + reduction_scratch(seq_parts, half, (rows, cols), (rows, cols))
        + small_scratch(seq_parts, half, small_block)
        + small_scratch(seq_parts, half, small_block)
        + keyval_scratch(seq_parts, half, kv_block),
        compiler_params=pltpu.CompilerParams(
            collective_id=0, has_side_effects=True, vmem_limit_bytes=VMEM_BYTES
        ),
    )(
        seq_lengths, attention_gain, attention_shift, feed_gain, feed_shift, query_bias, keyval_bias,
        dense_bias, expand_bias, project_bias, hidden_in, out_grad, query_weight, keyval_weight,
        dense_weight, expand_weight, project_weight,
    )
    vectors = (width, width, width, width, width, 2 * HD, width, hidden_units, width)
    outs = pl.pallas_call(
        functools.partial(finish_kernel, seq_parts),
        out_shape=large
        + (sd((rows, cols), f32), sd((rows, cols), f32), sd((rows, kv_block[0]), f32))
        + tuple(sd((size,), f32) for size in vectors),
        in_specs=[in_hbm] * 4 + [in_vmem] * 4,
        out_specs=(in_hbm,) * 4 + (in_vmem,) * 12,
        scratch_shapes=[pltpu.VMEM(v.shape, v.dtype) for v in large] + [dma((4,)), dma((4,))],
    )(*mids)
    (output, input_grad, expand_grad, project_grad, query_grad, dense_grad, keyval_grad, a_gain, a_shift,
     f_gain, f_shift, q_bias, kv_bias, d_bias, e_bias, p_bias) = outs
    return (
        output, input_grad, a_gain, a_shift, f_gain, f_shift, query_grad, q_bias, keyval_grad, kv_bias,
        dense_grad, d_bias, expand_grad, e_bias, project_grad, p_bias,
    )


def fits(hidden, expand_weight):
    seq_parts, dp_parts = lax.axis_size("seq"), lax.axis_size("dp")
    width, hidden_units = expand_weight.shape
    return (
        hidden.shape[0] == 1
        and dp_parts == 2 * seq_parts
        and seq_parts == 4
        and HEADS % seq_parts == 0
        and hidden_units == seq_parts * width
        and width % (16 * dp_parts) == 0
        and width % (16 * seq_parts) == 0
        and hidden_units % (128 * dp_parts) == 0
        and hidden.shape[1] % 128 == 0
    )


def solution(mesh):
    def either_way(*args):
        return (fast_device if fits(args[0], args[12]) else per_device)(*args)

    return jax.shard_map(
        either_way,
        mesh=mesh,
        in_specs=(
            P("dp", "seq", None),
            P("dp"),
            P(),
            P(),
            P(),
            P(),
            P(),
            P(),
            P(),
            P(),
            P(),
            P(),
            P(),
            P(),
            P(),
            P(),
            P("dp", "seq", None),
        ),
        out_specs=(
            P("dp", "seq", None),
            P("dp", "seq", None),
            P(),
            P(),
            P(),
            P(),
            P("dp", "seq"),
            P(),
            P("dp", "seq"),
            P(),
            P("dp", "seq"),
            P(),
            P("dp", "seq"),
            P(),
            P("dp", "seq"),
            P(),
        ),
        check_vma=False,
    )
```

```python
import functools

import jax
import jax.numpy as jnp
from jax import lax
from jax.experimental import pallas as pl
from jax.experimental.pallas import tpu as pltpu
from jax.sharding import PartitionSpec as P

HEADS = 12
HD = 64
ROT = 16
f32 = jnp.float32
bf16 = jnp.bfloat16


norm_eps = 1e-05
masked_score = -1e30


def layer_norm(values, gains, shifts):
    average = jnp.mean(values, axis=-1, keepdims=True)
    centered = values - average
    variance = jnp.mean(centered * centered, axis=-1, keepdims=True)
    return centered * lax.rsqrt(variance + norm_eps) * gains + shifts


def rotate(vectors, positions):
    half_rot = ROT // 2
    frequency = 10000.0 ** (-2.0 * jnp.arange(half_rot, dtype=jnp.float32) / ROT)
    angles = positions.astype(jnp.float32)[:, None] * frequency[None, :]
    cosine = jnp.cos(angles)
    sine_part = jnp.sin(angles)
    lead_part = vectors[..., :half_rot]
    pair_part = vectors[..., half_rot:ROT]
    rest_part = vectors[..., ROT:]
    return jnp.concatenate(
        [
            lead_part * cosine - pair_part * sine_part,
            pair_part * cosine + lead_part * sine_part,
            rest_part,
        ],
        axis=-1,
    )


def exact_gelu(values):
    return jax.nn.gelu(values, approximate=False)


def outer_sum(left, right):
    return lax.dot_general(
        left, right, (((0,), (0,)), ((), ())), preferred_element_type=jnp.float32
    )


def per_device(
    hidden_in,
    seq_lengths,
    attention_gain,
    attention_shift,
    feed_gain,
    feed_shift,
    query_weight,
    query_bias,
    keyval_weight,
    keyval_bias,
    dense_weight,
    dense_bias,
    expand_weight,
    expand_bias,
    project_weight,
    project_bias,
    out_grad,
):
    seq_count, stretch_len, model_width = hidden_in.shape
    seq_parts = lax.axis_size("seq")
    whole_len = stretch_len * seq_parts
    offset = lax.axis_index("seq") * stretch_len
    positions = offset + jnp.arange(stretch_len, dtype=jnp.int32)
    row_count = seq_count * stretch_len
    query_scale = HD ** (-0.5)
    inputs = hidden_in.astype(jnp.float32).reshape(row_count, model_width)
    valid_rows = positions[None, :] < seq_lengths[:, None]
    grad_out = jnp.where(valid_rows[:, :, None], out_grad, jnp.zeros_like(out_grad)).reshape(
        row_count, model_width
    )
    attn_norm, attn_norm_back = jax.vjp(layer_norm, inputs, attention_gain, attention_shift)
    feed_norm, feed_norm_back = jax.vjp(layer_norm, inputs, feed_gain, feed_shift)
    attn_in = attn_norm.astype(jnp.bfloat16)
    feed_in = feed_norm.astype(jnp.bfloat16)
    query_pre = jnp.dot(attn_in, query_weight, preferred_element_type=jnp.float32) + query_bias
    keyval_pre = jnp.dot(attn_in, keyval_weight, preferred_element_type=jnp.float32) + keyval_bias

    def turn_query(flat_query):
        shaped = flat_query.reshape(seq_count, stretch_len, HEADS, HD).transpose(0, 2, 1, 3)
        return rotate(shaped, positions) * query_scale

    def turn_keyval(flat_keyval):
        shaped = flat_keyval.reshape(seq_count, stretch_len, 2 * HD)
        return jnp.concatenate([rotate(shaped[..., :HD], positions), shaped[..., HD:]], axis=-1)

    query_rot, query_back = jax.vjp(turn_query, query_pre)
    keyval_rot, keyval_back = jax.vjp(turn_keyval, keyval_pre)
    query_low = query_rot.astype(jnp.bfloat16)
    keyval_low = keyval_rot.astype(jnp.bfloat16)
    gathered = lax.all_gather(keyval_low, "seq", axis=1, tiled=True)
    grad_mixed = jnp.dot(grad_out, dense_weight.T, preferred_element_type=jnp.float32).astype(
        jnp.bfloat16
    )
    grad_heads = grad_mixed.reshape(seq_count, stretch_len, HEADS, HD).transpose(0, 2, 1, 3)
    key_block = min(512, whole_len)
    block_count = whole_len // key_block
    group_size = 4

    def attend(operands):
        query_seq, grad_seq, keyval_seq, length = operands
        extent = block_count * key_block
        key_rows = keyval_seq[:extent, :HD]
        values = keyval_seq[:extent, HD:]
        key_pos = jnp.arange(extent, dtype=jnp.int32)
        allowed = (key_pos[None, :] <= positions[:, None]) & (key_pos[None, :] < length)

        def one_group(group_pair):
            query_grp, grad_grp = group_pair
            scores = jnp.einsum(
                "gtd,sd->gts", query_grp, key_rows, preferred_element_type=jnp.float32
            )
            scores = jnp.where(allowed[None], scores, masked_score)
            log_total = jax.nn.logsumexp(scores, axis=-1, keepdims=True)
            soft_weights = jnp.exp(scores - log_total)
            soft_low = soft_weights.astype(jnp.bfloat16)
            mixed_part = jnp.einsum(
                "gts,sd->gtd", soft_low, values, preferred_element_type=jnp.float32
            )
            grad_soft = jnp.einsum(
                "gtd,sd->gts", grad_grp, values, preferred_element_type=jnp.float32
            )
            row_delta = jnp.sum(soft_weights * grad_soft, axis=-1, keepdims=True)
            grad_scores = (soft_weights * (grad_soft - row_delta)).astype(jnp.bfloat16)
            grad_query = jnp.einsum(
                "gts,sd->gtd", grad_scores, key_rows, preferred_element_type=jnp.float32
            )
            grad_keys = jnp.einsum(
                "gts,gtd->sd", grad_scores, query_grp, preferred_element_type=jnp.float32
            )
            grad_values = jnp.einsum(
                "gts,gtd->sd", soft_low, grad_grp, preferred_element_type=jnp.float32
            )
            return (mixed_part, grad_query, jnp.concatenate([grad_keys, grad_values], axis=-1))

        grouped_query = query_seq.reshape(HEADS // group_size, group_size, stretch_len, HD)
        grouped_grad = grad_seq.reshape(HEADS // group_size, group_size, stretch_len, HD)
        mixed_part, grad_query, grad_keyval = lax.map(one_group, (grouped_query, grouped_grad))
        grad_keyval = jnp.sum(grad_keyval, axis=0)
        return (
            mixed_part.reshape(HEADS, stretch_len, HD),
            grad_query.reshape(HEADS, stretch_len, HD),
            grad_keyval,
        )

    mixed_all, grad_query_all, grad_keyval_all = lax.map(
        attend, (query_low, grad_heads, gathered, seq_lengths)
    )
    grad_keyval_own = lax.psum_scatter(grad_keyval_all, "seq", scatter_dimension=1, tiled=True)
    mixed_low = mixed_all.transpose(0, 2, 1, 3).reshape(row_count, model_width).astype(jnp.bfloat16)
    attn_out = jnp.dot(mixed_low, dense_weight, preferred_element_type=jnp.float32) + dense_bias
    upper = jnp.dot(feed_in, expand_weight, preferred_element_type=jnp.float32) + expand_bias
    active, active_back = jax.vjp(exact_gelu, upper)
    active_low = active.astype(jnp.bfloat16)
    feed_out = (
        jnp.dot(active_low, project_weight, preferred_element_type=jnp.float32) + project_bias
    )
    output = (
        (inputs + attn_out + feed_out)
        .astype(jnp.bfloat16)
        .reshape(seq_count, stretch_len, model_width)
    )
    grad_active = jnp.dot(grad_out, project_weight.T, preferred_element_type=jnp.float32)
    grad_upper = active_back(grad_active)[0].astype(jnp.bfloat16)
    grad_query_pre = query_back(grad_query_all)[0].astype(jnp.bfloat16)
    grad_keyval_pre = keyval_back(grad_keyval_own)[0].astype(jnp.bfloat16)
    grad_attn_in = jnp.dot(
        grad_query_pre, query_weight.T, preferred_element_type=jnp.float32
    ) + jnp.dot(grad_keyval_pre, keyval_weight.T, preferred_element_type=jnp.float32)
    grad_feed_in = jnp.dot(grad_upper, expand_weight.T, preferred_element_type=jnp.float32)
    attn_dx, attn_dgain, attn_dshift = attn_norm_back(grad_attn_in)
    feed_dx, feed_dgain, feed_dshift = feed_norm_back(grad_feed_in)
    input_grad = (grad_out.astype(jnp.float32) + attn_dx + feed_dx).reshape(
        seq_count, stretch_len, model_width
    )
    query_term = outer_sum(attn_in, grad_query_pre)
    keyval_term = outer_sum(attn_in, grad_keyval_pre)
    dense_term = outer_sum(mixed_low, grad_out)
    expand_term = outer_sum(feed_in, grad_upper)
    project_term = outer_sum(active_low, grad_out)
    row_sums = (
        lax.psum_scatter(query_term, "dp", scatter_dimension=0, tiled=True),
        lax.psum_scatter(keyval_term, "dp", scatter_dimension=0, tiled=True),
        lax.psum_scatter(dense_term, "dp", scatter_dimension=0, tiled=True),
        lax.psum_scatter(expand_term, "dp", scatter_dimension=0, tiled=True),
        lax.psum_scatter(project_term, "dp", scatter_dimension=0, tiled=True),
    )
    weight_grads = (
        lax.psum_scatter(row_sums[0], "seq", scatter_dimension=1, tiled=True),
        lax.psum_scatter(row_sums[1], "seq", scatter_dimension=1, tiled=True),
        lax.psum_scatter(row_sums[2], "seq", scatter_dimension=1, tiled=True),
        lax.psum_scatter(row_sums[3], "seq", scatter_dimension=1, tiled=True),
        lax.psum_scatter(row_sums[4], "seq", scatter_dimension=1, tiled=True),
    )
    out_total = jnp.sum(grad_out, axis=0, dtype=jnp.float32)
    small_sums = lax.psum(
        (
            attn_dgain,
            attn_dshift,
            feed_dgain,
            feed_dshift,
            jnp.sum(grad_query_pre, axis=0, dtype=jnp.float32),
            jnp.sum(grad_keyval_pre, axis=0, dtype=jnp.float32),
            out_total,
            jnp.sum(grad_upper, axis=0, dtype=jnp.float32),
        ),
        ("seq", "dp"),
    )
    return (
        output,
        input_grad,
        small_sums[0],
        small_sums[1],
        small_sums[2],
        small_sums[3],
        weight_grads[0],
        small_sums[4],
        weight_grads[1],
        small_sums[5],
        weight_grads[2],
        small_sums[6],
        weight_grads[3],
        small_sums[7],
        weight_grads[4],
        small_sums[6],
    )


NT_DIMS = (((1,), (1,)), ((), ()))
MESH_ID = pl.DeviceIdType.MESH
VMEM_BYTES = 67043328


def dot(left, right):
    return jnp.dot(left, right, preferred_element_type=f32)


def dot_nt(left, right):
    return lax.dot_general(left, right, NT_DIMS, preferred_element_type=f32)


def aligned(start, size, unit):
    return pl.ds(pl.multiple_of(start, unit), size)


class Place:
    def __init__(self, seq_parts, half):
        self.seq_parts, self.half = seq_parts, half
        self.seq = lax.axis_index("seq")
        self.dp = lax.axis_index("dp")
        self.core = lax.rem(self.dp, 2)
        self.line = lax.div(self.dp, 2)
        self.partner = {"dp": self.dp + 1 - 2 * self.core}

    def seq_at(self, hop):
        return lax.rem(self.seq + hop, self.seq_parts)

    def line_at(self, hop):
        return lax.rem(self.line + hop, self.half)

    def flip(self, mask):
        return {"seq": self.swapped(mask)}

    def swapped(self, mask):
        low, high = lax.rem(self.seq, 2), lax.div(self.seq, 2)
        low = lax.rem(low + lax.rem(mask, 2), 2)
        return low + 2 * lax.rem(high + lax.div(mask, 2), 2)

    def plane_peer(self, hop):
        return {"seq": self.seq_at(hop)}

    def line_peer(self, hop):
        return {"dp": self.line_at(hop) * 2 + self.core}


def remote(src, dst, send, recv, peer):
    return pltpu.make_async_remote_copy(
        src_ref=src, dst_ref=dst, send_sem=send, recv_sem=recv, device_id=peer,
        device_id_type=MESH_ID,
    )


class Reduction:
    def __init__(self, place, bufs, sems):
        self.at = place
        self.ge, self.gp, self.ce, self.cp, self.pe, self.pp, self.sums, self.landed = bufs
        (self.cs, self.cr, self.es, self.er, self.ps, self.pr, self.zs, self.zr) = sems

    def core_copies(self, step):
        at, slot = self.at, lax.rem(step, 2)
        return [
            remote(src.at[slot, 1 - at.core], dst.at[step], self.cs.at[step, i], self.cr.at[step, i],
                   at.partner)
            for i, (src, dst) in enumerate(((self.ge, self.ce), (self.gp, self.cp)))
        ]

    def core_start(self, step):
        for copy in self.core_copies(step):
            copy.start()

    def core_finish(self, step):
        at, slot = self.at, lax.rem(step, 2)
        for copy in self.core_copies(step):
            copy.wait()
        for src, dst in ((self.ge, self.ce), (self.gp, self.cp)):
            for i in range(dst.shape[1]):
                dst[step, i] = (src[slot, at.core, i].astype(f32) + dst[step, i].astype(f32)).astype(
                    bf16
                )

    def col_copy(self, step):
        return remote(self.ce.at[step], self.pe.at[step], self.es.at[step], self.er.at[step],
                      self.at.plane_peer(step + 1))

    def row_copy(self, step, hop):
        at, part = self.at, self.at.seq_at(step + 1)
        return remote(self.cp.at[step, at.seq_at(hop)], self.pp.at[part, hop - 1],
                      self.ps.at[step, hop - 1], self.pr.at[part, hop - 1], at.plane_peer(hop))

    def plane_start(self, step):
        @pl.when(step < self.at.seq_parts - 1)
        def _():
            self.col_copy(step).start()

        for hop in range(1, self.at.seq_parts):
            self.row_copy(step, hop).start()

    def sum_finish(self):
        at, last = self.at, self.at.seq_parts - 1
        for step in range(last):
            self.col_copy(step).wait()
        for step in range(at.seq_parts):
            for hop in range(1, at.seq_parts):
                self.row_copy(step, hop).wait()
        split = self.ce.shape[-1]
        for i in range(at.half):
            total = self.ce[last, i].astype(f32)
            for step in range(last):
                total = total + self.pe[step, i].astype(f32)
            self.sums[i, :, 0:split] = total.astype(bf16)
        for step in range(at.seq_parts):
            part = at.seq_at(step + 1)
            total = self.cp[step, at.seq].astype(f32)
            for hop in range(1, at.seq_parts):
                total = total + self.pp[part, hop - 1].astype(f32)
            self.sums[part, :, split:] = total.astype(bf16)

    def line_copy(self, hop):
        at = self.at
        return remote(self.sums.at[at.line_at(hop)], self.landed.at[hop - 1], self.zs.at[hop - 1],
                      self.zr.at[hop - 1], at.line_peer(hop))

    def line_start(self):
        for hop in range(1, self.at.half):
            self.line_copy(hop).start()

    def line_finish(self):
        total = self.sums[self.at.line].astype(f32)
        for hop in range(1, self.at.half):
            self.line_copy(hop).wait()
            total = total + self.landed[hop - 1].astype(f32)
        return total


def reduction_scratch(seq_parts, half, col_block, row_block):
    dma = pltpu.SemaphoreType.DMA
    hops, legs = seq_parts - 1, half - 1
    bufs = [
        (2, 2, half) + col_block, (2, 2, seq_parts) + row_block,
        (seq_parts, half) + col_block, (seq_parts, seq_parts) + row_block,
        (hops, half) + col_block, (seq_parts, hops) + row_block,
        (half, col_block[0], col_block[1] + row_block[1]),
        (legs, col_block[0], col_block[1] + row_block[1]),
    ]
    sems = [
        dma((seq_parts, 2)), dma((seq_parts, 2)), dma((hops,)), dma((hops,)),
        dma((seq_parts, hops)), dma((seq_parts, hops)), dma((legs,)), dma((legs,)),
    ]
    return [pltpu.VMEM(shape, bf16) for shape in bufs] + sems


class TreeSum:
    def __init__(self, place, bufs, sems):
        self.at = place
        self.made, self.core, self.via, self.side, self.sums, self.landed = bufs
        self.cs, self.cr, self.vs, self.vr, self.ss, self.sr, self.zs, self.zr = sems
        self.half = self.at.half // 2

    def core_copy(self, step):
        at, slot = self.at, lax.rem(step, 2)
        return remote(self.made.at[slot, 1 - at.core], self.core.at[step], self.cs.at[step],
                      self.cr.at[step], at.partner)

    def core_finish(self, step):
        at, slot = self.at, lax.rem(step, 2)
        self.core_copy(step).wait()
        for i in range(at.half):
            self.core[step, i] = (
                self.made[slot, at.core, i].astype(f32) + self.core[step, i].astype(f32)
            ).astype(bf16)

    def via_copy(self, side):
        span = pl.ds(side * self.half, self.half)
        return remote(self.core.at[0, span], self.via.at[side], self.vs.at[side], self.vr.at[side],
                      self.at.flip(1 + side))

    def via_start(self):
        for side in range(2):
            self.via_copy(side).start()

    def side_copy(self, side):
        return remote(self.core.at[1 + side], self.side.at[side], self.ss.at[side],
                      self.sr.at[side], self.at.flip(2 - side))

    def side_start(self):
        for side in range(2):
            self.via_copy(side).wait()
            for i in range(self.half):
                j = side * self.half + i
                self.core[1 + side, j] = (
                    self.core[1 + side, j].astype(f32) + self.via[side, i].astype(f32)
                ).astype(bf16)
        for side in range(2):
            self.side_copy(side).start()

    def side_finish(self):
        for side in range(2):
            self.side_copy(side).wait()
        for i in range(self.at.half):
            self.sums[i] = (
                self.core[3, i].astype(f32) + self.side[0, i].astype(f32) + self.side[1, i].astype(f32)
            ).astype(bf16)

    def line_copy(self, hop):
        at = self.at
        return remote(self.sums.at[at.line_at(hop)], self.landed.at[hop - 1], self.zs.at[hop - 1],
                      self.zr.at[hop - 1], at.line_peer(hop))

    def line_start(self):
        for hop in range(1, self.at.half):
            self.line_copy(hop).start()

    def line_finish(self):
        total = self.sums[self.at.line].astype(f32)
        for hop in range(1, self.at.half):
            self.line_copy(hop).wait()
            total = total + self.landed[hop - 1].astype(f32)
        return total


def tree_scratch(half, block):
    dma = pltpu.SemaphoreType.DMA
    bufs = [
        (2, 2, half) + block, (4, half) + block, (2, half // 2) + block, (2, half) + block,
        (half,) + block, (half - 1,) + block,
    ]
    return [pltpu.VMEM(shape, bf16) for shape in bufs] + [
        dma((4,)), dma((4,)), dma((2,)), dma((2,)), dma((2,)), dma((2,)), dma((half - 1,)),
        dma((half - 1,)),
    ]


class Small:
    def __init__(self, place, own, cbuf, pbuf, zbuf, sems):
        self.at, self.own, self.cbuf, self.pbuf, self.zbuf = place, own, cbuf, pbuf, zbuf
        self.cs, self.cr, self.ps, self.pr, self.zs, self.zr = sems

    def core_copy(self):
        return remote(self.own, self.cbuf, self.cs.at[0], self.cr.at[0], self.at.partner)

    def plane_copy(self, hop):
        at = self.at
        mine = self.pbuf.at[at.seq]
        return remote(mine, mine, self.ps.at[hop - 1], self.pr.at[hop - 1], at.plane_peer(hop))

    def plane_start(self):
        self.core_copy().wait()
        self.pbuf[self.at.seq] = self.own[...] + self.cbuf[...]
        for hop in range(1, self.at.seq_parts):
            self.plane_copy(hop).start()

    def plane_finish(self):
        for hop in range(1, self.at.seq_parts):
            self.plane_copy(hop).wait()
        total = self.pbuf[0].astype(f32)
        for i in range(1, self.at.seq_parts):
            total = total + self.pbuf[i].astype(f32)
        return total

    def line_copy(self, hop):
        at = self.at
        mine = self.zbuf.at[at.line]
        return remote(mine, mine, self.zs.at[hop - 1], self.zr.at[hop - 1], at.line_peer(hop))

    def line_start(self):
        self.zbuf[self.at.line] = self.plane_finish()
        for hop in range(1, self.at.half):
            self.line_copy(hop).start()

    def line_sum(self):
        for hop in range(1, self.at.half):
            self.line_copy(hop).wait()
        total = self.zbuf[0].astype(f32)
        for i in range(1, self.at.half):
            total = total + self.zbuf[i].astype(f32)
        return total


class KeyvalSum:
    def __init__(self, place, bufs, sems):
        self.at = place
        self.made, self.core, self.side, self.sums, self.landed = bufs
        self.cs, self.cr, self.ps, self.pr, self.zs, self.zr = sems

    def core_copy(self):
        return remote(self.made.at[1 - self.at.core], self.core, self.cs.at[0], self.cr.at[0],
                      self.at.partner)

    def plane_copy(self, hop):
        return remote(self.core.at[self.at.seq_at(hop)], self.side.at[hop - 1], self.ps.at[hop - 1],
                      self.pr.at[hop - 1], self.at.plane_peer(hop))

    def core_finish(self):
        self.core_copy().wait()
        self.core[...] = (
            self.made[self.at.core].astype(f32) + self.core[...].astype(f32)
        ).astype(bf16)

    def plane_start(self):
        for hop in range(1, self.at.seq_parts):
            self.plane_copy(hop).start()

    def plane_finish(self):
        total = self.core[self.at.seq].astype(f32)
        for hop in range(1, self.at.seq_parts):
            self.plane_copy(hop).wait()
            total = total + self.side[hop - 1].astype(f32)
        self.sums[...] = total.astype(bf16)

    def line_copy(self, hop):
        at = self.at
        return remote(self.sums.at[at.line_at(hop)], self.landed.at[hop - 1], self.zs.at[hop - 1],
                      self.zr.at[hop - 1], at.line_peer(hop))

    def line_start(self):
        for hop in range(1, self.at.half):
            self.line_copy(hop).start()

    def line_finish(self):
        total = self.sums[self.at.line].astype(f32)
        for hop in range(1, self.at.half):
            self.line_copy(hop).wait()
            total = total + self.landed[hop - 1].astype(f32)
        return total


def keyval_scratch(seq_parts, half, block):
    dma = pltpu.SemaphoreType.DMA
    bufs = [
        (2, seq_parts, half) + block, (seq_parts, half) + block, (seq_parts - 1, half) + block,
        (half,) + block, (half - 1,) + block,
    ]
    return [pltpu.VMEM(shape, bf16) for shape in bufs] + [
        dma((1,)), dma((1,)), dma((seq_parts - 1,)), dma((seq_parts - 1,)), dma((half - 1,)),
        dma((half - 1,)),
    ]


def layer_kernel(seq_parts, half, *refs):
    refs = list(refs)

    def take(count):
        taken, refs[:count] = refs[:count], []
        return taken

    (length_ref, again_ref, ashift_ref, fgain_ref, fshift_ref, qbias_ref, kvbias_ref, dbias_ref,
     ebias_ref, pbias_ref) = take(10)
    hid_hbm, og_hbm, wq_hbm, wkv_hbm, wd_hbm, we_hbm, wp_hbm = take(7)
    out_hbm, dx_hbm, eout_hbm, pout_hbm, qd_ref, kvout_ref, feed_small_ref, attn_small_ref = take(8)
    (hid, go, wq, wkv, wd, we, wp, norm, rstd, feed, feed_t, go_t, attn_t, base, query_t, gm_t, mix_t,
     gq_t, active_all, kvt, kt, vt, kaug, kv, score, expo, qaug, pair, dkv, dkv_out, dkv_in, ebias,
     turns, dx, eout, pout) = take(36)
    load_sem, store_sem, kv_send, kv_recv, dk_send, dk_recv = take(6)
    place = Place(seq_parts, half)
    expand_sum = TreeSum(place, take(6), take(8))
    project_sum = TreeSum(place, take(6), take(8))
    attn_sum = Reduction(place, take(8), take(8))
    feed_small = Small(place, *take(4), take(6))
    attn_small = Small(place, *take(4), take(6))
    keyval_sum = KeyvalSum(place, take(5), take(6))
    seq = place.seq
    stretch, width = hid.shape
    chunk = we.shape[2]
    col_rows = expand_sum.made.shape[3]
    row_rows, row_cols = project_sum.made.shape[3:]
    group = HEADS // seq_parts
    group_rows = group * HD
    half_rot = ROT // 2
    scale = HD ** (-0.5)

    def load(src, dst, index):
        return pltpu.make_async_copy(src, dst, load_sem.at[index])

    def load_chunk(step):
        slot = lax.rem(step, 2)
        start = place.swapped(3 - step) * chunk
        return (
            load(we_hbm.at[:, aligned(start, chunk, 128)], we.at[slot], 5 + 2 * slot),
            load(wp_hbm.at[aligned(start, chunk, 16), :], wp.at[slot], 6 + 2 * slot),
        )

    loads = (load(hid_hbm.at[0], hid, 0), load(wkv_hbm, wkv, 1), load(wq_hbm, wq, 2), load(og_hbm.at[0], go, 3),
             load(wd_hbm, wd, 4))
    for copy in loads:
        copy.start()
    for copy in load_chunk(0):
        copy.start()

    barrier = pltpu.get_barrier_semaphore()
    pl.semaphore_signal(barrier, inc=1, device_id=place.partner, device_id_type=MESH_ID)
    for hop in range(1, seq_parts):
        pl.semaphore_signal(barrier, inc=1, device_id=place.plane_peer(hop), device_id_type=MESH_ID)
    for hop in range(1, half):
        pl.semaphore_signal(barrier, inc=1, device_id=place.line_peer(hop), device_id_type=MESH_ID)

    def row(ref):
        return ref[...].reshape(1, ref.shape[0])

    def column(ref):
        return jnp.broadcast_to(row(ref), (128, ref.shape[0])).T[:, 0:1]

    def store(src, dst, index):
        return pltpu.make_async_copy(src, dst, store_sem.at[index])

    length = length_ref[0]
    loads[0].wait()
    values = hid[...].astype(f32)
    average = jnp.mean(values, axis=1, keepdims=True)
    centered = values - average
    inverse = lax.rsqrt(jnp.mean(centered * centered, axis=1, keepdims=True) + norm_eps)
    normed = centered * inverse
    norm[...] = normed
    rstd[...] = jnp.broadcast_to(inverse, rstd.shape)
    base[...] = values + (row(dbias_ref) + row(pbias_ref))
    attn_t[...] = (normed * row(again_ref) + row(ashift_ref)).astype(bf16).T
    low = (normed * row(fgain_ref) + row(fshift_ref)).astype(bf16)
    feed[...] = low
    feed_t[...] = low.T

    for i in range(seq_parts):
        ebias[i : i + 1, :] = ebias_ref[i * chunk : (i + 1) * chunk].reshape(1, chunk)
    which = lax.broadcasted_iota(jnp.int32, (half_rot, stretch), 0)
    spot = (seq * stretch + lax.broadcasted_iota(jnp.int32, (half_rot, stretch), 1)).astype(f32)
    frequency = jnp.zeros((half_rot, stretch), f32)
    for i in range(half_rot):
        frequency = jnp.where(which == i, 10000.0 ** (-2.0 * i / ROT), frequency)
    whole_cos, whole_sin = jnp.cos(spot * frequency), jnp.sin(spot * frequency)
    turns[0:half_rot, :] = whole_cos
    turns[half_rot:, :] = whole_sin

    def turn(rows, direction):
        lead, pair_part = rows[0:half_rot, :], rows[half_rot:ROT, :]
        cosine, sine = turns[0:half_rot, :], turns[half_rot:, :] * direction
        return jnp.concatenate(
            [lead * cosine - pair_part * sine, pair_part * cosine + lead * sine, rows[ROT:, :]], axis=0
        )

    loads[1].wait()
    own = lax.dot_general(wkv[...], attn_t[...], (((0,), (0,)), ((), ())),
                          preferred_element_type=f32) + column(kvbias_ref)
    kvt[0] = jnp.concatenate([turn(own[0:HD, :], 1.0), own[HD:, :]], axis=0).astype(bf16)

    def kv_copy(hop):
        return remote(kvt.at[0], kvt.at[seq_parts - hop], kv_send.at[hop - 1], kv_recv.at[hop - 1],
                      place.plane_peer(hop))

    pl.semaphore_wait(barrier, seq_parts + half - 1)
    loads[2].wait()
    query_pre = dot(wq[...].T, attn_t[...]) + column(qbias_ref)
    for hop in range(1, seq_parts):
        kv_copy(hop).start()
    for head in range(HEADS):
        span = slice(head * HD, (head + 1) * HD)
        query_t[span, :] = (turn(query_pre[span, :], 1.0) * scale).astype(bf16)

    loads[3].wait()
    token = seq * stretch + lax.broadcasted_iota(jnp.int32, (stretch, 1), 0)
    masked = jnp.where(token < length, go[...].astype(f32), 0.0).astype(bf16)
    go[...] = masked
    go_t[...] = masked.T
    loads[4].wait()
    gm_t[...] = dot(wd[...], go_t[...]).astype(bf16)
    ones = jnp.ones((16, stretch), bf16)
    feed_own, attn_own = feed_small.own, attn_small.own
    feed_own[...] = jnp.zeros(feed_own.shape, f32)
    attn_own[...] = jnp.zeros(attn_own.shape, f32)
    parts = seq_parts
    feed_own[parts + 2 : parts + 3, :] = dot(ones, go[...])[0:1, :]

    dx[...] = jnp.zeros(dx.shape, f32)

    def feed_step(step, carry):
        slot = lax.rem(step, 2)
        part = place.swapped(3 - step)

        @pl.when(step + 1 < seq_parts)
        def _():
            for copy in load_chunk(step + 1):
                copy.start()

        for copy in load_chunk(step):
            copy.wait()
        upper = dot(feed[...], we[slot]) + ebias[pl.ds(part, 1), :]
        grad_active = dot_nt(go[...], wp[slot])
        share = 0.5 * (1.0 + lax.erf(upper * (0.5**0.5)))
        slope = share + upper * (jnp.exp(-0.5 * upper * upper) * 0.3989422804014327)
        active = (upper * share).astype(bf16)
        active_all[:, aligned(part * chunk, chunk, 128)] = active
        grad_upper = (grad_active * slope).astype(bf16)
        col_grad = dot(feed_t[...], grad_upper).astype(bf16)
        for i in range(2 * half):
            expand_sum.made[slot, i % 2, i // 2] = col_grad[i * col_rows : (i + 1) * col_rows, :]
        feed_own[pl.ds(part, 1), :] = dot(ones, grad_upper)[0:1, :]

        @pl.when(step > 0)
        def _():
            expand_sum.core_finish(step - 1)

        base[...] += dot(active, wp[slot])
        dx[...] += dot_nt(grad_upper, we[slot])

        @pl.when(step == 1)
        def _():
            expand_sum.via_start()

        expand_sum.core_copy(step).start()
        return carry

    lax.fori_loop(0, seq_parts, feed_step, 0)

    def project_step(step, carry):
        slot = lax.rem(step, 2)

        @pl.when(step == 1)
        def _():
            expand_sum.core_finish(3)

        @pl.when(step > 1)
        def _():
            project_sum.core_finish(step - 2)

        rows = aligned(place.swapped(3 - step) * row_rows, row_rows, 16)
        row_grad = dot(go_t[rows, :], active_all[...]).astype(bf16)
        for i in range(2 * half):
            project_sum.made[slot, i % 2, i // 2] = row_grad[:, i * row_cols : (i + 1) * row_cols]

        @pl.when(step == 3)
        def _():
            expand_sum.side_start()
            project_sum.via_start()

        project_sum.core_copy(step).start()
        return carry

    lax.fori_loop(0, seq_parts, project_step, 0)
    grad_feed = dx[...]
    feed_own[parts : parts + 1, :] = jnp.sum(grad_feed * norm[...], axis=0, keepdims=True)
    feed_own[parts + 1 : parts + 2, :] = jnp.sum(grad_feed, axis=0, keepdims=True)
    dx[...] = grad_feed * row(fgain_ref)

    lane = lax.broadcasted_iota(jnp.int32, (16, stretch), 1)
    first = lax.broadcasted_iota(jnp.int32, (16, stretch), 0) == 0
    unit_row = jnp.where(first, 1.0, 0.0).astype(bf16)
    rest = jnp.zeros((HD - 16, stretch), bf16)
    for hop in range(1, seq_parts):
        kv_copy(hop).wait()
    for i in range(seq_parts):
        span = slice(i * stretch, (i + 1) * stretch)
        held = kvt[i]
        owner = place.seq_at(i)
        usable = (owner * stretch + lane < length) & (owner <= seq)
        fence = jnp.where(first & jnp.logical_not(usable), masked_score, 0.0).astype(bf16)
        kaug[span, :] = jnp.concatenate([held[0:HD, :], fence, rest], axis=0).T
        kv[span, :] = held.T
        kt[:, span] = held[0:HD, :]
        vt[0:HD, span] = held[HD:, :]
        vt[HD:, span] = unit_row
    qaug[HD : HD + 16, :] = unit_row
    qaug[HD + 16 :, :] = rest
    pair[...] = jnp.zeros(pair.shape, bf16)
    dkv[...] = jnp.zeros(dkv.shape, f32)
    key_pos = lax.broadcasted_iota(jnp.int32, (stretch, stretch), 0)
    query_pos = lax.broadcasted_iota(jnp.int32, (stretch, stretch), 1)

    def attend(head):
        rows = aligned(head * HD, HD, HD)
        query = query_t[rows, :]
        qaug[0:HD, :] = query
        top = None
        for i in range(seq_parts):
            span = slice(i * stretch, (i + 1) * stretch)
            block = dot(kaug[span, :], qaug[...])
            if i == 0:
                block = jnp.where(key_pos <= query_pos, block, masked_score)
            score[span, :] = block
            block_top = jnp.max(block, axis=0, keepdims=True)
            top = block_top if top is None else jnp.maximum(top, block_top)
        mixed = jnp.zeros((HD + 16, stretch), f32)
        for i in range(seq_parts):
            span = slice(i * stretch, (i + 1) * stretch)
            low = jnp.exp(score[span, :] - top).astype(bf16)
            expo[span, :] = low
            mixed = mixed + dot(vt[:, span], low)
        inverse = 1.0 / mixed[HD : HD + 1, :]
        mixed = mixed[0:HD, :] * inverse
        mix_t[rows, :] = mixed.astype(bf16)
        grad = (gm_t[rows, :].astype(f32) * inverse).astype(bf16)
        delta = jnp.sum(grad.astype(f32) * mixed, axis=0, keepdims=True)
        pair[0:HD, 0:stretch] = query
        pair[HD:, stretch:] = grad
        grad_query = jnp.zeros((HD, stretch), f32)
        for i in range(seq_parts):
            span = slice(i * stretch, (i + 1) * stretch)
            block = dot(kv[span, :], pair[:, stretch:])
            low = expo[span, :]
            grad_score = (low.astype(f32) * (block - delta)).astype(bf16)
            grad_query = grad_query + dot(kt[:, span], grad_score)
            dkv[span, :] += dot_nt(jnp.concatenate([grad_score, low], axis=1), pair[...])
        gq_t[rows, :] = (turn(grad_query, -1.0) * scale).astype(bf16)

    def group_grads(step):
        slot = lax.rem(step, 2)
        rows = aligned(place.seq_at(step + 1) * group_rows, group_rows, 16)
        col_grad = dot_nt(attn_t[...], gq_t[rows, :]).astype(bf16)
        each = col_grad.shape[0] // (2 * half)
        for i in range(2 * half):
            attn_sum.ge[slot, i % 2, i // 2] = col_grad[i * each : (i + 1) * each, :]
        mixed_rows = mix_t[rows, :]
        across = width // seq_parts
        for i in range(seq_parts):
            block = dot_nt(mixed_rows, go_t[i * across : (i + 1) * across, :]).astype(bf16)
            for c in range(2):
                attn_sum.gp[slot, c, i] = block[c * each : (c + 1) * each, :]

    def head_step(index, carry):
        step = lax.div(index, group)
        attend(place.seq_at(step + 1) * group + lax.rem(index, group))

        @pl.when(index == 0)
        def _():
            project_sum.core_finish(2)
            project_sum.core_finish(3)

        @pl.when(index == FIRST_EVENT)
        def _():
            expand_sum.side_finish()
            expand_sum.line_start()

        @pl.when(index == SMALL_EVENT + 0)
        def _():
            feed_small.core_copy().start()

        @pl.when(index == SMALL_EVENT + 1)
        def _():
            feed_small.plane_start()

        @pl.when(index == SMALL_EVENT + 2)
        def _():
            feed_small.line_start()

        @pl.when(index == SIDE_EVENT)
        def _():
            project_sum.side_start()

        @pl.when(index == LINE_EVENT)
        def _():
            project_sum.side_finish()
            project_sum.line_start()

        @pl.when((lax.rem(index, group) == 0) & (index > 0))
        def _():
            attn_sum.core_finish(step - 1)
            attn_sum.plane_start(step - 1)

        @pl.when((lax.rem(index, group) == group - 1) & (index < HEADS - 1))
        def _():
            group_grads(step)
            attn_sum.core_start(step)

        return carry

    lax.fori_loop(0, HEADS, head_step, 0)

    def dkv_copy(hop):
        return remote(dkv_out.at[hop - 1], dkv_in.at[hop - 1], dk_send.at[hop - 1],
                      dk_recv.at[hop - 1], place.plane_peer(hop))

    for hop in range(1, seq_parts):
        dkv_out[hop - 1] = dkv[hop * stretch : (hop + 1) * stretch, :].astype(bf16)
    for hop in range(1, seq_parts):
        dkv_copy(hop).start()
    last = seq_parts - 1
    group_grads(last)
    attn_sum.core_start(last)
    feed[...] = (base[...] + dot(mix_t[...].T, wd[...])).astype(bf16)
    attn_own[2:3, :] = dot_nt(ones, gq_t[...])[0:1, :]
    grad_attn = dot_nt(gq_t[...].T, wq[...])
    attn_sum.core_finish(last)
    attn_sum.plane_start(last)
    stores = [store(feed, out_hbm.at[0], 0)]
    stores[0].start()
    total = dkv[0:stretch, :]
    for hop in range(1, seq_parts):
        dkv_copy(hop).wait()
        total = total + dkv_in[hop - 1].astype(f32)
    total_t = total.T
    gkv_t = jnp.concatenate([turn(total_t[0:HD, :], -1.0), total_t[HD:, :]], axis=0).astype(bf16)
    kv_each, each = keyval_sum.made.shape[3:]
    for i in range(2 * half):
        block = dot_nt(gkv_t, attn_t[i * each : (i + 1) * each, :]).astype(bf16)
        for j in range(seq_parts):
            keyval_sum.made[i % 2, j, i // 2] = block[j * kv_each : (j + 1) * kv_each, :]
    keyval_sum.core_copy().start()
    grad_attn = grad_attn + dot_nt(gkv_t.T, wkv[...])
    attn_own[0:1, :] = jnp.sum(grad_attn * norm[...], axis=0, keepdims=True)
    attn_own[1:2, :] = jnp.sum(grad_attn, axis=0, keepdims=True)
    attn_own[3:4, 0 : 2 * HD] = dot_nt(ones, gkv_t)[0:1, :]
    attn_small.core_copy().start()
    attn_sum.sum_finish()
    attn_sum.line_start()
    back = dx[...] + grad_attn * row(again_ref)
    normed = norm[...]
    back_mean = jnp.mean(back, axis=1, keepdims=True)
    back_dot = jnp.mean(back * normed, axis=1, keepdims=True)
    keyval_sum.core_finish()
    keyval_sum.plane_start()
    attn_small.plane_start()
    dx[...] = go[...].astype(f32) + (back - back_mean - normed * back_dot) * rstd[:, 0:1]
    eout[...] = expand_sum.line_finish()
    pout[...] = project_sum.line_finish()
    stores += [store(dx, dx_hbm.at[0], 1), store(eout, eout_hbm, 2), store(pout, pout_hbm, 3)]
    for copy in stores[1:]:
        copy.start()
    keyval_sum.plane_finish()
    keyval_sum.line_start()
    attn_small.line_start()
    feed_small_ref[...] = feed_small.line_sum()
    qd_ref[...] = attn_sum.line_finish()
    summed = keyval_sum.line_finish()
    kvout_ref[...] = summed
    attn_small_ref[...] = attn_small.line_sum()
    for copy in stores:
        copy.wait()


def finish_kernel(
    parts, out_in, dx_in, e_in, p_in, qd_ref, kv_ref, feed_ref, attn_ref, out_hbm, dx_hbm, e_hbm, p_hbm,
    wq_ref, wd_ref, wkv_ref, again_ref, ashift_ref, fgain_ref, fshift_ref, qbias_ref, kvbias_ref,
    dbias_ref, ebias_ref, pbias_ref, out_buf, dx_buf, e_buf, p_buf, in_sem, out_sem,
):
    sources, targets = (out_in, dx_in, e_in, p_in), (out_hbm, dx_hbm, e_hbm, p_hbm)
    pieces = []
    for src, buf, dst in zip(sources, (out_buf, dx_buf, e_buf, p_buf), targets):
        count = 4 if len(src.shape) == 3 else 1
        size = src.shape[-2] // count
        for i in range(count):
            span = pl.ds(i * size, size)
            pieces.append(
                [v.at[0, span] if len(v.shape) == 3 else v.at[span] for v in (src, buf, dst)]
            )
    incoming = [pltpu.make_async_copy(p[0], p[1], in_sem.at[i]) for i, p in enumerate(pieces)]
    outgoing = [pltpu.make_async_copy(p[1], p[2], out_sem.at[i]) for i, p in enumerate(pieces)]
    for copy in incoming:
        copy.start()
    cols = wq_ref.shape[1]
    wq_ref[...] = qd_ref[:, 0:cols]
    wd_ref[...] = qd_ref[:, cols:]
    wkv_ref[...] = kv_ref[...]
    fgain_ref[...] = feed_ref[parts, :]
    fshift_ref[...] = feed_ref[parts + 1, :]
    dbias_ref[...] = feed_ref[parts + 2, :]
    pbias_ref[...] = feed_ref[parts + 2, :]
    width = feed_ref.shape[1]
    for i in range(parts):
        ebias_ref[i * width : (i + 1) * width] = feed_ref[i, :]
    again_ref[...] = attn_ref[0, :]
    ashift_ref[...] = attn_ref[1, :]
    qbias_ref[...] = attn_ref[2, :]
    kvbias_ref[...] = attn_ref[3, 0 : kvbias_ref.shape[0]]
    for i in range(len(pieces)):
        incoming[i].wait()
        outgoing[i].start()
    for copy in outgoing:
        copy.wait()


FIRST_EVENT = 3
SIDE_EVENT = 4
LINE_EVENT = 8
SMALL_EVENT = 9


def small_scratch(seq_parts, half, block):
    dma = pltpu.SemaphoreType.DMA
    return [
        pltpu.VMEM(block, f32), pltpu.VMEM(block, f32), pltpu.VMEM((seq_parts,) + block, f32),
        pltpu.VMEM((half,) + block, f32), dma((1,)), dma((1,)), dma((seq_parts - 1,)),
        dma((seq_parts - 1,)), dma((half - 1,)), dma((half - 1,)),
    ]


def fast_device(
    hidden_in, seq_lengths, attention_gain, attention_shift, feed_gain, feed_shift, query_weight,
    query_bias, keyval_weight, keyval_bias, dense_weight, dense_bias, expand_weight, expand_bias,
    project_weight, project_bias, out_grad,
):
    _, stretch, width = hidden_in.shape
    seq_parts, dp_parts = lax.axis_size("seq"), lax.axis_size("dp")
    half = dp_parts // 2
    hidden_units = expand_weight.shape[1]
    chunk = hidden_units // seq_parts
    whole_len = stretch * seq_parts
    rows, cols = width // dp_parts, width // seq_parts
    col_block, row_block = (rows, chunk), (cols, hidden_units // dp_parts)
    kv_block = (2 * HD // seq_parts, rows)
    small_block = (-(-(seq_parts + 3) // 8) * 8, width)
    sd, dma = jax.ShapeDtypeStruct, pltpu.SemaphoreType.DMA

    def vm(shape, dtype=bf16):
        return pltpu.VMEM(shape, dtype)

    in_vmem, in_hbm = pl.BlockSpec(memory_space=pltpu.VMEM), pl.BlockSpec(memory_space=pl.ANY)
    large = (
        sd((1, stretch, width), bf16), sd((1, stretch, width), f32), sd(col_block, f32),
        sd(row_block, f32),
    )
    mids = pl.pallas_call(
        functools.partial(layer_kernel, seq_parts, half),
        out_shape=large
        + (sd((rows, 2 * cols), f32), sd(kv_block, f32), sd(small_block, f32), sd(small_block, f32)),
        in_specs=[pl.BlockSpec(memory_space=pltpu.SMEM)] + [in_vmem] * 9 + [in_hbm] * 7,
        out_specs=(in_hbm,) * 4 + (in_vmem,) * 4,
        scratch_shapes=[
            vm((stretch, width)), vm((stretch, width)), vm((width, width)), vm((width, 2 * HD)),
            vm((width, width)), vm((2, width, chunk)), vm((2, chunk, width)),
            vm((stretch, width), f32), vm((stretch, 128), f32), vm((stretch, width)),
            vm((width, stretch)), vm((width, stretch)), vm((width, stretch)),
            vm((stretch, width), f32), vm((width, stretch)), vm((width, stretch)),
            vm((width, stretch)), vm((width, stretch)), vm((stretch, hidden_units)),
            vm((seq_parts, 2 * HD, stretch)), vm((HD, whole_len)), vm((HD + 16, whole_len)),
            vm((whole_len, 2 * HD)), vm((whole_len, 2 * HD)), vm((whole_len, stretch), f32),
            vm((whole_len, stretch)), vm((2 * HD, stretch)), vm((2 * HD, 2 * stretch)),
            vm((whole_len, 2 * HD), f32), vm((seq_parts - 1, stretch, 2 * HD)),
            vm((seq_parts - 1, stretch, 2 * HD)), vm((8, chunk), f32), vm((ROT, stretch), f32),
            vm((stretch, width), f32), vm(col_block, f32), vm(row_block, f32),
            dma((9,)), dma((4,)), dma((seq_parts - 1,)), dma((seq_parts - 1,)), dma((seq_parts - 1,)),
            dma((seq_parts - 1,)),
        ]
        + tree_scratch(half, col_block)
        + tree_scratch(half, row_block)
        + reduction_scratch(seq_parts, half, (rows, cols), (rows, cols))
        + small_scratch(seq_parts, half, small_block)
        + small_scratch(seq_parts, half, small_block)
        + keyval_scratch(seq_parts, half, kv_block),
        compiler_params=pltpu.CompilerParams(
            collective_id=0, has_side_effects=True, vmem_limit_bytes=VMEM_BYTES
        ),
    )(
        seq_lengths, attention_gain, attention_shift, feed_gain, feed_shift, query_bias, keyval_bias,
        dense_bias, expand_bias, project_bias, hidden_in, out_grad, query_weight, keyval_weight,
        dense_weight, expand_weight, project_weight,
    )
    vectors = (width, width, width, width, width, 2 * HD, width, hidden_units, width)
    outs = pl.pallas_call(
        functools.partial(finish_kernel, seq_parts),
        out_shape=large
        + (sd((rows, cols), f32), sd((rows, cols), f32), sd(kv_block, f32))
        + tuple(sd((size,), f32) for size in vectors),
        in_specs=[in_hbm] * 4 + [in_vmem] * 4,
        out_specs=(in_hbm,) * 4 + (in_vmem,) * 12,
        scratch_shapes=[pltpu.VMEM(v.shape, v.dtype) for v in large] + [dma((10,)), dma((10,))],
    )(*mids)
    (output, input_grad, expand_grad, project_grad, query_grad, dense_grad, keyval_grad, a_gain, a_shift,
     f_gain, f_shift, q_bias, kv_bias, d_bias, e_bias, p_bias) = outs
    return (
        output, input_grad, a_gain, a_shift, f_gain, f_shift, query_grad, q_bias, keyval_grad.T, kv_bias,
        dense_grad, d_bias, expand_grad, e_bias, project_grad.T, p_bias,
    )


def fits(hidden, expand_weight):
    seq_parts, dp_parts = lax.axis_size("seq"), lax.axis_size("dp")
    width, hidden_units = expand_weight.shape
    return (
        hidden.shape[0] == 1
        and dp_parts == 2 * seq_parts
        and seq_parts == 4
        and HEADS % seq_parts == 0
        and hidden_units == seq_parts * width
        and width % (16 * dp_parts) == 0
        and width % (16 * seq_parts) == 0
        and hidden_units % (128 * dp_parts) == 0
        and hidden.shape[1] % 128 == 0
    )


def solution(mesh):
    def either_way(*args):
        return (fast_device if fits(args[0], args[12]) else per_device)(*args)

    return jax.shard_map(
        either_way,
        mesh=mesh,
        in_specs=(
            P("dp", "seq", None),
            P("dp"),
            P(),
            P(),
            P(),
            P(),
            P(),
            P(),
            P(),
            P(),
            P(),
            P(),
            P(),
            P(),
            P(),
            P(),
            P("dp", "seq", None),
        ),
        out_specs=(
            P("dp", "seq", None),
            P("dp", "seq", None),
            P(),
            P(),
            P(),
            P(),
            P("dp", "seq"),
            P(),
            P("dp", "seq"),
            P(),
            P("dp", "seq"),
            P(),
            P("dp", "seq"),
            P(),
            P("dp", "seq"),
            P(),
        ),
        check_vma=False,
    )
```

```python
import functools

import jax
import jax.numpy as jnp
from jax import lax
from jax.experimental import pallas as pl
from jax.experimental.pallas import tpu as pltpu
from jax.sharding import PartitionSpec as P

HEADS = 12
HD = 64
ROT = 16
f32 = jnp.float32
bf16 = jnp.bfloat16


norm_eps = 1e-05
masked_score = -1e30


def layer_norm(values, gains, shifts):
    average = jnp.mean(values, axis=-1, keepdims=True)
    centered = values - average
    variance = jnp.mean(centered * centered, axis=-1, keepdims=True)
    return centered * lax.rsqrt(variance + norm_eps) * gains + shifts


def rotate(vectors, positions):
    half_rot = ROT // 2
    frequency = 10000.0 ** (-2.0 * jnp.arange(half_rot, dtype=jnp.float32) / ROT)
    angles = positions.astype(jnp.float32)[:, None] * frequency[None, :]
    cosine = jnp.cos(angles)
    sine_part = jnp.sin(angles)
    lead_part = vectors[..., :half_rot]
    pair_part = vectors[..., half_rot:ROT]
    rest_part = vectors[..., ROT:]
    return jnp.concatenate(
        [
            lead_part * cosine - pair_part * sine_part,
            pair_part * cosine + lead_part * sine_part,
            rest_part,
        ],
        axis=-1,
    )


def exact_gelu(values):
    return jax.nn.gelu(values, approximate=False)


def outer_sum(left, right):
    return lax.dot_general(
        left, right, (((0,), (0,)), ((), ())), preferred_element_type=jnp.float32
    )


def per_device(
    hidden_in,
    seq_lengths,
    attention_gain,
    attention_shift,
    feed_gain,
    feed_shift,
    query_weight,
    query_bias,
    keyval_weight,
    keyval_bias,
    dense_weight,
    dense_bias,
    expand_weight,
    expand_bias,
    project_weight,
    project_bias,
    out_grad,
):
    seq_count, stretch_len, model_width = hidden_in.shape
    seq_parts = lax.axis_size("seq")
    whole_len = stretch_len * seq_parts
    offset = lax.axis_index("seq") * stretch_len
    positions = offset + jnp.arange(stretch_len, dtype=jnp.int32)
    row_count = seq_count * stretch_len
    query_scale = HD ** (-0.5)
    inputs = hidden_in.astype(jnp.float32).reshape(row_count, model_width)
    valid_rows = positions[None, :] < seq_lengths[:, None]
    grad_out = jnp.where(valid_rows[:, :, None], out_grad, jnp.zeros_like(out_grad)).reshape(
        row_count, model_width
    )
    attn_norm, attn_norm_back = jax.vjp(layer_norm, inputs, attention_gain, attention_shift)
    feed_norm, feed_norm_back = jax.vjp(layer_norm, inputs, feed_gain, feed_shift)
    attn_in = attn_norm.astype(jnp.bfloat16)
    feed_in = feed_norm.astype(jnp.bfloat16)
    query_pre = jnp.dot(attn_in, query_weight, preferred_element_type=jnp.float32) + query_bias
    keyval_pre = jnp.dot(attn_in, keyval_weight, preferred_element_type=jnp.float32) + keyval_bias

    def turn_query(flat_query):
        shaped = flat_query.reshape(seq_count, stretch_len, HEADS, HD).transpose(0, 2, 1, 3)
        return rotate(shaped, positions) * query_scale

    def turn_keyval(flat_keyval):
        shaped = flat_keyval.reshape(seq_count, stretch_len, 2 * HD)
        return jnp.concatenate([rotate(shaped[..., :HD], positions), shaped[..., HD:]], axis=-1)

    query_rot, query_back = jax.vjp(turn_query, query_pre)
    keyval_rot, keyval_back = jax.vjp(turn_keyval, keyval_pre)
    query_low = query_rot.astype(jnp.bfloat16)
    keyval_low = keyval_rot.astype(jnp.bfloat16)
    gathered = lax.all_gather(keyval_low, "seq", axis=1, tiled=True)
    grad_mixed = jnp.dot(grad_out, dense_weight.T, preferred_element_type=jnp.float32).astype(
        jnp.bfloat16
    )
    grad_heads = grad_mixed.reshape(seq_count, stretch_len, HEADS, HD).transpose(0, 2, 1, 3)
    key_block = min(512, whole_len)
    block_count = whole_len // key_block
    group_size = 4

    def attend(operands):
        query_seq, grad_seq, keyval_seq, length = operands
        extent = block_count * key_block
        key_rows = keyval_seq[:extent, :HD]
        values = keyval_seq[:extent, HD:]
        key_pos = jnp.arange(extent, dtype=jnp.int32)
        allowed = (key_pos[None, :] <= positions[:, None]) & (key_pos[None, :] < length)

        def one_group(group_pair):
            query_grp, grad_grp = group_pair
            scores = jnp.einsum(
                "gtd,sd->gts", query_grp, key_rows, preferred_element_type=jnp.float32
            )
            scores = jnp.where(allowed[None], scores, masked_score)
            log_total = jax.nn.logsumexp(scores, axis=-1, keepdims=True)
            soft_weights = jnp.exp(scores - log_total)
            soft_low = soft_weights.astype(jnp.bfloat16)
            mixed_part = jnp.einsum(
                "gts,sd->gtd", soft_low, values, preferred_element_type=jnp.float32
            )
            grad_soft = jnp.einsum(
                "gtd,sd->gts", grad_grp, values, preferred_element_type=jnp.float32
            )
            row_delta = jnp.sum(soft_weights * grad_soft, axis=-1, keepdims=True)
            grad_scores = (soft_weights * (grad_soft - row_delta)).astype(jnp.bfloat16)
            grad_query = jnp.einsum(
                "gts,sd->gtd", grad_scores, key_rows, preferred_element_type=jnp.float32
            )
            grad_keys = jnp.einsum(
                "gts,gtd->sd", grad_scores, query_grp, preferred_element_type=jnp.float32
            )
            grad_values = jnp.einsum(
                "gts,gtd->sd", soft_low, grad_grp, preferred_element_type=jnp.float32
            )
            return (mixed_part, grad_query, jnp.concatenate([grad_keys, grad_values], axis=-1))

        grouped_query = query_seq.reshape(HEADS // group_size, group_size, stretch_len, HD)
        grouped_grad = grad_seq.reshape(HEADS // group_size, group_size, stretch_len, HD)
        mixed_part, grad_query, grad_keyval = lax.map(one_group, (grouped_query, grouped_grad))
        grad_keyval = jnp.sum(grad_keyval, axis=0)
        return (
            mixed_part.reshape(HEADS, stretch_len, HD),
            grad_query.reshape(HEADS, stretch_len, HD),
            grad_keyval,
        )

    mixed_all, grad_query_all, grad_keyval_all = lax.map(
        attend, (query_low, grad_heads, gathered, seq_lengths)
    )
    grad_keyval_own = lax.psum_scatter(grad_keyval_all, "seq", scatter_dimension=1, tiled=True)
    mixed_low = mixed_all.transpose(0, 2, 1, 3).reshape(row_count, model_width).astype(jnp.bfloat16)
    attn_out = jnp.dot(mixed_low, dense_weight, preferred_element_type=jnp.float32) + dense_bias
    upper = jnp.dot(feed_in, expand_weight, preferred_element_type=jnp.float32) + expand_bias
    active, active_back = jax.vjp(exact_gelu, upper)
    active_low = active.astype(jnp.bfloat16)
    feed_out = (
        jnp.dot(active_low, project_weight, preferred_element_type=jnp.float32) + project_bias
    )
    output = (
        (inputs + attn_out + feed_out)
        .astype(jnp.bfloat16)
        .reshape(seq_count, stretch_len, model_width)
    )
    grad_active = jnp.dot(grad_out, project_weight.T, preferred_element_type=jnp.float32)
    grad_upper = active_back(grad_active)[0].astype(jnp.bfloat16)
    grad_query_pre = query_back(grad_query_all)[0].astype(jnp.bfloat16)
    grad_keyval_pre = keyval_back(grad_keyval_own)[0].astype(jnp.bfloat16)
    grad_attn_in = jnp.dot(
        grad_query_pre, query_weight.T, preferred_element_type=jnp.float32
    ) + jnp.dot(grad_keyval_pre, keyval_weight.T, preferred_element_type=jnp.float32)
    grad_feed_in = jnp.dot(grad_upper, expand_weight.T, preferred_element_type=jnp.float32)
    attn_dx, attn_dgain, attn_dshift = attn_norm_back(grad_attn_in)
    feed_dx, feed_dgain, feed_dshift = feed_norm_back(grad_feed_in)
    input_grad = (grad_out.astype(jnp.float32) + attn_dx + feed_dx).reshape(
        seq_count, stretch_len, model_width
    )
    query_term = outer_sum(attn_in, grad_query_pre)
    keyval_term = outer_sum(attn_in, grad_keyval_pre)
    dense_term = outer_sum(mixed_low, grad_out)
    expand_term = outer_sum(feed_in, grad_upper)
    project_term = outer_sum(active_low, grad_out)
    row_sums = (
        lax.psum_scatter(query_term, "dp", scatter_dimension=0, tiled=True),
        lax.psum_scatter(keyval_term, "dp", scatter_dimension=0, tiled=True),
        lax.psum_scatter(dense_term, "dp", scatter_dimension=0, tiled=True),
        lax.psum_scatter(expand_term, "dp", scatter_dimension=0, tiled=True),
        lax.psum_scatter(project_term, "dp", scatter_dimension=0, tiled=True),
    )
    weight_grads = (
        lax.psum_scatter(row_sums[0], "seq", scatter_dimension=1, tiled=True),
        lax.psum_scatter(row_sums[1], "seq", scatter_dimension=1, tiled=True),
        lax.psum_scatter(row_sums[2], "seq", scatter_dimension=1, tiled=True),
        lax.psum_scatter(row_sums[3], "seq", scatter_dimension=1, tiled=True),
        lax.psum_scatter(row_sums[4], "seq", scatter_dimension=1, tiled=True),
    )
    out_total = jnp.sum(grad_out, axis=0, dtype=jnp.float32)
    small_sums = lax.psum(
        (
            attn_dgain,
            attn_dshift,
            feed_dgain,
            feed_dshift,
            jnp.sum(grad_query_pre, axis=0, dtype=jnp.float32),
            jnp.sum(grad_keyval_pre, axis=0, dtype=jnp.float32),
            out_total,
            jnp.sum(grad_upper, axis=0, dtype=jnp.float32),
        ),
        ("seq", "dp"),
    )
    return (
        output,
        input_grad,
        small_sums[0],
        small_sums[1],
        small_sums[2],
        small_sums[3],
        weight_grads[0],
        small_sums[4],
        weight_grads[1],
        small_sums[5],
        weight_grads[2],
        small_sums[6],
        weight_grads[3],
        small_sums[7],
        weight_grads[4],
        small_sums[6],
    )


NT_DIMS = (((1,), (1,)), ((), ()))
MESH_ID = pl.DeviceIdType.MESH
VMEM_BYTES = 67043328


def dot(left, right):
    return jnp.dot(left, right, preferred_element_type=f32)


def dot_nt(left, right):
    return lax.dot_general(left, right, NT_DIMS, preferred_element_type=f32)


def aligned(start, size, unit):
    return pl.ds(pl.multiple_of(start, unit), size)


class Place:
    def __init__(self, seq_parts, half):
        self.seq_parts, self.half = seq_parts, half
        self.seq = lax.axis_index("seq")
        self.dp = lax.axis_index("dp")
        self.core = lax.rem(self.dp, 2)
        self.line = lax.div(self.dp, 2)
        self.partner = {"dp": self.dp + 1 - 2 * self.core}

    def seq_at(self, hop):
        return lax.rem(self.seq + hop, self.seq_parts)

    def line_at(self, hop):
        return lax.rem(self.line + hop, self.half)

    def flip(self, mask):
        return {"seq": self.swapped(mask)}

    def swapped(self, mask):
        low, high = lax.rem(self.seq, 2), lax.div(self.seq, 2)
        low = lax.rem(low + lax.rem(mask, 2), 2)
        return low + 2 * lax.rem(high + lax.div(mask, 2), 2)

    def plane_peer(self, hop):
        return {"seq": self.seq_at(hop)}

    def line_peer(self, hop):
        return {"dp": self.line_at(hop) * 2 + self.core}


def remote(src, dst, send, recv, peer):
    return pltpu.make_async_remote_copy(
        src_ref=src, dst_ref=dst, send_sem=send, recv_sem=recv, device_id=peer,
        device_id_type=MESH_ID,
    )


class Reduction:
    def __init__(self, place, bufs, sems):
        self.at = place
        self.ge, self.gp, self.ce, self.cp, self.pe, self.pp, self.sums, self.landed = bufs
        (self.cs, self.cr, self.es, self.er, self.ps, self.pr, self.zs, self.zr) = sems

    def core_copies(self, step):
        at, slot = self.at, lax.rem(step, 2)
        return [
            remote(src.at[slot, 1 - at.core], dst.at[step], self.cs.at[step, i], self.cr.at[step, i],
                   at.partner)
            for i, (src, dst) in enumerate(((self.ge, self.ce), (self.gp, self.cp)))
        ]

    def core_start(self, step):
        for copy in self.core_copies(step):
            copy.start()

    def core_finish(self, step):
        at, slot = self.at, lax.rem(step, 2)
        for copy in self.core_copies(step):
            copy.wait()
        for src, dst in ((self.ge, self.ce), (self.gp, self.cp)):
            for i in range(dst.shape[1]):
                dst[step, i] = (src[slot, at.core, i].astype(f32) + dst[step, i].astype(f32)).astype(
                    bf16
                )

    def col_copy(self, step):
        return remote(self.ce.at[step], self.pe.at[step], self.es.at[step], self.er.at[step],
                      self.at.plane_peer(step + 1))

    def row_copy(self, step, hop):
        at, part = self.at, self.at.seq_at(step + 1)
        return remote(self.cp.at[step, at.seq_at(hop)], self.pp.at[part, hop - 1],
                      self.ps.at[step, hop - 1], self.pr.at[part, hop - 1], at.plane_peer(hop))

    def plane_start(self, step):
        @pl.when(step < self.at.seq_parts - 1)
        def _():
            self.col_copy(step).start()

        for hop in range(1, self.at.seq_parts):
            self.row_copy(step, hop).start()

    def sum_finish(self):
        at, last = self.at, self.at.seq_parts - 1
        for step in range(last):
            self.col_copy(step).wait()
        for step in range(at.seq_parts):
            for hop in range(1, at.seq_parts):
                self.row_copy(step, hop).wait()
        split = self.ce.shape[-1]
        for i in range(at.half):
            total = self.ce[last, i].astype(f32)
            for step in range(last):
                total = total + self.pe[step, i].astype(f32)
            self.sums[i, :, 0:split] = total.astype(bf16)
        for step in range(at.seq_parts):
            part = at.seq_at(step + 1)
            total = self.cp[step, at.seq].astype(f32)
            for hop in range(1, at.seq_parts):
                total = total + self.pp[part, hop - 1].astype(f32)
            self.sums[part, :, split:] = total.astype(bf16)

    def line_copy(self, hop):
        at = self.at
        return remote(self.sums.at[at.line_at(hop)], self.landed.at[hop - 1], self.zs.at[hop - 1],
                      self.zr.at[hop - 1], at.line_peer(hop))

    def line_start(self):
        for hop in range(1, self.at.half):
            self.line_copy(hop).start()

    def line_finish(self):
        total = self.sums[self.at.line].astype(f32)
        for hop in range(1, self.at.half):
            self.line_copy(hop).wait()
            total = total + self.landed[hop - 1].astype(f32)
        return total


def reduction_scratch(seq_parts, half, col_block, row_block):
    dma = pltpu.SemaphoreType.DMA
    hops, legs = seq_parts - 1, half - 1
    bufs = [
        (2, 2, half) + col_block, (2, 2, seq_parts) + row_block,
        (seq_parts, half) + col_block, (seq_parts, seq_parts) + row_block,
        (hops, half) + col_block, (seq_parts, hops) + row_block,
        (half, col_block[0], col_block[1] + row_block[1]),
        (legs, col_block[0], col_block[1] + row_block[1]),
    ]
    sems = [
        dma((seq_parts, 2)), dma((seq_parts, 2)), dma((hops,)), dma((hops,)),
        dma((seq_parts, hops)), dma((seq_parts, hops)), dma((legs,)), dma((legs,)),
    ]
    return [pltpu.VMEM(shape, bf16) for shape in bufs] + sems


class TreeSum:
    def __init__(self, place, bufs, sems):
        self.at = place
        self.made, self.core, self.via, self.side, self.sums, self.landed = bufs
        self.cs, self.cr, self.vs, self.vr, self.ss, self.sr, self.zs, self.zr = sems
        self.half = self.at.half // 2

    def core_copy(self, step):
        at, slot = self.at, lax.rem(step, 2)
        return remote(self.made.at[slot, 1 - at.core], self.core.at[step], self.cs.at[step],
                      self.cr.at[step], at.partner)

    def core_finish(self, step):
        at, slot = self.at, lax.rem(step, 2)
        self.core_copy(step).wait()
        for i in range(at.half):
            self.core[step, i] = (
                self.made[slot, at.core, i].astype(f32) + self.core[step, i].astype(f32)
            ).astype(bf16)

    def via_copy(self, side):
        span = pl.ds(side * self.half, self.half)
        return remote(self.core.at[0, span], self.via.at[side], self.vs.at[side], self.vr.at[side],
                      self.at.flip(1 + side))

    def via_start(self):
        for side in range(2):
            self.via_copy(side).start()

    def side_copy(self, side):
        return remote(self.core.at[1 + side], self.side.at[side], self.ss.at[side],
                      self.sr.at[side], self.at.flip(2 - side))

    def side_start(self):
        for side in range(2):
            self.via_copy(side).wait()
            for i in range(self.half):
                j = side * self.half + i
                self.core[1 + side, j] = (
                    self.core[1 + side, j].astype(f32) + self.via[side, i].astype(f32)
                ).astype(bf16)
        for side in range(2):
            self.side_copy(side).start()

    def side_finish(self):
        for side in range(2):
            self.side_copy(side).wait()
        for i in range(self.at.half):
            self.sums[i] = (
                self.core[3, i].astype(f32) + self.side[0, i].astype(f32) + self.side[1, i].astype(f32)
            ).astype(bf16)

    def line_copy(self, hop):
        at = self.at
        return remote(self.sums.at[at.line_at(hop)], self.landed.at[hop - 1], self.zs.at[hop - 1],
                      self.zr.at[hop - 1], at.line_peer(hop))

    def line_start(self):
        for hop in range(1, self.at.half):
            self.line_copy(hop).start()

    def line_finish(self):
        total = self.sums[self.at.line].astype(f32)
        for hop in range(1, self.at.half):
            self.line_copy(hop).wait()
            total = total + self.landed[hop - 1].astype(f32)
        return total


def tree_scratch(half, block):
    dma = pltpu.SemaphoreType.DMA
    bufs = [
        (2, 2, half) + block, (4, half) + block, (2, half // 2) + block, (2, half) + block,
        (half,) + block, (half - 1,) + block,
    ]
    return [pltpu.VMEM(shape, bf16) for shape in bufs] + [
        dma((4,)), dma((4,)), dma((2,)), dma((2,)), dma((2,)), dma((2,)), dma((half - 1,)),
        dma((half - 1,)),
    ]


class Small:
    def __init__(self, place, own, cbuf, pbuf, zbuf, sems):
        self.at, self.own, self.cbuf, self.pbuf, self.zbuf = place, own, cbuf, pbuf, zbuf
        self.cs, self.cr, self.ps, self.pr, self.zs, self.zr = sems

    def core_copy(self):
        return remote(self.own, self.cbuf, self.cs.at[0], self.cr.at[0], self.at.partner)

    def plane_copy(self, hop):
        at = self.at
        mine = self.pbuf.at[at.seq]
        return remote(mine, mine, self.ps.at[hop - 1], self.pr.at[hop - 1], at.plane_peer(hop))

    def plane_start(self):
        self.core_copy().wait()
        self.pbuf[self.at.seq] = self.own[...] + self.cbuf[...]
        for hop in range(1, self.at.seq_parts):
            self.plane_copy(hop).start()

    def plane_finish(self):
        for hop in range(1, self.at.seq_parts):
            self.plane_copy(hop).wait()
        total = self.pbuf[0].astype(f32)
        for i in range(1, self.at.seq_parts):
            total = total + self.pbuf[i].astype(f32)
        return total

    def line_copy(self, hop):
        at = self.at
        mine = self.zbuf.at[at.line]
        return remote(mine, mine, self.zs.at[hop - 1], self.zr.at[hop - 1], at.line_peer(hop))

    def line_start(self):
        self.zbuf[self.at.line] = self.plane_finish()
        for hop in range(1, self.at.half):
            self.line_copy(hop).start()

    def line_sum(self):
        for hop in range(1, self.at.half):
            self.line_copy(hop).wait()
        total = self.zbuf[0].astype(f32)
        for i in range(1, self.at.half):
            total = total + self.zbuf[i].astype(f32)
        return total


class KeyvalSum:
    def __init__(self, place, bufs, sems):
        self.at = place
        self.made, self.core, self.side, self.sums, self.landed = bufs
        self.cs, self.cr, self.ps, self.pr, self.zs, self.zr = sems

    def core_copy(self):
        return remote(self.made.at[1 - self.at.core], self.core, self.cs.at[0], self.cr.at[0],
                      self.at.partner)

    def plane_copy(self, hop):
        return remote(self.core.at[self.at.seq_at(hop)], self.side.at[hop - 1], self.ps.at[hop - 1],
                      self.pr.at[hop - 1], self.at.plane_peer(hop))

    def core_finish(self):
        self.core_copy().wait()
        self.core[...] = (
            self.made[self.at.core].astype(f32) + self.core[...].astype(f32)
        ).astype(bf16)

    def plane_start(self):
        for hop in range(1, self.at.seq_parts):
            self.plane_copy(hop).start()

    def plane_finish(self):
        total = self.core[self.at.seq].astype(f32)
        for hop in range(1, self.at.seq_parts):
            self.plane_copy(hop).wait()
            total = total + self.side[hop - 1].astype(f32)
        self.sums[...] = total.astype(bf16)

    def line_copy(self, hop):
        at = self.at
        return remote(self.sums.at[at.line_at(hop)], self.landed.at[hop - 1], self.zs.at[hop - 1],
                      self.zr.at[hop - 1], at.line_peer(hop))

    def line_start(self):
        for hop in range(1, self.at.half):
            self.line_copy(hop).start()

    def line_finish(self):
        total = self.sums[self.at.line].astype(f32)
        for hop in range(1, self.at.half):
            self.line_copy(hop).wait()
            total = total + self.landed[hop - 1].astype(f32)
        return total


def keyval_scratch(seq_parts, half, block):
    dma = pltpu.SemaphoreType.DMA
    bufs = [
        (2, seq_parts, half) + block, (seq_parts, half) + block, (seq_parts - 1, half) + block,
        (half,) + block, (half - 1,) + block,
    ]
    return [pltpu.VMEM(shape, bf16) for shape in bufs] + [
        dma((1,)), dma((1,)), dma((seq_parts - 1,)), dma((seq_parts - 1,)), dma((half - 1,)),
        dma((half - 1,)),
    ]


def layer_kernel(seq_parts, half, *refs):
    refs = list(refs)

    def take(count):
        taken, refs[:count] = refs[:count], []
        return taken

    (length_ref, again_ref, ashift_ref, fgain_ref, fshift_ref, qbias_ref, kvbias_ref, dbias_ref,
     ebias_ref, pbias_ref) = take(10)
    hid_hbm, og_hbm, wq_hbm, wkv_hbm, wd_hbm, we_hbm, wp_hbm = take(7)
    out_hbm, dx_hbm, eout_hbm, pout_hbm, qd_ref, kvout_ref, feed_small_ref, attn_small_ref = take(8)
    (hid, go, wq, wkv, wd, we, wp, norm, rstd, feed, feed_t, go_t, attn_t, base, query_t, gm_t, mix_t,
     gq_t, active_all, kvt, kt, vt, kaug, kv, score, expo, qaug, pair, dkv, dkv_out, dkv_in, ebias,
     turns, dx, eout, pout) = take(36)
    load_sem, store_sem, kv_send, kv_recv, dk_send, dk_recv = take(6)
    place = Place(seq_parts, half)
    expand_sum = TreeSum(place, take(6), take(8))
    project_sum = TreeSum(place, take(6), take(8))
    attn_sum = Reduction(place, take(8), take(8))
    feed_small = Small(place, *take(4), take(6))
    attn_small = Small(place, *take(4), take(6))
    keyval_sum = KeyvalSum(place, take(5), take(6))
    seq = place.seq
    stretch, width = hid.shape
    chunk = we.shape[2]
    col_rows = expand_sum.made.shape[3]
    row_rows, row_cols = project_sum.made.shape[3:]
    group = HEADS // seq_parts
    group_rows = group * HD
    half_rot = ROT // 2
    scale = HD ** (-0.5)

    def load(src, dst, index):
        return pltpu.make_async_copy(src, dst, load_sem.at[index])

    def load_chunk(step):
        slot = lax.rem(step, 2)
        start = place.swapped(3 - step) * chunk
        return (
            load(we_hbm.at[:, aligned(start, chunk, 128)], we.at[slot], 5 + 2 * slot),
            load(wp_hbm.at[aligned(start, chunk, 16), :], wp.at[slot], 6 + 2 * slot),
        )

    loads = (load(hid_hbm.at[0], hid, 0), load(wkv_hbm, wkv, 1), load(wq_hbm, wq, 2), load(og_hbm.at[0], go, 3),
             load(wd_hbm, wd, 4))
    for copy in loads:
        copy.start()
    for copy in load_chunk(0):
        copy.start()

    barrier = pltpu.get_barrier_semaphore()
    pl.semaphore_signal(barrier, inc=1, device_id=place.partner, device_id_type=MESH_ID)
    for hop in range(1, seq_parts):
        pl.semaphore_signal(barrier, inc=1, device_id=place.plane_peer(hop), device_id_type=MESH_ID)
    for hop in range(1, half):
        pl.semaphore_signal(barrier, inc=1, device_id=place.line_peer(hop), device_id_type=MESH_ID)

    def row(ref):
        return ref[...].reshape(1, ref.shape[0])

    def column(ref):
        return jnp.broadcast_to(row(ref), (128, ref.shape[0])).T[:, 0:1]

    def store(src, dst, index):
        return pltpu.make_async_copy(src, dst, store_sem.at[index])

    length = length_ref[0]
    loads[0].wait()
    values = hid[...].astype(f32)
    average = jnp.mean(values, axis=1, keepdims=True)
    centered = values - average
    inverse = lax.rsqrt(jnp.mean(centered * centered, axis=1, keepdims=True) + norm_eps)
    normed = centered * inverse
    norm[...] = normed
    rstd[...] = jnp.broadcast_to(inverse, rstd.shape)
    base[...] = values + (row(dbias_ref) + row(pbias_ref))
    attn_t[...] = (normed * row(again_ref) + row(ashift_ref)).astype(bf16).T
    low = (normed * row(fgain_ref) + row(fshift_ref)).astype(bf16)
    feed[...] = low
    feed_t[...] = low.T

    for i in range(seq_parts):
        ebias[i : i + 1, :] = ebias_ref[i * chunk : (i + 1) * chunk].reshape(1, chunk)
    which = lax.broadcasted_iota(jnp.int32, (half_rot, stretch), 0)
    spot = (seq * stretch + lax.broadcasted_iota(jnp.int32, (half_rot, stretch), 1)).astype(f32)
    frequency = jnp.zeros((half_rot, stretch), f32)
    for i in range(half_rot):
        frequency = jnp.where(which == i, 10000.0 ** (-2.0 * i / ROT), frequency)
    whole_cos, whole_sin = jnp.cos(spot * frequency), jnp.sin(spot * frequency)
    turns[0:half_rot, :] = whole_cos
    turns[half_rot:, :] = whole_sin

    def turn(rows, direction):
        lead, pair_part = rows[0:half_rot, :], rows[half_rot:ROT, :]
        cosine, sine = turns[0:half_rot, :], turns[half_rot:, :] * direction
        return jnp.concatenate(
            [lead * cosine - pair_part * sine, pair_part * cosine + lead * sine, rows[ROT:, :]], axis=0
        )

    loads[1].wait()
    own = lax.dot_general(wkv[...], attn_t[...], (((0,), (0,)), ((), ())),
                          preferred_element_type=f32) + column(kvbias_ref)
    kvt[0] = jnp.concatenate([turn(own[0:HD, :], 1.0), own[HD:, :]], axis=0).astype(bf16)

    def kv_copy(hop):
        return remote(kvt.at[0], kvt.at[seq_parts - hop], kv_send.at[hop - 1], kv_recv.at[hop - 1],
                      place.plane_peer(hop))

    pl.semaphore_wait(barrier, seq_parts + half - 1)
    loads[2].wait()
    query_pre = dot(wq[...].T, attn_t[...]) + column(qbias_ref)
    for hop in range(1, seq_parts):
        kv_copy(hop).start()
    for head in range(HEADS):
        span = slice(head * HD, (head + 1) * HD)
        query_t[span, :] = (turn(query_pre[span, :], 1.0) * scale).astype(bf16)

    loads[3].wait()
    token = seq * stretch + lax.broadcasted_iota(jnp.int32, (stretch, 1), 0)
    masked = jnp.where(token < length, go[...].astype(f32), 0.0).astype(bf16)
    go[...] = masked
    go_t[...] = masked.T
    loads[4].wait()
    gm_t[...] = dot(wd[...], go_t[...]).astype(bf16)
    ones = jnp.ones((16, stretch), bf16)
    feed_own, attn_own = feed_small.own, attn_small.own
    feed_own[...] = jnp.zeros(feed_own.shape, f32)
    attn_own[...] = jnp.zeros(attn_own.shape, f32)
    parts = seq_parts
    feed_own[parts + 2 : parts + 3, :] = dot(ones, go[...])[0:1, :]

    dx[...] = jnp.zeros(dx.shape, f32)

    def feed_step(step, carry):
        slot = lax.rem(step, 2)
        part = place.swapped(3 - step)

        @pl.when(step + 1 < seq_parts)
        def _():
            for copy in load_chunk(step + 1):
                copy.start()

        for copy in load_chunk(step):
            copy.wait()
        upper = dot(feed[...], we[slot]) + ebias[pl.ds(part, 1), :]
        grad_active = dot_nt(go[...], wp[slot])
        share = 0.5 * (1.0 + lax.erf(upper * (0.5**0.5)))
        slope = share + upper * (jnp.exp(-0.5 * upper * upper) * 0.3989422804014327)
        active = (upper * share).astype(bf16)
        active_all[:, aligned(part * chunk, chunk, 128)] = active
        grad_upper = (grad_active * slope).astype(bf16)
        col_grad = dot(feed_t[...], grad_upper).astype(bf16)
        for i in range(2 * half):
            expand_sum.made[slot, i % 2, i // 2] = col_grad[i * col_rows : (i + 1) * col_rows, :]
        feed_own[pl.ds(part, 1), :] = dot(ones, grad_upper)[0:1, :]

        dx[...] += dot_nt(grad_upper, we[slot])

        @pl.when(step > 0)
        def _():
            expand_sum.core_finish(step - 1)

        @pl.when(step == 1)
        def _():
            expand_sum.via_start()

        expand_sum.core_copy(step).start()
        return carry

    lax.fori_loop(0, seq_parts, feed_step, 0)

    def project_step(step, carry):
        slot = lax.rem(step, 2)

        @pl.when(step == 1)
        def _():
            expand_sum.core_finish(3)

        @pl.when(step > 1)
        def _():
            project_sum.core_finish(step - 2)

        rows = aligned(place.swapped(3 - step) * row_rows, row_rows, 16)
        row_grad = dot(go_t[rows, :], active_all[...]).astype(bf16)
        for i in range(2 * half):
            project_sum.made[slot, i % 2, i // 2] = row_grad[:, i * row_cols : (i + 1) * row_cols]

        @pl.when(step == 3)
        def _():
            expand_sum.side_start()
            project_sum.via_start()

        project_sum.core_copy(step).start()
        return carry

    lax.fori_loop(0, seq_parts, project_step, 0)
    grad_feed = dx[...]
    feed_own[parts : parts + 1, :] = jnp.sum(grad_feed * norm[...], axis=0, keepdims=True)
    feed_own[parts + 1 : parts + 2, :] = jnp.sum(grad_feed, axis=0, keepdims=True)
    dx[...] = grad_feed * row(fgain_ref)

    lane = lax.broadcasted_iota(jnp.int32, (16, stretch), 1)
    first = lax.broadcasted_iota(jnp.int32, (16, stretch), 0) == 0
    unit_row = jnp.where(first, 1.0, 0.0).astype(bf16)
    rest = jnp.zeros((HD - 16, stretch), bf16)
    for hop in range(1, seq_parts):
        kv_copy(hop).wait()
    for i in range(seq_parts):
        span = slice(i * stretch, (i + 1) * stretch)
        held = kvt[i]
        owner = place.seq_at(i)
        usable = (owner * stretch + lane < length) & (owner <= seq)
        fence = jnp.where(first & jnp.logical_not(usable), masked_score, 0.0).astype(bf16)
        kaug[span, :] = jnp.concatenate([held[0:HD, :], fence, rest], axis=0).T
        kv[span, :] = held.T
        kt[:, span] = held[0:HD, :]
        vt[0:HD, span] = held[HD:, :]
        vt[HD:, span] = unit_row
    qaug[HD : HD + 16, :] = unit_row
    qaug[HD + 16 :, :] = rest
    pair[...] = jnp.zeros(pair.shape, bf16)
    dkv[...] = jnp.zeros(dkv.shape, f32)
    key_pos = lax.broadcasted_iota(jnp.int32, (stretch, stretch), 0)
    query_pos = lax.broadcasted_iota(jnp.int32, (stretch, stretch), 1)

    def attend(head):
        rows = aligned(head * HD, HD, HD)
        query = query_t[rows, :]
        qaug[0:HD, :] = query
        top = None
        for i in range(seq_parts):
            span = slice(i * stretch, (i + 1) * stretch)
            block = dot(kaug[span, :], qaug[...])
            if i == 0:
                block = jnp.where(key_pos <= query_pos, block, masked_score)
            score[span, :] = block
            block_top = jnp.max(block, axis=0, keepdims=True)
            top = block_top if top is None else jnp.maximum(top, block_top)
        mixed = jnp.zeros((HD + 16, stretch), f32)
        for i in range(seq_parts):
            span = slice(i * stretch, (i + 1) * stretch)
            low = jnp.exp(score[span, :] - top).astype(bf16)
            expo[span, :] = low
            mixed = mixed + dot(vt[:, span], low)
        inverse = 1.0 / mixed[HD : HD + 1, :]
        mixed = mixed[0:HD, :] * inverse
        mix_t[rows, :] = mixed.astype(bf16)
        grad = (gm_t[rows, :].astype(f32) * inverse).astype(bf16)
        delta = jnp.sum(grad.astype(f32) * mixed, axis=0, keepdims=True)
        pair[0:HD, 0:stretch] = query
        pair[HD:, stretch:] = grad
        grad_query = jnp.zeros((HD, stretch), f32)
        for i in range(seq_parts):
            span = slice(i * stretch, (i + 1) * stretch)
            block = dot(kv[span, :], pair[:, stretch:])
            low = expo[span, :]
            grad_score = (low.astype(f32) * (block - delta)).astype(bf16)
            grad_query = grad_query + dot(kt[:, span], grad_score)
            dkv[span, :] += dot_nt(jnp.concatenate([grad_score, low], axis=1), pair[...])
        gq_t[rows, :] = (turn(grad_query, -1.0) * scale).astype(bf16)

    def group_grads(step):
        slot = lax.rem(step, 2)
        rows = aligned(place.seq_at(step + 1) * group_rows, group_rows, 16)
        col_grad = dot_nt(attn_t[...], gq_t[rows, :]).astype(bf16)
        each = col_grad.shape[0] // (2 * half)
        for i in range(2 * half):
            attn_sum.ge[slot, i % 2, i // 2] = col_grad[i * each : (i + 1) * each, :]
        mixed_rows = mix_t[rows, :]
        across = width // seq_parts
        for i in range(seq_parts):
            block = dot_nt(mixed_rows, go_t[i * across : (i + 1) * across, :]).astype(bf16)
            for c in range(2):
                attn_sum.gp[slot, c, i] = block[c * each : (c + 1) * each, :]

    def head_step(index, carry):
        step = lax.div(index, group)
        attend(place.seq_at(step + 1) * group + lax.rem(index, group))

        @pl.when(index == 0)
        def _():
            project_sum.core_finish(2)
            project_sum.core_finish(3)

        @pl.when(index == FIRST_EVENT)
        def _():
            expand_sum.side_finish()
            expand_sum.line_start()

        @pl.when(index == SMALL_EVENT + 0)
        def _():
            feed_small.core_copy().start()

        @pl.when(index == SMALL_EVENT + 1)
        def _():
            feed_small.plane_start()

        @pl.when(index == SMALL_EVENT + 2)
        def _():
            feed_small.line_start()

        @pl.when(index == SIDE_EVENT)
        def _():
            project_sum.side_start()

        @pl.when(index == LINE_EVENT)
        def _():
            project_sum.side_finish()
            project_sum.line_start()

        @pl.when((lax.rem(index, group) == 0) & (index > 0))
        def _():
            attn_sum.core_finish(step - 1)
            attn_sum.plane_start(step - 1)

        @pl.when((lax.rem(index, group) == group - 1) & (index < HEADS - 1))
        def _():
            group_grads(step)
            attn_sum.core_start(step)

        return carry

    def load_again(i):
        return load(wp_hbm.at[i * chunk : (i + 1) * chunk, :], wp.at[i % 2], 6 + 2 * (i % 2))

    for i in range(2):
        load_again(i).start()
    lax.fori_loop(0, HEADS, head_step, 0)

    def dkv_copy(hop):
        return remote(dkv_out.at[hop - 1], dkv_in.at[hop - 1], dk_send.at[hop - 1],
                      dk_recv.at[hop - 1], place.plane_peer(hop))

    for hop in range(1, seq_parts):
        dkv_out[hop - 1] = dkv[hop * stretch : (hop + 1) * stretch, :].astype(bf16)
    for hop in range(1, seq_parts):
        dkv_copy(hop).start()
    last = seq_parts - 1
    group_grads(last)
    attn_sum.core_start(last)
    grad_attn = dot_nt(gq_t[...].T, wq[...])
    attn_own[2:3, :] = dot_nt(ones, gq_t[...])[0:1, :]
    attn_sum.core_finish(last)
    attn_sum.plane_start(last)
    total = dkv[0:stretch, :]
    for hop in range(1, seq_parts):
        dkv_copy(hop).wait()
        total = total + dkv_in[hop - 1].astype(f32)
    total_t = total.T
    gkv_t = jnp.concatenate([turn(total_t[0:HD, :], -1.0), total_t[HD:, :]], axis=0).astype(bf16)
    kv_each, each = keyval_sum.made.shape[3:]
    for i in range(2 * half):
        block = dot_nt(gkv_t, attn_t[i * each : (i + 1) * each, :]).astype(bf16)
        for j in range(seq_parts):
            keyval_sum.made[i % 2, j, i // 2] = block[j * kv_each : (j + 1) * kv_each, :]
    keyval_sum.core_copy().start()
    grad_attn = grad_attn + dot_nt(gkv_t.T, wkv[...])
    attn_own[0:1, :] = jnp.sum(grad_attn * norm[...], axis=0, keepdims=True)
    attn_own[1:2, :] = jnp.sum(grad_attn, axis=0, keepdims=True)
    attn_own[3:4, 0 : 2 * HD] = dot_nt(ones, gkv_t)[0:1, :]
    attn_small.core_copy().start()
    attn_sum.sum_finish()
    attn_sum.line_start()
    keyval_sum.core_finish()
    keyval_sum.plane_start()
    attn_small.plane_start()
    back = dx[...] + grad_attn * row(again_ref)
    normed = norm[...]
    back_mean = jnp.mean(back, axis=1, keepdims=True)
    back_dot = jnp.mean(back * normed, axis=1, keepdims=True)
    dx[...] = go[...].astype(f32) + (back - back_mean - normed * back_dot) * rstd[:, 0:1]
    keyval_sum.plane_finish()
    keyval_sum.line_start()
    attn_small.line_start()
    stores = [store(dx, dx_hbm.at[0], 1)]
    stores[0].start()
    for i in range(seq_parts):
        load_again(i).wait()
        base[...] += dot(active_all[:, i * chunk : (i + 1) * chunk], wp[i % 2])
        if i + 2 < seq_parts:
            load_again(i + 2).start()
    feed[...] = (base[...] + dot(mix_t[...].T, wd[...])).astype(bf16)
    eout[...] = expand_sum.line_finish()
    pout[...] = project_sum.line_finish()
    stores += [store(feed, out_hbm.at[0], 0), store(eout, eout_hbm, 2), store(pout, pout_hbm, 3)]
    for copy in stores[1:]:
        copy.start()
    feed_small_ref[...] = feed_small.line_sum()
    qd_ref[...] = attn_sum.line_finish()
    summed = keyval_sum.line_finish()
    kvout_ref[...] = summed
    attn_small_ref[...] = attn_small.line_sum()
    for copy in stores:
        copy.wait()


def finish_kernel(
    parts, out_in, dx_in, e_in, p_in, qd_ref, kv_ref, feed_ref, attn_ref, out_hbm, dx_hbm, e_hbm, p_hbm,
    wq_ref, wd_ref, wkv_ref, again_ref, ashift_ref, fgain_ref, fshift_ref, qbias_ref, kvbias_ref,
    dbias_ref, ebias_ref, pbias_ref, out_buf, dx_buf, e_buf, p_buf, in_sem, out_sem,
):
    sources, targets = (out_in, dx_in, e_in, p_in), (out_hbm, dx_hbm, e_hbm, p_hbm)
    pieces = []
    for src, buf, dst in zip(sources, (out_buf, dx_buf, e_buf, p_buf), targets):
        count = 4 if len(src.shape) == 3 else 1
        size = src.shape[-2] // count
        for i in range(count):
            span = pl.ds(i * size, size)
            pieces.append(
                [v.at[0, span] if len(v.shape) == 3 else v.at[span] for v in (src, buf, dst)]
            )
    incoming = [pltpu.make_async_copy(p[0], p[1], in_sem.at[i]) for i, p in enumerate(pieces)]
    outgoing = [pltpu.make_async_copy(p[1], p[2], out_sem.at[i]) for i, p in enumerate(pieces)]
    for copy in incoming:
        copy.start()
    cols = wq_ref.shape[1]
    wq_ref[...] = qd_ref[:, 0:cols]
    wd_ref[...] = qd_ref[:, cols:]
    wkv_ref[...] = kv_ref[...]
    fgain_ref[...] = feed_ref[parts, :]
    fshift_ref[...] = feed_ref[parts + 1, :]
    dbias_ref[...] = feed_ref[parts + 2, :]
    pbias_ref[...] = feed_ref[parts + 2, :]
    width = feed_ref.shape[1]
    for i in range(parts):
        ebias_ref[i * width : (i + 1) * width] = feed_ref[i, :]
    again_ref[...] = attn_ref[0, :]
    ashift_ref[...] = attn_ref[1, :]
    qbias_ref[...] = attn_ref[2, :]
    kvbias_ref[...] = attn_ref[3, 0 : kvbias_ref.shape[0]]
    for i in range(len(pieces)):
        incoming[i].wait()
        outgoing[i].start()
    for copy in outgoing:
        copy.wait()


FIRST_EVENT = 3
SIDE_EVENT = 4
LINE_EVENT = 8
SMALL_EVENT = 9


def small_scratch(seq_parts, half, block):
    dma = pltpu.SemaphoreType.DMA
    return [
        pltpu.VMEM(block, f32), pltpu.VMEM(block, f32), pltpu.VMEM((seq_parts,) + block, f32),
        pltpu.VMEM((half,) + block, f32), dma((1,)), dma((1,)), dma((seq_parts - 1,)),
        dma((seq_parts - 1,)), dma((half - 1,)), dma((half - 1,)),
    ]


def fast_device(
    hidden_in, seq_lengths, attention_gain, attention_shift, feed_gain, feed_shift, query_weight,
    query_bias, keyval_weight, keyval_bias, dense_weight, dense_bias, expand_weight, expand_bias,
    project_weight, project_bias, out_grad,
):
    _, stretch, width = hidden_in.shape
    seq_parts, dp_parts = lax.axis_size("seq"), lax.axis_size("dp")
    half = dp_parts // 2
    hidden_units = expand_weight.shape[1]
    chunk = hidden_units // seq_parts
    whole_len = stretch * seq_parts
    rows, cols = width // dp_parts, width // seq_parts
    col_block, row_block = (rows, chunk), (cols, hidden_units // dp_parts)
    kv_block = (2 * HD // seq_parts, rows)
    small_block = (-(-(seq_parts + 3) // 8) * 8, width)
    sd, dma = jax.ShapeDtypeStruct, pltpu.SemaphoreType.DMA

    def vm(shape, dtype=bf16):
        return pltpu.VMEM(shape, dtype)

    in_vmem, in_hbm = pl.BlockSpec(memory_space=pltpu.VMEM), pl.BlockSpec(memory_space=pl.ANY)
    large = (
        sd((1, stretch, width), bf16), sd((1, stretch, width), f32), sd(col_block, f32),
        sd(row_block, f32),
    )
    mids = pl.pallas_call(
        functools.partial(layer_kernel, seq_parts, half),
        out_shape=large
        + (sd((rows, 2 * cols), f32), sd(kv_block, f32), sd(small_block, f32), sd(small_block, f32)),
        in_specs=[pl.BlockSpec(memory_space=pltpu.SMEM)] + [in_vmem] * 9 + [in_hbm] * 7,
        out_specs=(in_hbm,) * 4 + (in_vmem,) * 4,
        scratch_shapes=[
            vm((stretch, width)), vm((stretch, width)), vm((width, width)), vm((width, 2 * HD)),
            vm((width, width)), vm((2, width, chunk)), vm((2, chunk, width)),
            vm((stretch, width), f32), vm((stretch, 128), f32), vm((stretch, width)),
            vm((width, stretch)), vm((width, stretch)), vm((width, stretch)),
            vm((stretch, width), f32), vm((width, stretch)), vm((width, stretch)),
            vm((width, stretch)), vm((width, stretch)), vm((stretch, hidden_units)),
            vm((seq_parts, 2 * HD, stretch)), vm((HD, whole_len)), vm((HD + 16, whole_len)),
            vm((whole_len, 2 * HD)), vm((whole_len, 2 * HD)), vm((whole_len, stretch), f32),
            vm((whole_len, stretch)), vm((2 * HD, stretch)), vm((2 * HD, 2 * stretch)),
            vm((whole_len, 2 * HD), f32), vm((seq_parts - 1, stretch, 2 * HD)),
            vm((seq_parts - 1, stretch, 2 * HD)), vm((8, chunk), f32), vm((ROT, stretch), f32),
            vm((stretch, width), f32), vm(col_block, f32), vm(row_block, f32),
            dma((9,)), dma((4,)), dma((seq_parts - 1,)), dma((seq_parts - 1,)), dma((seq_parts - 1,)),
            dma((seq_parts - 1,)),
        ]
        + tree_scratch(half, col_block)
        + tree_scratch(half, row_block)
        + reduction_scratch(seq_parts, half, (rows, cols), (rows, cols))
        + small_scratch(seq_parts, half, small_block)
        + small_scratch(seq_parts, half, small_block)
        + keyval_scratch(seq_parts, half, kv_block),
        compiler_params=pltpu.CompilerParams(
            collective_id=0, has_side_effects=True, vmem_limit_bytes=VMEM_BYTES
        ),
    )(
        seq_lengths, attention_gain, attention_shift, feed_gain, feed_shift, query_bias, keyval_bias,
        dense_bias, expand_bias, project_bias, hidden_in, out_grad, query_weight, keyval_weight,
        dense_weight, expand_weight, project_weight,
    )
    vectors = (width, width, width, width, width, 2 * HD, width, hidden_units, width)
    outs = pl.pallas_call(
        functools.partial(finish_kernel, seq_parts),
        out_shape=large
        + (sd((rows, cols), f32), sd((rows, cols), f32), sd(kv_block, f32))
        + tuple(sd((size,), f32) for size in vectors),
        in_specs=[in_hbm] * 4 + [in_vmem] * 4,
        out_specs=(in_hbm,) * 4 + (in_vmem,) * 12,
        scratch_shapes=[pltpu.VMEM(v.shape, v.dtype) for v in large] + [dma((10,)), dma((10,))],
    )(*mids)
    (output, input_grad, expand_grad, project_grad, query_grad, dense_grad, keyval_grad, a_gain, a_shift,
     f_gain, f_shift, q_bias, kv_bias, d_bias, e_bias, p_bias) = outs
    return (
        output, input_grad, a_gain, a_shift, f_gain, f_shift, query_grad, q_bias, keyval_grad.T, kv_bias,
        dense_grad, d_bias, expand_grad, e_bias, project_grad.T, p_bias,
    )


def fits(hidden, expand_weight):
    seq_parts, dp_parts = lax.axis_size("seq"), lax.axis_size("dp")
    width, hidden_units = expand_weight.shape
    return (
        hidden.shape[0] == 1
        and dp_parts == 2 * seq_parts
        and seq_parts == 4
        and HEADS % seq_parts == 0
        and hidden_units == seq_parts * width
        and width % (16 * dp_parts) == 0
        and width % (16 * seq_parts) == 0
        and hidden_units % (128 * dp_parts) == 0
        and hidden.shape[1] % 128 == 0
    )


def solution(mesh):
    def either_way(*args):
        return (fast_device if fits(args[0], args[12]) else per_device)(*args)

    return jax.shard_map(
        either_way,
        mesh=mesh,
        in_specs=(
            P("dp", "seq", None),
            P("dp"),
            P(),
            P(),
            P(),
            P(),
            P(),
            P(),
            P(),
            P(),
            P(),
            P(),
            P(),
            P(),
            P(),
            P(),
            P("dp", "seq", None),
        ),
        out_specs=(
            P("dp", "seq", None),
            P("dp", "seq", None),
            P(),
            P(),
            P(),
            P(),
            P("dp", "seq"),
            P(),
            P("dp", "seq"),
            P(),
            P("dp", "seq"),
            P(),
            P("dp", "seq"),
            P(),
            P("dp", "seq"),
            P(),
        ),
        check_vma=False,
    )
```
